32 devices in a mesh: dp: 8 (over y, x, core), ctx: 4 (over z).
Axes of the slice: x: 2, y: 2, z: 4, core: 2. Of those that a mesh axis runs over, the one named last changes fastest.
Arguments:
- inputs: bfloat16 [16, 1024, 1024], P('dp', 'ctx'), may hold values from -6 to 6
- segment_ids: int32 [16, 1024], P('dp', 'ctx'), may hold values from 0 to 7, never falling along the last dimension, each value on 1 to 512 neighbouring positions
- first_gain: bfloat16 [1024], P(('dp', 'ctx')), may hold values from 0.5 to 1.5
- first_shift: bfloat16 [1024], P(('dp', 'ctx')), may hold values from -3 to 3
- query_weight: bfloat16 [1024, 1024], P(('dp', 'ctx')), may hold values from -0.1875 to 0.1875
- query_bias: bfloat16 [1024], P(('dp', 'ctx')), may hold values from -3 to 3
- key_weight: bfloat16 [1024, 1024], P(('dp', 'ctx')), may hold values from -0.1875 to 0.1875
- value_weight: bfloat16 [1024, 1024], P(('dp', 'ctx')), may hold values from -0.1875 to 0.1875
- value_bias: bfloat16 [1024], P(('dp', 'ctx')), may hold values from -3 to 3
- out_weight: bfloat16 [1024, 1024], P(('dp', 'ctx')), may hold values from -0.75 to 0.75
- out_bias: bfloat16 [1024], P(('dp', 'ctx')), may hold values from -3 to 3
- second_gain: bfloat16 [1024], P(('dp', 'ctx')), may hold values from 0.5 to 1.5
- second_shift: bfloat16 [1024], P(('dp', 'ctx')), may hold values from -3 to 3
- up_weight: bfloat16 [1024, 4096], P(('dp', 'ctx')), may hold values from -0.1875 to 0.1875
- up_bias: bfloat16 [4096], P(('dp', 'ctx')), may hold values from -3 to 3
- down_weight: bfloat16 [4096, 1024], P(('dp', 'ctx')), may hold values from -0.09375 to 0.09375
- down_bias: bfloat16 [1024], P(('dp', 'ctx')), may hold values from -3 to 3
- cotangent: bfloat16 [16, 1024, 1024], P('dp', 'ctx'), may hold values from -6 to 6
Outputs:
- output: bfloat16 [16, 1024, 1024], P('dp', 'ctx')
- input_grad: float32 [16, 1024, 1024], P('dp', 'ctx')
- first_gain_grad: float32 [1024], P(('dp', 'ctx'))
- first_shift_grad: float32 [1024], P(('dp', 'ctx'))
- query_weight_grad: float32 [1024, 1024], P(('dp', 'ctx'))
- query_bias_grad: float32 [1024], P(('dp', 'ctx'))
- key_weight_grad: float32 [1024, 1024], P(('dp', 'ctx'))
- value_weight_grad: float32 [1024, 1024], P(('dp', 'ctx'))
- value_bias_grad: float32 [1024], P(('dp', 'ctx'))
- out_weight_grad: float32 [1024, 1024], P(('dp', 'ctx'))
- out_bias_grad: float32 [1024], P(('dp', 'ctx'))
- second_gain_grad: float32 [1024], P(('dp', 'ctx'))
- second_shift_grad: float32 [1024], P(('dp', 'ctx'))
- up_weight_grad: float32 [1024, 4096], P(('dp', 'ctx'))
- up_bias_grad: float32 [4096], P(('dp', 'ctx'))
- down_weight_grad: float32 [4096, 1024], P(('dp', 'ctx'))
- down_bias_grad: float32 [1024], P(('dp', 'ctx'))
The draws below stay inside these ranges and needn't reach their ends.
Inputs may be any that keep to these rules, and one draw needn't show every extreme that they name: `segment_ids`: along each sequence the document numbers never fall; each document has 1 to half of 1024 tokens, and one of each sequence has exactly half of 1024.
All inputs are finite; a program needn't handle non-finite values.
Results may differ from the reference program's by a relative error of at most 0.013.
Values may be sent and summed in bfloat16 or wider, within the bound.
No kernel may reach another device: no remote copies, remote signals or barrier semaphores. Data moves between devices by JAX's collectives and lax.ppermute only.
A program may use at most 256 MiB of HBM per device.

```python
import math
import jax
import jax.numpy as jnp
import numpy as np
from jax import lax

D = 1024
H = 16
FF = 4096
SEQ = 1024
SEQS = 16


def levels(stream_key, dims, pieces, least, largest):
    def one(dim, shards_of):
        heights = jax.random.uniform(jax.random.fold_in(jax.random.fold_in(stream_key, 6), dim), (shards_of,), jnp.float32, least / len(pieces), largest / len(pieces))
        return jnp.repeat(jnp.exp(heights), dims[dim] // shards_of).reshape((-1,) + (1,) * (len(dims) - dim - 1))

    factor_of = one(*pieces[0])
    for cut in pieces[1:]:
        factor_of = factor_of * one(*cut)
    return factor_of


def profile(count, total, reach, skew):
    portions = [(1 << 20) // math.isqrt(rank ** skew) + 1 for rank in range(2, count + 1)]
    rest, counts = total - reach - (count - 1), [1] * (count - 1)
    while rest > 0:
        free = [i for i in range(count - 1) if counts[i] < reach]
        mass, left = sum([portions[i] for i in free]), rest
        for i in free:
            more = min(reach - counts[i], max(1, left * portions[i] // mass), rest)
            counts[i] = counts[i] + more
            rest = rest - more
    return np.array([reach] + counts)


def ragged(stream_key, number_of, total, reach, slope):
    if number_of == 2:
        one = jax.random.randint(stream_key, (), max(1, total - reach), min(reach, total - 1) + 1)
        return jnp.stack([one, total - one])
    tallies = jnp.asarray(profile(number_of, total, reach, slope), jnp.int32)
    pairs = (number_of - 1) // 2
    donor, sink = tallies[1:1 + 2 * pairs:2], tallies[2:2 + 2 * pairs:2]
    room = jnp.minimum(donor - 1, reach - sink)
    passed = jax.random.randint(jax.random.fold_in(stream_key, 1), (pairs,), 0, 1 << 20) % (room + 1)
    tallies = tallies.at[1:1 + 2 * pairs:2].set(donor - passed).at[2:2 + 2 * pairs:2].set(sink + passed)
    return tallies[jax.random.permutation(jax.random.fold_in(stream_key, 2), number_of)]


def bell_draw(stream_key, extent, scale, reach, shards=(), kind=jnp.bfloat16):
    drawn = scale * jax.random.normal(stream_key, extent, jnp.float32)
    if shards:
        drawn = drawn * levels(stream_key, extent, shards, -0.22, 0.18)
    return jnp.clip(drawn, -reach, reach).astype(kind)


def setup_inputs(seed: int = 0) -> dict:
    splits = jax.random.split(jax.random.key(seed), 19)
    inputs = bell_draw(splits[0], (SEQS, SEQ, D), 1.0, 6.0, ((0, 8), (1, 4)))
    segment_ids = jax.vmap(lambda own: jnp.searchsorted(jnp.cumsum(ragged(own, max(4, SEQ // 128), SEQ, SEQ // 2, 2)), jnp.arange(SEQ), side="right"))(jax.random.split(splits[1], SEQS)).reshape((SEQS, SEQ)).astype(jnp.int32)
    first_gain = jnp.clip(1.0 + 0.1 * jax.random.normal(splits[2], (D,), jnp.float32), 0.5, 1.5).astype(jnp.bfloat16)
    first_shift = bell_draw(splits[3], (D,), 0.2, 3.0, ((0, 32),))
    query_weight = bell_draw(splits[4], (D, D), D ** -0.5, 0.1875, ((0, 32),))
    query_bias = bell_draw(splits[5], (D,), 0.2, 3.0, ((0, 32),))
    key_weight = bell_draw(splits[6], (D, D), D ** -0.5, 0.1875, ((0, 32),))
    value_weight = bell_draw(splits[7], (D, D), D ** -0.5, 0.1875, ((0, 32),))
    value_bias = bell_draw(splits[8], (D,), 0.2, 3.0, ((0, 32),))
    out_weight = bell_draw(splits[9], (D, D), (D // 16) ** -0.5, 0.75, ((0, 32),))
    out_bias = bell_draw(splits[10], (D,), 0.2, 3.0, ((0, 32),))
    second_gain = jnp.clip(1.0 + 0.1 * jax.random.normal(splits[11], (D,), jnp.float32), 0.5, 1.5).astype(jnp.bfloat16)
    second_shift = bell_draw(splits[12], (D,), 0.2, 3.0, ((0, 32),))
    up_weight = bell_draw(splits[13], (D, FF), D ** -0.5, 0.1875, ((0, 32),))
    up_bias = bell_draw(splits[14], (FF,), 0.5, 3.0, ((0, 32),))
    down_weight = bell_draw(splits[15], (FF, D), FF ** -0.5, 0.09375, ((0, 32),))
    down_bias = bell_draw(splits[16], (D,), 0.2, 3.0, ((0, 32),))
    cotangent = bell_draw(splits[17], (SEQS, SEQ, D), 1.0, 6.0, ((0, 8), (1, 4)))
    return {"inputs": inputs, "segment_ids": segment_ids, "first_gain": first_gain, "first_shift": first_shift, "query_weight": query_weight, "query_bias": query_bias, "key_weight": key_weight, "value_weight": value_weight, "value_bias": value_bias, "out_weight": out_weight, "out_bias": out_bias, "second_gain": second_gain, "second_shift": second_shift, "up_weight": up_weight, "up_bias": up_bias, "down_weight": down_weight, "down_bias": down_bias, "cotangent": cotangent}


EPS = 1e-05
MASKED = -1e+30
HIGH = lax.Precision.HIGHEST

@jax.custom_vjp
def low(v):
    return lax.optimization_barrier(v.astype(jnp.bfloat16)).astype(jnp.float32)

@jax.custom_vjp
def low_back(v):
    return v

def low_keep(v):
    return (low(v), None)

def low_pass(kept, grad):
    return (grad,)

def back_keep(v):
    return (v, None)

def back_low(kept, grad):
    return (low(grad),)
low.defvjp(low_keep, low_pass)
low_back.defvjp(back_keep, back_low)

def normalize(values, gain, shift):
    mean = lax.optimization_barrier(jnp.mean(values, axis=-1, keepdims=True))
    centered = values - mean
    spread = lax.optimization_barrier(jnp.mean(centered * centered, axis=-1, keepdims=True))
    return centered * lax.rsqrt(spread + EPS) * gain + shift

def matmul(left, right):
    return jnp.einsum('...d,de->...e', left, right, precision=HIGH)

def attend(queries, keys, values, segments):
    length, width = queries.shape
    size = width // H
    query_heads = queries.reshape(length, H, size)
    key_heads = keys.reshape(length, H, size)
    value_heads = values.reshape(length, H, size)
    raw = jnp.einsum('qhd,khd->hqk', query_heads, key_heads, precision=HIGH)
    scores = low_back(raw * (1.0 / math.sqrt(size)))
    position = jnp.arange(length, dtype=jnp.int32)
    allowed = (position[None, :] <= position[:, None]) & (segments[None, :] == segments[:, None])
    scores = jnp.where(allowed[None], scores, MASKED)
    probs = low(jax.nn.softmax(scores, axis=-1))
    mixed = jnp.einsum('hqk,khd->qhd', probs, value_heads, precision=HIGH)
    return mixed.reshape(length, width)

def layer(params, inputs, segments):
    first_gain, first_shift, query_weight, query_bias, key_weight, value_weight, value_bias, out_weight, out_bias, second_gain, second_shift, up_weight, up_bias, down_weight, down_bias = params
    normed = low(normalize(inputs, first_gain, first_shift))
    queries = low(low_back(matmul(normed, query_weight) + query_bias))
    keys = low(low_back(matmul(normed, key_weight)))
    values = low(low_back(matmul(normed, value_weight) + value_bias))

    def one_sequence(item):
        return attend(item[0], item[1], item[2], item[3])
    mixed = lax.map(jax.checkpoint(one_sequence), (queries, keys, values, segments))
    mixed = low(low_back(mixed))
    middle = inputs + low_back(matmul(mixed, out_weight) + out_bias)
    second = low(normalize(middle, second_gain, second_shift))
    hidden_pre = low_back(matmul(second, up_weight) + up_bias)
    hidden = low(jax.nn.gelu(hidden_pre, approximate=False))
    return middle + low_back(matmul(hidden, down_weight) + down_bias)

def reference(inputs, segment_ids, first_gain, first_shift, query_weight, query_bias, key_weight, value_weight, value_bias, out_weight, out_bias, second_gain, second_shift, up_weight, up_bias, down_weight, down_bias, cotangent):
    params = tuple((item.astype(jnp.float32) for item in (first_gain, first_shift, query_weight, query_bias, key_weight, value_weight, value_bias, out_weight, out_bias, second_gain, second_shift, up_weight, up_bias, down_weight, down_bias)))
    group = 4 if SEQS % 4 == 0 else 2 if SEQS % 2 == 0 else 1
    blocks = SEQS // group
    source = inputs.astype(jnp.float32).reshape(blocks, group, SEQ, D)
    segments = segment_ids.reshape(blocks, group, SEQ)

    def forward(weights, values):

        def one_group(item):
            return layer(weights, item[0], item[1])
        return lax.map(jax.checkpoint(one_group), (values, segments))
    result, backward = jax.vjp(forward, params, source)
    grads, input_grad = backward(cotangent.astype(jnp.float32).reshape(blocks, group, SEQ, D))
    return (result.reshape(SEQS, SEQ, D).astype(jnp.bfloat16), input_grad.reshape(SEQS, SEQ, D), grads[0], grads[1], grads[2], grads[3], grads[4], grads[5], grads[6], grads[7], grads[8], grads[9], grads[10], grads[11], grads[12], grads[13], grads[14])
```

```python
from functools import partial
import math

import jax
import jax.numpy as jnp
from jax import lax
from jax.experimental import pallas as pl
from jax.experimental.pallas import tpu as pltpu
from jax.sharding import PartitionSpec as P

H = 16


EPS = 1e-05
MASKED = -1e30


def normalize(values, gain, shift):
    mean = jnp.mean(values, axis=-1, keepdims=True)
    centered = values - mean
    spread = jnp.mean(centered * centered, axis=-1, keepdims=True)
    return centered * lax.rsqrt(spread + EPS) * gain + shift


def product(left, right):
    return jnp.einsum("btd,de->bte", left, right, preferred_element_type=jnp.float32)


def product_back(left, right):
    return jnp.einsum("bte,de->btd", left, right, preferred_element_type=jnp.float32)


def outer_sum(left, right):
    return jnp.einsum("btd,bte->de", left, right, preferred_element_type=jnp.float32)


def column_sum(values):
    return jnp.sum(values.astype(jnp.float32), axis=(0, 1))


def gather_attention(
    first_gain,
    first_shift,
    query_weight,
    query_bias,
    key_weight,
    value_weight,
    value_bias,
    out_weight,
    out_bias,
):
    return (
        lax.all_gather(first_gain, ("dp", "ctx"), axis=0, tiled=True),
        lax.all_gather(first_shift, ("dp", "ctx"), axis=0, tiled=True),
        lax.all_gather(query_weight, ("dp", "ctx"), axis=0, tiled=True),
        lax.all_gather(query_bias, ("dp", "ctx"), axis=0, tiled=True),
        lax.all_gather(key_weight, ("dp", "ctx"), axis=0, tiled=True),
        lax.all_gather(value_weight, ("dp", "ctx"), axis=0, tiled=True),
        lax.all_gather(value_bias, ("dp", "ctx"), axis=0, tiled=True),
        lax.all_gather(out_weight, ("dp", "ctx"), axis=0, tiled=True),
        lax.all_gather(out_bias, ("dp", "ctx"), axis=0, tiled=True),
    )


def gather_feed(second_gain, second_shift, up_weight, up_bias, down_weight, down_bias):
    return (
        lax.all_gather(second_gain, ("dp", "ctx"), axis=0, tiled=True),
        lax.all_gather(second_shift, ("dp", "ctx"), axis=0, tiled=True),
        lax.all_gather(up_weight, ("dp", "ctx"), axis=0, tiled=True),
        lax.all_gather(up_bias, ("dp", "ctx"), axis=0, tiled=True),
        lax.all_gather(down_weight, ("dp", "ctx"), axis=0, tiled=True),
        lax.all_gather(down_bias, ("dp", "ctx"), axis=0, tiled=True),
    )


def gather_keys(keys, values, segments):
    return (
        lax.all_gather(keys, "ctx", axis=1, tiled=True),
        lax.all_gather(values, "ctx", axis=1, tiled=True),
        lax.all_gather(segments, "ctx", axis=1, tiled=True),
    )


def score_block(queries, keys_all, segments, segments_all):
    batch, rows, width = queries.shape
    size = width // H
    total_len = keys_all.shape[1]
    query_heads = queries.reshape(batch, rows, H, size)
    key_heads = keys_all.reshape(batch, total_len, H, size)
    raw = jnp.einsum("bqhd,bkhd->bhqk", query_heads, key_heads, preferred_element_type=jnp.float32)
    scores = raw * (1.0 / math.sqrt(size))
    offset = lax.axis_index("ctx") * rows
    query_pos = offset + jnp.arange(rows, dtype=jnp.int32)
    key_pos = jnp.arange(total_len, dtype=jnp.int32)
    causal = key_pos[None, :] <= query_pos[:, None]
    same_doc = segments[:, :, None] == segments_all[:, None, :]
    allowed = (causal[None] & same_doc)[:, None]
    return jnp.where(allowed, scores, MASKED)


def forward_part(inputs, segments, attn, feed):
    (
        first_gain,
        first_shift,
        query_weight,
        query_bias,
        key_weight,
        value_weight,
        value_bias,
        out_weight,
        out_bias,
    ) = attn
    second_gain, second_shift, up_weight, up_bias, down_weight, down_bias = feed
    batch, rows, width = inputs.shape
    size = width // H
    source = inputs.astype(jnp.float32)
    normed = normalize(
        source, first_gain.astype(jnp.float32), first_shift.astype(jnp.float32)
    ).astype(jnp.bfloat16)
    queries = (product(normed, query_weight) + query_bias.astype(jnp.float32)).astype(jnp.bfloat16)
    keys = product(normed, key_weight).astype(jnp.bfloat16)
    values = (product(normed, value_weight) + value_bias.astype(jnp.float32)).astype(jnp.bfloat16)
    keys_all, values_all, segments_all = gather_keys(keys, values, segments)
    scores = score_block(queries, keys_all, segments, segments_all)
    top = jnp.max(scores, axis=-1, keepdims=True)
    expo = jnp.exp(scores - top)
    row_total = jnp.sum(expo, axis=-1, keepdims=True)
    probs = (expo / row_total).astype(jnp.bfloat16)
    log_total = top + jnp.log(row_total)
    value_heads = values_all.reshape(batch, values_all.shape[1], H, size)
    mixed = jnp.einsum("bhqk,bkhd->bqhd", probs, value_heads, preferred_element_type=jnp.float32)
    mixed = mixed.reshape(batch, rows, width).astype(jnp.bfloat16)
    middle = source + product(mixed, out_weight) + out_bias.astype(jnp.float32)
    second = normalize(
        middle, second_gain.astype(jnp.float32), second_shift.astype(jnp.float32)
    ).astype(jnp.bfloat16)
    hidden_pre = product(second, up_weight) + up_bias.astype(jnp.float32)
    hidden = jax.nn.gelu(hidden_pre, approximate=False).astype(jnp.bfloat16)
    output = (middle + product(hidden, down_weight) + down_bias.astype(jnp.float32)).astype(
        jnp.bfloat16
    )
    kept = (
        source,
        normed,
        queries,
        keys,
        values,
        log_total,
        mixed,
        middle,
        second,
        hidden_pre,
        hidden,
    )
    return (output, kept, (keys_all, values_all, segments_all))


def backward_part(kept, gathered, segments, cotangent, attn, feed):
    (
        first_gain,
        first_shift,
        query_weight,
        query_bias,
        key_weight,
        value_weight,
        value_bias,
        out_weight,
        out_bias,
    ) = attn
    second_gain, second_shift, up_weight, up_bias, down_weight, down_bias = feed
    source, normed, queries, keys, values, log_total, mixed, middle, second, hidden_pre, hidden = (
        kept
    )
    keys_all, values_all, segments_all = gathered
    batch, rows, width = source.shape
    size = width // H
    total_len = keys_all.shape[1]
    scale = 1.0 / math.sqrt(size)
    down_grad = outer_sum(hidden, cotangent)
    down_bias_grad = column_sum(cotangent)
    hidden_grad = product_back(cotangent, down_weight)
    _, gelu_back = jax.vjp(partial(jax.nn.gelu, approximate=False), hidden_pre)
    pre_grad = gelu_back(hidden_grad)[0].astype(jnp.bfloat16)
    up_grad = outer_sum(second, pre_grad)
    up_bias_grad = column_sum(pre_grad)
    second_grad = product_back(pre_grad, up_weight)
    _, second_back = jax.vjp(
        normalize, middle, second_gain.astype(jnp.float32), second_shift.astype(jnp.float32)
    )
    middle_part, second_gain_grad, second_shift_grad = second_back(second_grad)
    feed_grads = (
        lax.psum_scatter(second_gain_grad, ("dp", "ctx"), scatter_dimension=0, tiled=True),
        lax.psum_scatter(second_shift_grad, ("dp", "ctx"), scatter_dimension=0, tiled=True),
        lax.psum_scatter(up_grad, ("dp", "ctx"), scatter_dimension=0, tiled=True),
        lax.psum_scatter(up_bias_grad, ("dp", "ctx"), scatter_dimension=0, tiled=True),
        lax.psum_scatter(down_grad, ("dp", "ctx"), scatter_dimension=0, tiled=True),
        lax.psum_scatter(down_bias_grad, ("dp", "ctx"), scatter_dimension=0, tiled=True),
    )
    middle_grad = cotangent.astype(jnp.float32) + middle_part
    branch_grad = middle_grad.astype(jnp.bfloat16)
    out_grad = outer_sum(mixed, branch_grad)
    out_bias_grad = column_sum(branch_grad)
    mixed_grad = product_back(branch_grad, out_weight).astype(jnp.bfloat16)
    scores = score_block(queries, keys_all, segments, segments_all)
    probs_full = jnp.exp(scores - log_total)
    probs = probs_full.astype(jnp.bfloat16)
    grad_heads = mixed_grad.reshape(batch, rows, H, size)
    query_heads = queries.reshape(batch, rows, H, size)
    key_heads = keys_all.reshape(batch, total_len, H, size)
    value_heads = values_all.reshape(batch, total_len, H, size)
    value_grad_all = jnp.einsum(
        "bhqk,bqhd->bkhd", probs, grad_heads, preferred_element_type=jnp.float32
    )
    prob_grad = jnp.einsum(
        "bqhd,bkhd->bhqk", grad_heads, value_heads, preferred_element_type=jnp.float32
    )
    delta = jnp.sum(probs_full * prob_grad, axis=-1, keepdims=True)
    score_grad = (probs_full * (prob_grad - delta)).astype(jnp.bfloat16)
    query_grad = (
        jnp.einsum("bhqk,bkhd->bqhd", score_grad, key_heads, preferred_element_type=jnp.float32)
        * scale
    )
    query_grad = query_grad.reshape(batch, rows, width).astype(jnp.bfloat16)
    key_grad_all = (
        jnp.einsum("bhqk,bqhd->bkhd", score_grad, query_heads, preferred_element_type=jnp.float32)
        * scale
    )
    key_sum, value_sum = (
        lax.psum_scatter(
            key_grad_all.reshape(batch, total_len, width).astype(jnp.bfloat16),
            "ctx",
            scatter_dimension=1,
            tiled=True,
        ).astype(jnp.float32),
        lax.psum_scatter(
            value_grad_all.reshape(batch, total_len, width).astype(jnp.bfloat16),
            "ctx",
            scatter_dimension=1,
            tiled=True,
        ).astype(jnp.float32),
    )
    key_grad = key_sum.astype(jnp.bfloat16)
    value_grad = value_sum.astype(jnp.bfloat16)
    query_weight_grad = outer_sum(normed, query_grad)
    query_bias_grad = column_sum(query_grad)
    key_weight_grad = outer_sum(normed, key_grad)
    value_weight_grad = outer_sum(normed, value_grad)
    value_bias_grad = column_sum(value_grad)
    normed_grad = (
        product_back(query_grad, query_weight)
        + product_back(key_grad, key_weight)
        + product_back(value_grad, value_weight)
    )
    _, first_back = jax.vjp(
        normalize, source, first_gain.astype(jnp.float32), first_shift.astype(jnp.float32)
    )
    input_part, first_gain_grad, first_shift_grad = first_back(normed_grad)
    input_grad = middle_grad + input_part
    attn_grads = (
        lax.psum_scatter(first_gain_grad, ("dp", "ctx"), scatter_dimension=0, tiled=True),
        lax.psum_scatter(first_shift_grad, ("dp", "ctx"), scatter_dimension=0, tiled=True),
        lax.psum_scatter(query_weight_grad, ("dp", "ctx"), scatter_dimension=0, tiled=True),
        lax.psum_scatter(query_bias_grad, ("dp", "ctx"), scatter_dimension=0, tiled=True),
        lax.psum_scatter(key_weight_grad, ("dp", "ctx"), scatter_dimension=0, tiled=True),
        lax.psum_scatter(value_weight_grad, ("dp", "ctx"), scatter_dimension=0, tiled=True),
        lax.psum_scatter(value_bias_grad, ("dp", "ctx"), scatter_dimension=0, tiled=True),
        lax.psum_scatter(out_grad, ("dp", "ctx"), scatter_dimension=0, tiled=True),
        lax.psum_scatter(out_bias_grad, ("dp", "ctx"), scatter_dimension=0, tiled=True),
    )
    return (input_grad, attn_grads, feed_grads)


def local(
    inputs,
    segment_ids,
    first_gain,
    first_shift,
    query_weight,
    query_bias,
    key_weight,
    value_weight,
    value_bias,
    out_weight,
    out_bias,
    second_gain,
    second_shift,
    up_weight,
    up_bias,
    down_weight,
    down_bias,
    cotangent,
):
    attn = gather_attention(
        first_gain,
        first_shift,
        query_weight,
        query_bias,
        key_weight,
        value_weight,
        value_bias,
        out_weight,
        out_bias,
    )
    feed = gather_feed(second_gain, second_shift, up_weight, up_bias, down_weight, down_bias)
    output, kept, gathered = forward_part(inputs, segment_ids, attn, feed)
    key_set = gather_keys(kept[3], kept[4], segment_ids)
    input_grad, attn_grads, feed_grads = backward_part(
        kept, key_set, segment_ids, cotangent, attn, feed
    )
    result = (output, input_grad)
    return result + tuple(attn_grads) + tuple(feed_grads)


AXES = ("dp", "ctx")
BLOCK = 256


def links(step):
    pairs = []
    for o in range(4):
        for c in range(2):
            for z in range(4):
                o2, c2, z2 = step(o, c, z)
                pairs.append(((o * 2 + c) * 4 + z, (o2 * 2 + c2) * 4 + z2))
    return pairs


X_SWAP = links(lambda o, c, z: (o ^ 1, c, z))
Y_SWAP = links(lambda o, c, z: (o ^ 2, c, z))
CORE_SWAP = links(lambda o, c, z: (o, 1 - c, z))
Z_UP = links(lambda o, c, z: (o, c, (z + 1) % 4))
Z_DOWN = links(lambda o, c, z: (o, c, (z + 3) % 4))
TO_SEQ = [links(lambda o, c, z, k=k: (o, z >> 1, 2 * c + ((z & 1) ^ k))) for k in range(2)]
TO_TOK = [links(lambda o, c, z, k=k: (o, z >> 1, 2 * c + ((z & 1) ^ k))) for k in range(2)]


def send(value, pairs):
    return lax.ppermute(value, AXES, pairs)


def place_position():
    dp = lax.axis_index("dp")
    return dp // 2, dp % 2, lax.axis_index("ctx")


def ring_index(kind, o, z):
    if kind == "z":
        return z, (z + 3) % 4, (z + 1) % 4, (z + 2) % 4
    return o, o ^ 1, o ^ 2, o ^ 3


def ring_gather(value, kind):
    n1, n2 = (Z_UP, Z_DOWN) if kind == "z" else (X_SWAP, Y_SWAP)
    f1, f2 = (n1, n2) if kind == "z" else (n2, n1)
    a = send(value, n1)
    b = send(value, n2)
    half = value.shape[0] // 2
    if value.ndim == 2:
        half = half // 16 * 16
    c1 = send(a[:half], f1)
    c2 = send(b[half:], f2)
    return value, a, b, c1, c2


def copy_kernel(moves, n_in, n_out):
    def body(*refs):
        ins, outs, sems = refs[:n_in], refs[n_in : n_in + n_out], refs[n_in + n_out]
        todo = moves(ins, outs)
        copies = [pltpu.make_async_copy(s, d, sems.at[i]) for i, (s, d) in enumerate(todo)]
        for copy in copies:
            copy.start()
        for copy in copies:
            copy.wait()

    return body


def assemble(pieces, shapes, moves, count, name):
    any_space = pl.BlockSpec(memory_space=pl.ANY)
    return pl.pallas_call(
        copy_kernel(moves, len(pieces), len(shapes)),
        out_shape=[jax.ShapeDtypeStruct(s, jnp.bfloat16) for s in shapes],
        in_specs=[any_space] * len(pieces),
        out_specs=[pl.BlockSpec(memory_space=pltpu.VMEM)] * len(shapes),
        scratch_shapes=[pltpu.SemaphoreType.DMA((count,))],
        name=name,
    )(*pieces)


def gather_ring_whole(value, kind, name):
    pieces = ring_gather(value, kind)
    rows = value.shape[0]
    half = pieces[3].shape[0]

    def moves(ins, outs):
        o, c, z = place_position()
        me, first, second, both = ring_index(kind, o, z)
        out = outs[0]
        return [
            (ins[0], out.at[me]),
            (ins[1], out.at[first]),
            (ins[2], out.at[second]),
            (ins[3], out.at[both, pl.ds(0, half)]),
            (ins[4], out.at[both, pl.ds(half, rows - half)]),
        ]

    return assemble(pieces, [(4,) + value.shape], moves, 5, name)[0]


def gather_chips(value, order, shapes, blocks, per_block, name):
    inner, outer = ("z", "xy") if order == "zx" else ("xy", "z")
    whole = gather_ring_whole(value, inner, name + "_inner")
    pieces = ring_gather(whole, outer)

    def moves(ins, outs):
        o, c, z = place_position()
        me, first, second, both = ring_index(outer, o, z)
        todo = []
        for ref, far, inners in (
            (ins[0], me, (0, 1, 2, 3)),
            (ins[1], first, (0, 1, 2, 3)),
            (ins[2], second, (0, 1, 2, 3)),
            (ins[3], both, (0, 1)),
            (ins[4], both, (2, 3)),
        ):
            for j, near in enumerate(inners):
                yx, zz = (far, near) if outer == "xy" else (near, far)
                todo += blocks(ref.at[j], outs, yx, zz)
        return todo

    return assemble(pieces, shapes, moves, 16 * per_block, name)


def split_half(block, axis):
    half = block.shape[axis] // 2
    return (
        lax.slice_in_dim(block, 0, half, axis=axis),
        lax.slice_in_dim(block, half, block.shape[axis], axis=axis),
    )


def ring_scatter(parts, axis, cut, kind, o, z):
    bf = jnp.bfloat16
    take = lambda k: lax.dynamic_index_in_dim(parts, k, axis, keepdims=False)
    if kind == "z":
        n1, n2 = Z_UP, Z_DOWN
        i1, i2, far = (z + 1) % 4, (z + 3) % 4, (z + 2) % 4
        me = z
    else:
        n1, n2 = X_SWAP, Y_SWAP
        i1, i2, far = o ^ 1, o ^ 2, o ^ 3
        me = o
    h1, h2 = split_half(take(far), cut)
    t1 = send(h1.astype(bf), n1)
    t2 = send(h2.astype(bf), n2)
    b1, b2 = split_half(take(i1), cut), split_half(take(i2), cut)
    f32 = jnp.float32
    plus = lambda u, v: (u.astype(f32) + v.astype(f32)).astype(bf)
    if kind == "z":
        s1 = lax.concatenate([plus(b1[0], t1), b1[1].astype(bf)], cut)
        s2 = lax.concatenate([b2[0].astype(bf), plus(b2[1], t2)], cut)
    else:
        s1 = lax.concatenate([b1[0].astype(bf), plus(b1[1], t2)], cut)
        s2 = lax.concatenate([plus(b2[0], t1), b2[1].astype(bf)], cut)
    u1 = send(s1, n1)
    u2 = send(s2, n2)
    return take(me).astype(f32) + u1.astype(f32) + u2.astype(f32)


def allowed_mask(column, row, i, low, high):
    rows = i * BLOCK + lax.broadcasted_iota(jnp.int32, (BLOCK, high - low), 0)
    cols = low + lax.broadcasted_iota(jnp.int32, (BLOCK, high - low), 1)
    same = column[i * BLOCK : i * BLOCK + BLOCK, :] == row[:, low:high]
    return same & (cols <= rows)


def key_range(i, total):
    return max(0, (i * BLOCK - total // 2 + 1) // BLOCK * BLOCK), (i + 1) * BLOCK


NT = (((1,), (1,)), ((), ()))
NN = (((1,), (0,)), ((), ()))
TN = (((0,), (0,)), ((), ()))


def dot32(left, right, dims):
    return lax.dot_general(left, right, dims, preferred_element_type=jnp.float32)


def attend_kernel(scale, column, row, q_ref, k_ref, v_ref, mixed_ref, log_ref):
    total = q_ref.shape[0]
    size = q_ref.shape[1] // 2
    lane = lax.broadcasted_iota(jnp.int32, (BLOCK, 2 * size), 1) < size
    for i in range(total // BLOCK):
        low, high = key_range(i, total)
        rows = pl.ds(i * BLOCK, BLOCK)
        mask = allowed_mask(column, row, i, low, high)
        keys, values = k_ref[low:high, :], v_ref[low:high, :]
        q = q_ref[rows, :]
        zero = jnp.zeros_like(q)
        outs, logs = [], []
        for own in (jnp.where(lane, q, zero), jnp.where(lane, zero, q)):
            s = jnp.where(mask, dot32(own, keys, NT) * scale, MASKED)
            top = jnp.max(s, axis=-1, keepdims=True)
            e = jnp.exp(s - top)
            tot = jnp.sum(e, axis=-1, keepdims=True)
            p = (e * (1.0 / tot)).astype(jnp.bfloat16)
            outs.append(dot32(p, values, NN))
            logs.append(top + jnp.log(tot))
        mixed_ref[rows, :] = jnp.where(lane, outs[0], outs[1]).astype(jnp.bfloat16)
        log_ref[rows, :] = jnp.where(lane, logs[0], logs[1])


def attend_back_kernel(
    scale, column, row, q_ref, k_ref, v_ref, log_ref, grad_ref, out_ref, bias_ref, dk, dv
):
    total = q_ref.shape[0]
    size = q_ref.shape[1] // 2
    bf = jnp.bfloat16
    lane = lax.broadcasted_iota(jnp.int32, (BLOCK, 2 * size), 1) < size
    dk[...] = jnp.zeros_like(dk)
    dv[...] = jnp.zeros_like(dv)
    dq_sum = jnp.zeros((1, 2 * size), jnp.float32)
    for i in range(total // BLOCK):
        low, high = key_range(i, total)
        rows = pl.ds(i * BLOCK, BLOCK)
        mask = allowed_mask(column, row, i, low, high)
        keys, values = k_ref[low:high, :], v_ref[low:high, :]
        q, g = q_ref[rows, :], grad_ref[rows, :]
        zero = jnp.zeros_like(q)
        dqs = []
        for h in range(2):
            qh = jnp.where(lane, q, zero) if h == 0 else jnp.where(lane, zero, q)
            gh = jnp.where(lane, g, zero) if h == 0 else jnp.where(lane, zero, g)
            log = log_ref[rows, h * size : h * size + 1]
            s = jnp.where(mask, dot32(qh, keys, NT) * scale, MASKED)
            p = jnp.exp(s - log)
            dp = dot32(gh, values, NT)
            delta = jnp.sum(p * dp, axis=-1, keepdims=True)
            ds = (p * (dp - delta)).astype(bf)
            dqs.append(dot32(ds, keys, NN))
            dk[low:high, :] += dot32(ds, qh, TN)
            dv[low:high, :] += dot32(p.astype(bf), gh, TN)
        dq = (jnp.where(lane, dqs[0], dqs[1]) * scale).astype(bf)
        out_ref[0, rows, :] = dq
        dq_sum += jnp.sum(dq.astype(jnp.float32), axis=0, keepdims=True)
    out_ref[1, :, :] = (dk[...] * scale).astype(bf)
    dvb = dv[...].astype(bf)
    out_ref[2, :, :] = dvb
    bias_ref[0:1, :] = dq_sum
    bias_ref[1:2, :] = jnp.sum(dvb.astype(jnp.float32), axis=0, keepdims=True)


def attend_specs(total, width):
    pick = lambda j: pl.BlockSpec((None, total, width), lambda h: (j, 0, h))
    return [
        pl.BlockSpec((total, 1), lambda h: (0, 0)),
        pl.BlockSpec((1, total), lambda h: (0, 0)),
        pick(0),
        pick(1),
        pick(2),
    ]


def attend(qkv, column, row, size):
    _, total, width = qkv.shape
    pair = 2 * size
    scale = 1.0 / math.sqrt(size)
    flat = pl.BlockSpec((total, pair), lambda h: (0, h))
    return pl.pallas_call(
        partial(attend_kernel, scale),
        grid=(width // pair,),
        in_specs=attend_specs(total, pair),
        out_specs=[flat, flat],
        out_shape=[
            jax.ShapeDtypeStruct((total, width), jnp.bfloat16),
            jax.ShapeDtypeStruct((total, width), jnp.float32),
        ],
        name="attend",
    )(column, row, qkv, qkv, qkv)


def attend_back(qkv, log, grad, column, row, size):
    _, total, width = qkv.shape
    pair = 2 * size
    scale = 1.0 / math.sqrt(size)
    flat = pl.BlockSpec((total, pair), lambda h: (0, h))
    return pl.pallas_call(
        partial(attend_back_kernel, scale),
        grid=(width // pair,),
        in_specs=attend_specs(total, pair) + [flat, flat],
        out_specs=[
            pl.BlockSpec((3, total, pair), lambda h: (0, 0, h)),
            pl.BlockSpec((2, pair), lambda h: (0, h)),
        ],
        out_shape=[
            jax.ShapeDtypeStruct((3, total, width), jnp.bfloat16),
            jax.ShapeDtypeStruct((2, width), jnp.float32),
        ],
        scratch_shapes=[pltpu.VMEM((total, pair), jnp.float32)] * 2,
        name="attend_back",
    )(column, row, qkv, qkv, qkv, log, grad)


def feed_kernel(second, cot, up, bias, down, hidden_ref, pre_ref, sum_ref):
    total = second.shape[0]
    root = math.sqrt(0.5)
    norm = 1.0 / math.sqrt(2.0 * math.pi)
    sums = jnp.zeros(sum_ref.shape, jnp.float32)
    for i in range(total // BLOCK):
        rows = pl.ds(i * BLOCK, BLOCK)
        v = dot32(second[rows, :], up[...], NN) + bias[...].astype(jnp.float32)
        g = dot32(cot[rows, :], down[...], NT)
        cdf = 0.5 * (1.0 + lax.erf(v * root))
        hidden_ref[rows, :] = (v * cdf).astype(jnp.bfloat16)
        pre = (g * (cdf + v * (norm * jnp.exp(-0.5 * (v * v))))).astype(jnp.bfloat16)
        pre_ref[rows, :] = pre
        sums += jnp.sum(pre.astype(jnp.float32), axis=0, keepdims=True)
    sum_ref[...] = sums


def feed_forward(second, cot, up, bias, down, tile=256):
    total, width = second.shape
    units = up.shape[1]
    whole = pl.BlockSpec((total, width), lambda u: (0, 0))
    cols = pl.BlockSpec((total, tile), lambda u: (0, u))
    line = pl.BlockSpec((1, tile), lambda u: (0, u))
    return pl.pallas_call(
        feed_kernel,
        grid=(units // tile,),
        in_specs=[
            whole,
            whole,
            pl.BlockSpec((width, tile), lambda u: (0, u)),
            line,
            pl.BlockSpec((tile, width), lambda u: (u, 0)),
        ],
        out_specs=[cols, cols, line],
        out_shape=[
            jax.ShapeDtypeStruct((total, units), jnp.bfloat16),
            jax.ShapeDtypeStruct((total, units), jnp.bfloat16),
            jax.ShapeDtypeStruct((1, units), jnp.float32),
        ],
        name="feed",
    )(second, cot, up, bias, down)


def moments(values):
    mean = jnp.mean(values, axis=-1, keepdims=True)
    centered = values - mean
    spread = lax.rsqrt(jnp.mean(centered * centered, axis=-1, keepdims=True) + EPS)
    return centered * spread, spread


def norm_back(n, spread, gain, grad):
    g = grad * gain
    part = spread * (
        g - jnp.mean(g, axis=-1, keepdims=True) - n * jnp.mean(g * n, axis=-1, keepdims=True)
    )
    return part, jnp.sum(grad * n, axis=0), jnp.sum(grad, axis=0)


def mm(left, right):
    return dot32(left, right, NN)


def mm_back(left, right):
    return dot32(left, right, NT)


def mm_outer(left, right):
    return dot32(left, right, TN)


def fast_local(
    inputs,
    segment_ids,
    first_gain,
    first_shift,
    query_weight,
    query_bias,
    key_weight,
    value_weight,
    value_bias,
    out_weight,
    out_bias,
    second_gain,
    second_shift,
    up_weight,
    up_bias,
    down_weight,
    down_bias,
    cotangent,
):
    bf, f32 = jnp.bfloat16, jnp.float32
    batch, rows, width = inputs.shape
    o, c, z = place_position()
    other = 1 - c
    total = batch * rows * 2
    half = width // 2
    units = up_weight.shape[1]
    own_units = units // 2
    lead = query_weight.shape[0]
    down_rows = down_weight.shape[0]
    size = width // H
    small_count = 8 * lead + down_rows

    def halves(weight):
        view = weight.reshape(lead, 4, 2, weight.shape[1] // 8)
        pick = lambda k: lax.dynamic_index_in_dim(view, k, 2, keepdims=False).reshape(
            lead, weight.shape[1] // 2
        )
        return pick(c), pick(other)

    q_own, q_far = halves(query_weight)
    k_own, k_far = halves(key_weight)
    v_own, v_far = halves(value_weight)
    up_own, up_far = halves(up_weight)
    small = jnp.concatenate(
        [
            first_gain,
            first_shift,
            query_bias,
            value_bias,
            out_bias,
            second_gain,
            second_shift,
            down_bias,
            up_bias,
        ]
    )
    small = jnp.pad(small, (0, half - small_count)).reshape(1, half)
    small = jnp.concatenate([small, jnp.zeros((7, half), bf)], axis=0)
    far = send(jnp.concatenate([q_far, k_far, v_far, small], axis=0), CORE_SWAP)
    up_recv = send(up_far, CORE_SWAP)

    def by_core(own, recv):
        return jnp.where(c == 0, jnp.stack([own, recv]), jnp.stack([recv, own]))

    attn_pay = jnp.concatenate(
        [out_weight[:, :half], out_weight[:, half:]]
        + [
            by_core(own, far[j * lead : (j + 1) * lead]).reshape(2 * lead, half)
            for j, own in enumerate((q_own, k_own, v_own))
        ]
        + [by_core(small, far[3 * lead :]).reshape(16, half)],
        axis=0,
    )
    up_pay = by_core(up_own, up_recv).reshape(2 * lead, own_units)

    def to_sequence(values, name):
        tail = values.shape[1:]
        parity = z & 1
        first = lax.dynamic_index_in_dim(values, parity, 0, keepdims=False)
        again = lax.dynamic_index_in_dim(values, 1 - parity, 0, keepdims=False)
        got = [send(first, TO_SEQ[0]), send(again, TO_SEQ[1])]
        mate = [send(g, CORE_SWAP) for g in got]

        def moves(ins, outs):
            _, cc, zz = place_position()
            out = outs[0]
            return [
                (ins[2 * m + k], out.at[(1 - cc if m else cc), (zz & 1) ^ k])
                for m in range(2)
                for k in range(2)
            ]

        return assemble(got + mate, [(2, 2) + tail], moves, 4, name)[0]

    seg = jnp.zeros((batch, 16, width), bf).at[:, 0, :rows].set(segment_ids.astype(bf))
    x_blocks = to_sequence(jnp.concatenate([inputs, seg], axis=1), "sequence_in")
    x_bf = x_blocks[:, :, :rows].reshape(total, width)
    segments = x_blocks[:, :, rows, :rows].reshape(total).astype(f32)
    column, row = segments.reshape(total, 1), segments.reshape(1, total)

    def attn_blocks(src, outs, yx, zz):
        todo = [
            (
                src.at[pl.ds(h * lead, lead)],
                outs[1].at[yx, zz, :, pl.ds(h * half, half)],
            )
            for h in range(2)
        ]
        for j in range(3):
            for cc in range(2):
                at = (2 + 2 * j + cc) * lead
                todo.append((src.at[pl.ds(at, lead)], outs[0].at[j, yx, cc, zz]))
        todo.append((src.at[pl.ds(8 * lead, 16)], outs[2].at[yx, zz]))
        return todo

    wqkv, wout, small_all = gather_chips(
        attn_pay,
        "zx",
        [(3, 4, 2, 4, lead, half), (4, 4, lead, width), (4, 4, 16, half)],
        attn_blocks,
        9,
        "gather_attn",
    )
    wqkv = wqkv.reshape(3, width, half)
    wout = wout.reshape(half, width)

    def up_blocks(src, outs, yx, zz):
        return [(src.at[pl.ds(cc * lead, lead)], outs[0].at[yx, cc, zz]) for cc in range(2)]

    wup = gather_chips(
        up_pay, "xz", [(4, 2, 4, lead, own_units)], up_blocks, 2, "gather_up"
    )[0].reshape(width, own_units)

    def down_blocks(src, outs, yx, zz):
        return [(src, outs[0].at[yx, zz])]

    wdown = gather_chips(
        down_weight, "zx", [(4, 4, down_rows, width)], down_blocks, 1, "gather_down"
    )[0].reshape(own_units, width)
    cot = to_sequence(cotangent, "cotangent_in").reshape(total, width)

    small_all = small_all.reshape(4, 4, 2, 8, half)[:, :, :, 0, :small_count]
    vectors = small_all[..., : 8 * lead].reshape(4, 4, 2, 8, lead).transpose(3, 0, 2, 1, 4)
    own_cols = lax.dynamic_index_in_dim(vectors, c, 2, keepdims=False).reshape(8, half)
    vectors = vectors.reshape(8, width).astype(f32)
    gain1, shift1, _, _, bias_o, gain2, shift2, bias_d = [vectors[j] for j in range(8)]
    qkv_bias = jnp.stack([own_cols[2], jnp.zeros_like(own_cols[2]), own_cols[3]]).astype(f32)
    bias_u = lax.dynamic_index_in_dim(small_all[..., 8 * lead :], c, 2, keepdims=False)
    bias_u = bias_u.reshape(1, own_units)

    source = x_bf.astype(f32)
    n1, r1 = moments(source)
    normed = (n1 * gain1 + shift1).astype(bf)
    qkv = jnp.einsum("td,jde->jte", normed, wqkv, preferred_element_type=f32)
    qkv = (qkv + qkv_bias[:, None]).astype(bf)
    mixed, log = attend(qkv, column, row, size)
    part = mm(mixed, wout).astype(bf)
    middle = source + part.astype(f32) + send(part, CORE_SWAP).astype(f32) + bias_o

    n2, r2 = moments(middle)
    second = (n2 * gain2 + shift2).astype(bf)
    hidden, pre_grad, up_bias_grad = feed_forward(second, cot, wup, bias_u, wdown)
    part = mm_back(pre_grad, wup).astype(bf)
    second_grad = part.astype(f32) + send(part, CORE_SWAP).astype(f32)
    down_grad = mm_outer(hidden, cot).reshape(4, 4, down_rows, width)
    up_grad = mm_outer(second, pre_grad).reshape(4, 2, 4, lead, own_units)
    down_half = ring_scatter(down_grad, 0, 1, "xy", o, z)
    up_half = ring_scatter(up_grad, 2, 2, "z", o, z)
    down_out = ring_scatter(down_half, 0, 0, "z", o, z)
    up_sum = ring_scatter(up_half, 0, 1, "xy", o, z)

    tokens = total // 2
    mine = lambda a: lax.dynamic_slice_in_dim(a, c * tokens, tokens, 0)
    theirs = lambda a: lax.dynamic_slice_in_dim(a, other * tokens, tokens, 0)

    out_part = mm(hidden, wdown)
    out_recv = send(theirs(out_part).astype(bf), CORE_SWAP)
    result = (mine(middle) + mine(out_part) + out_recv.astype(f32) + bias_d).astype(bf)

    def to_tokens(values):
        blocks = values.reshape(2, tokens // 2, width)
        parity = z & 1
        got = [
            send(lax.dynamic_index_in_dim(blocks, parity ^ k, 0, keepdims=False), TO_TOK[k])
            for k in range(2)
        ]
        return jnp.where(parity == 0, jnp.stack(got), jnp.stack(got[::-1]))

    output = to_tokens(result)

    middle_part, gain2_grad, shift2_grad = norm_back(n2, r2, gain2, second_grad)
    cot32 = cot.astype(f32)
    middle_grad = cot32 + middle_part
    branch = middle_grad.astype(bf)
    mixed_grad = mm_back(branch, wout).astype(bf)
    grads, qv_bias_grad = attend_back(qkv, log, mixed_grad, column, row, size)
    part = sum(mm_back(grads[j], wqkv[j]) for j in range(3)).astype(bf)
    normed_grad = part.astype(f32) + send(part, CORE_SWAP).astype(f32)
    out_grad = mm_outer(mixed, branch).reshape(4, 4, lead, width)
    qkv_grad = jnp.einsum("td,jte->jde", normed, grads, preferred_element_type=f32)
    qkv_grad = qkv_grad.reshape(3, 4, 2, 4, lead, half)
    input_part, gain1_grad, shift1_grad = norm_back(n1, r1, gain1, normed_grad)
    input_grad = to_tokens((mine(middle_grad) + mine(input_part)).astype(bf)).astype(f32)

    def own_rows(vector):
        return lax.dynamic_index_in_dim(vector.reshape(4, 2, 4, lead), c, 1, keepdims=False)

    by_chip = lambda vector: vector.reshape(4, 4, -1)
    small_grad = jnp.concatenate(
        [
            own_rows(gain1_grad),
            own_rows(shift1_grad),
            by_chip(qv_bias_grad[0]),
            by_chip(qv_bias_grad[1]),
            own_rows(jnp.sum(branch.astype(f32), axis=0)),
            own_rows(gain2_grad),
            own_rows(shift2_grad),
            own_rows(jnp.sum(cot32, axis=0)),
            by_chip(up_bias_grad),
        ],
        axis=-1,
    )
    small_grad = jnp.pad(small_grad, ((0, 0), (0, 0), (0, half - small_count)))
    small_grad = jnp.pad(small_grad[:, :, None], ((0, 0), (0, 0), (0, 15), (0, 0)))

    pack = jnp.concatenate(
        [out_grad[..., :half], out_grad[..., half:]]
        + [
            qkv_grad[j].transpose(0, 2, 1, 3, 4).reshape(4, 4, 2 * lead, half)
            for j in range(3)
        ]
        + [small_grad],
        axis=2,
    ).astype(bf)
    pack = ring_scatter(pack, 0, 1, "xy", o, z)
    pack = ring_scatter(pack, 0, 0, "z", o, z)
    out_out = jnp.concatenate([pack[:lead], pack[lead : 2 * lead]], axis=1)
    qkv_sum = pack[2 * lead : 8 * lead].reshape(3, 2, lead, half)
    small_sum = pack[8 * lead]

    def own_columns(grads, axis):
        pick = lambda k: lax.dynamic_index_in_dim(grads, k, axis, keepdims=False)
        kept, got = pick(c), send(pick(other), CORE_SWAP)
        cols = kept.shape[-1] // 4
        kept, got = [a.reshape(a.shape[:-1] + (4, 1, cols)) for a in (kept, got)]
        both = jnp.where(
            c == 0, jnp.concatenate([kept, got], -2), jnp.concatenate([got, kept], -2)
        )
        return both.reshape(both.shape[:-3] + (8 * cols,))

    qkv_out = own_columns(qkv_sum, 1)
    up_out = own_columns(up_sum, 0)
    vec = lambda j: small_sum[j * lead : (j + 1) * lead]
    return (
        output,
        input_grad,
        vec(0),
        vec(1),
        qkv_out[0],
        vec(2),
        qkv_out[1],
        qkv_out[2],
        vec(3),
        out_out,
        vec(4),
        vec(5),
        vec(6),
        up_out,
        small_sum[8 * lead : 8 * lead + down_rows],
        down_out,
        vec(7),
    )


def solution(mesh):
    fast = mesh.shape["dp"] == 8 and mesh.shape["ctx"] == 4
    return jax.shard_map(
        fast_local if fast else local,
        mesh=mesh,
        in_specs=(
            P("dp", "ctx", None),
            P("dp", "ctx"),
            P(("dp", "ctx")),
            P(("dp", "ctx")),
            P(("dp", "ctx"), None),
            P(("dp", "ctx")),
            P(("dp", "ctx"), None),
            P(("dp", "ctx"), None),
            P(("dp", "ctx")),
            P(("dp", "ctx"), None),
            P(("dp", "ctx")),
            P(("dp", "ctx")),
            P(("dp", "ctx")),
            P(("dp", "ctx"), None),
            P(("dp", "ctx")),
            P(("dp", "ctx"), None),
            P(("dp", "ctx")),
            P("dp", "ctx", None),
        ),
        out_specs=(
            P("dp", "ctx", None),
            P("dp", "ctx", None),
            P(("dp", "ctx")),
            P(("dp", "ctx")),
            P(("dp", "ctx"), None),
            P(("dp", "ctx")),
            P(("dp", "ctx"), None),
            P(("dp", "ctx"), None),
            P(("dp", "ctx")),
            P(("dp", "ctx"), None),
            P(("dp", "ctx")),
            P(("dp", "ctx")),
            P(("dp", "ctx")),
            P(("dp", "ctx"), None),
            P(("dp", "ctx")),
            P(("dp", "ctx"), None),
            P(("dp", "ctx")),
        ),
        check_vma=False,
    )
```

```python
from functools import partial
import math

import jax
import jax.numpy as jnp
from jax import lax
from jax.experimental import pallas as pl
from jax.experimental.pallas import tpu as pltpu
from jax.sharding import PartitionSpec as P

H = 16


EPS = 1e-05
MASKED = -1e30


def normalize(values, gain, shift):
    mean = jnp.mean(values, axis=-1, keepdims=True)
    centered = values - mean
    spread = jnp.mean(centered * centered, axis=-1, keepdims=True)
    return centered * lax.rsqrt(spread + EPS) * gain + shift


def product(left, right):
    return jnp.einsum("btd,de->bte", left, right, preferred_element_type=jnp.float32)


def product_back(left, right):
    return jnp.einsum("bte,de->btd", left, right, preferred_element_type=jnp.float32)


def outer_sum(left, right):
    return jnp.einsum("btd,bte->de", left, right, preferred_element_type=jnp.float32)


def column_sum(values):
    return jnp.sum(values.astype(jnp.float32), axis=(0, 1))


def gather_attention(
    first_gain,
    first_shift,
    query_weight,
    query_bias,
    key_weight,
    value_weight,
    value_bias,
    out_weight,
    out_bias,
):
    return (
        lax.all_gather(first_gain, ("dp", "ctx"), axis=0, tiled=True),
        lax.all_gather(first_shift, ("dp", "ctx"), axis=0, tiled=True),
        lax.all_gather(query_weight, ("dp", "ctx"), axis=0, tiled=True),
        lax.all_gather(query_bias, ("dp", "ctx"), axis=0, tiled=True),
        lax.all_gather(key_weight, ("dp", "ctx"), axis=0, tiled=True),
        lax.all_gather(value_weight, ("dp", "ctx"), axis=0, tiled=True),
        lax.all_gather(value_bias, ("dp", "ctx"), axis=0, tiled=True),
        lax.all_gather(out_weight, ("dp", "ctx"), axis=0, tiled=True),
        lax.all_gather(out_bias, ("dp", "ctx"), axis=0, tiled=True),
    )


def gather_feed(second_gain, second_shift, up_weight, up_bias, down_weight, down_bias):
    return (
        lax.all_gather(second_gain, ("dp", "ctx"), axis=0, tiled=True),
        lax.all_gather(second_shift, ("dp", "ctx"), axis=0, tiled=True),
        lax.all_gather(up_weight, ("dp", "ctx"), axis=0, tiled=True),
        lax.all_gather(up_bias, ("dp", "ctx"), axis=0, tiled=True),
        lax.all_gather(down_weight, ("dp", "ctx"), axis=0, tiled=True),
        lax.all_gather(down_bias, ("dp", "ctx"), axis=0, tiled=True),
    )


def gather_keys(keys, values, segments):
    return (
        lax.all_gather(keys, "ctx", axis=1, tiled=True),
        lax.all_gather(values, "ctx", axis=1, tiled=True),
        lax.all_gather(segments, "ctx", axis=1, tiled=True),
    )


def score_block(queries, keys_all, segments, segments_all):
    batch, rows, width = queries.shape
    size = width // H
    total_len = keys_all.shape[1]
    query_heads = queries.reshape(batch, rows, H, size)
    key_heads = keys_all.reshape(batch, total_len, H, size)
    raw = jnp.einsum("bqhd,bkhd->bhqk", query_heads, key_heads, preferred_element_type=jnp.float32)
    scores = raw * (1.0 / math.sqrt(size))
    offset = lax.axis_index("ctx") * rows
    query_pos = offset + jnp.arange(rows, dtype=jnp.int32)
    key_pos = jnp.arange(total_len, dtype=jnp.int32)
    causal = key_pos[None, :] <= query_pos[:, None]
    same_doc = segments[:, :, None] == segments_all[:, None, :]
    allowed = (causal[None] & same_doc)[:, None]
    return jnp.where(allowed, scores, MASKED)


def forward_part(inputs, segments, attn, feed):
    (
        first_gain,
        first_shift,
        query_weight,
        query_bias,
        key_weight,
        value_weight,
        value_bias,
        out_weight,
        out_bias,
    ) = attn
    second_gain, second_shift, up_weight, up_bias, down_weight, down_bias = feed
    batch, rows, width = inputs.shape
    size = width // H
    source = inputs.astype(jnp.float32)
    normed = normalize(
        source, first_gain.astype(jnp.float32), first_shift.astype(jnp.float32)
    ).astype(jnp.bfloat16)
    queries = (product(normed, query_weight) + query_bias.astype(jnp.float32)).astype(jnp.bfloat16)
    keys = product(normed, key_weight).astype(jnp.bfloat16)
    values = (product(normed, value_weight) + value_bias.astype(jnp.float32)).astype(jnp.bfloat16)
    keys_all, values_all, segments_all = gather_keys(keys, values, segments)
    scores = score_block(queries, keys_all, segments, segments_all)
    top = jnp.max(scores, axis=-1, keepdims=True)
    expo = jnp.exp(scores - top)
    row_total = jnp.sum(expo, axis=-1, keepdims=True)
    probs = (expo / row_total).astype(jnp.bfloat16)
    log_total = top + jnp.log(row_total)
    value_heads = values_all.reshape(batch, values_all.shape[1], H, size)
    mixed = jnp.einsum("bhqk,bkhd->bqhd", probs, value_heads, preferred_element_type=jnp.float32)
    mixed = mixed.reshape(batch, rows, width).astype(jnp.bfloat16)
    middle = source + product(mixed, out_weight) + out_bias.astype(jnp.float32)
    second = normalize(
        middle, second_gain.astype(jnp.float32), second_shift.astype(jnp.float32)
    ).astype(jnp.bfloat16)
    hidden_pre = product(second, up_weight) + up_bias.astype(jnp.float32)
    hidden = jax.nn.gelu(hidden_pre, approximate=False).astype(jnp.bfloat16)
    output = (middle + product(hidden, down_weight) + down_bias.astype(jnp.float32)).astype(
        jnp.bfloat16
    )
    kept = (
        source,
        normed,
        queries,
        keys,
        values,
        log_total,
        mixed,
        middle,
        second,
        hidden_pre,
        hidden,
    )
    return (output, kept, (keys_all, values_all, segments_all))


def backward_part(kept, gathered, segments, cotangent, attn, feed):
    (
        first_gain,
        first_shift,
        query_weight,
        query_bias,
        key_weight,
        value_weight,
        value_bias,
        out_weight,
        out_bias,
    ) = attn
    second_gain, second_shift, up_weight, up_bias, down_weight, down_bias = feed
    source, normed, queries, keys, values, log_total, mixed, middle, second, hidden_pre, hidden = (
        kept
    )
    keys_all, values_all, segments_all = gathered
    batch, rows, width = source.shape
    size = width // H
    total_len = keys_all.shape[1]
    scale = 1.0 / math.sqrt(size)
    down_grad = outer_sum(hidden, cotangent)
    down_bias_grad = column_sum(cotangent)
    hidden_grad = product_back(cotangent, down_weight)
    _, gelu_back = jax.vjp(partial(jax.nn.gelu, approximate=False), hidden_pre)
    pre_grad = gelu_back(hidden_grad)[0].astype(jnp.bfloat16)
    up_grad = outer_sum(second, pre_grad)
    up_bias_grad = column_sum(pre_grad)
    second_grad = product_back(pre_grad, up_weight)
    _, second_back = jax.vjp(
        normalize, middle, second_gain.astype(jnp.float32), second_shift.astype(jnp.float32)
    )
    middle_part, second_gain_grad, second_shift_grad = second_back(second_grad)
    feed_grads = (
        lax.psum_scatter(second_gain_grad, ("dp", "ctx"), scatter_dimension=0, tiled=True),
        lax.psum_scatter(second_shift_grad, ("dp", "ctx"), scatter_dimension=0, tiled=True),
        lax.psum_scatter(up_grad, ("dp", "ctx"), scatter_dimension=0, tiled=True),
        lax.psum_scatter(up_bias_grad, ("dp", "ctx"), scatter_dimension=0, tiled=True),
        lax.psum_scatter(down_grad, ("dp", "ctx"), scatter_dimension=0, tiled=True),
        lax.psum_scatter(down_bias_grad, ("dp", "ctx"), scatter_dimension=0, tiled=True),
    )
    middle_grad = cotangent.astype(jnp.float32) + middle_part
    branch_grad = middle_grad.astype(jnp.bfloat16)
    out_grad = outer_sum(mixed, branch_grad)
    out_bias_grad = column_sum(branch_grad)
    mixed_grad = product_back(branch_grad, out_weight).astype(jnp.bfloat16)
    scores = score_block(queries, keys_all, segments, segments_all)
    probs_full = jnp.exp(scores - log_total)
    probs = probs_full.astype(jnp.bfloat16)
    grad_heads = mixed_grad.reshape(batch, rows, H, size)
    query_heads = queries.reshape(batch, rows, H, size)
    key_heads = keys_all.reshape(batch, total_len, H, size)
    value_heads = values_all.reshape(batch, total_len, H, size)
    value_grad_all = jnp.einsum(
        "bhqk,bqhd->bkhd", probs, grad_heads, preferred_element_type=jnp.float32
    )
    prob_grad = jnp.einsum(
        "bqhd,bkhd->bhqk", grad_heads, value_heads, preferred_element_type=jnp.float32
    )
    delta = jnp.sum(probs_full * prob_grad, axis=-1, keepdims=True)
    score_grad = (probs_full * (prob_grad - delta)).astype(jnp.bfloat16)
    query_grad = (
        jnp.einsum("bhqk,bkhd->bqhd", score_grad, key_heads, preferred_element_type=jnp.float32)
        * scale
    )
    query_grad = query_grad.reshape(batch, rows, width).astype(jnp.bfloat16)
    key_grad_all = (
        jnp.einsum("bhqk,bqhd->bkhd", score_grad, query_heads, preferred_element_type=jnp.float32)
        * scale
    )
    key_sum, value_sum = (
        lax.psum_scatter(
            key_grad_all.reshape(batch, total_len, width).astype(jnp.bfloat16),
            "ctx",
            scatter_dimension=1,
            tiled=True,
        ).astype(jnp.float32),
        lax.psum_scatter(
            value_grad_all.reshape(batch, total_len, width).astype(jnp.bfloat16),
            "ctx",
            scatter_dimension=1,
            tiled=True,
        ).astype(jnp.float32),
    )
    key_grad = key_sum.astype(jnp.bfloat16)
    value_grad = value_sum.astype(jnp.bfloat16)
    query_weight_grad = outer_sum(normed, query_grad)
    query_bias_grad = column_sum(query_grad)
    key_weight_grad = outer_sum(normed, key_grad)
    value_weight_grad = outer_sum(normed, value_grad)
    value_bias_grad = column_sum(value_grad)
    normed_grad = (
        product_back(query_grad, query_weight)
        + product_back(key_grad, key_weight)
        + product_back(value_grad, value_weight)
    )
    _, first_back = jax.vjp(
        normalize, source, first_gain.astype(jnp.float32), first_shift.astype(jnp.float32)
    )
    input_part, first_gain_grad, first_shift_grad = first_back(normed_grad)
    input_grad = middle_grad + input_part
    attn_grads = (
        lax.psum_scatter(first_gain_grad, ("dp", "ctx"), scatter_dimension=0, tiled=True),
        lax.psum_scatter(first_shift_grad, ("dp", "ctx"), scatter_dimension=0, tiled=True),
        lax.psum_scatter(query_weight_grad, ("dp", "ctx"), scatter_dimension=0, tiled=True),
        lax.psum_scatter(query_bias_grad, ("dp", "ctx"), scatter_dimension=0, tiled=True),
        lax.psum_scatter(key_weight_grad, ("dp", "ctx"), scatter_dimension=0, tiled=True),
        lax.psum_scatter(value_weight_grad, ("dp", "ctx"), scatter_dimension=0, tiled=True),
        lax.psum_scatter(value_bias_grad, ("dp", "ctx"), scatter_dimension=0, tiled=True),
        lax.psum_scatter(out_grad, ("dp", "ctx"), scatter_dimension=0, tiled=True),
        lax.psum_scatter(out_bias_grad, ("dp", "ctx"), scatter_dimension=0, tiled=True),
    )
    return (input_grad, attn_grads, feed_grads)


def local(
    inputs,
    segment_ids,
    first_gain,
    first_shift,
    query_weight,
    query_bias,
    key_weight,
    value_weight,
    value_bias,
    out_weight,
    out_bias,
    second_gain,
    second_shift,
    up_weight,
    up_bias,
    down_weight,
    down_bias,
    cotangent,
):
    attn = gather_attention(
        first_gain,
        first_shift,
        query_weight,
        query_bias,
        key_weight,
        value_weight,
        value_bias,
        out_weight,
        out_bias,
    )
    feed = gather_feed(second_gain, second_shift, up_weight, up_bias, down_weight, down_bias)
    output, kept, gathered = forward_part(inputs, segment_ids, attn, feed)
    key_set = gather_keys(kept[3], kept[4], segment_ids)
    input_grad, attn_grads, feed_grads = backward_part(
        kept, key_set, segment_ids, cotangent, attn, feed
    )
    result = (output, input_grad)
    return result + tuple(attn_grads) + tuple(feed_grads)


AXES = ("dp", "ctx")
BLOCK = 256
BF = jnp.bfloat16
F32 = jnp.float32
NT = (((1,), (1,)), ((), ()))
NN = (((1,), (0,)), ((), ()))
TN = (((0,), (0,)), ((), ()))
ANY = pl.BlockSpec(memory_space=pl.ANY)
VMEM = pl.BlockSpec(memory_space=pltpu.VMEM)


def links(step):
    pairs = []
    for o in range(4):
        for c in range(2):
            for z in range(4):
                o2, c2, z2 = step(o, c, z)
                pairs.append(((o * 2 + c) * 4 + z, (o2 * 2 + c2) * 4 + z2))
    return pairs


X_SWAP = links(lambda o, c, z: (o ^ 1, c, z))
Y_SWAP = links(lambda o, c, z: (o ^ 2, c, z))
CORE_SWAP = links(lambda o, c, z: (o, 1 - c, z))
Z_UP = links(lambda o, c, z: (o, c, (z + 1) % 4))
Z_DOWN = links(lambda o, c, z: (o, c, (z + 3) % 4))
SEQUENCE = [links(lambda o, c, z, k=k: (o, z >> 1, 2 * c + ((z & 1) ^ k))) for k in range(2)]


def send(value, pairs):
    return lax.ppermute(value, AXES, pairs)


def place():
    dp = lax.axis_index("dp")
    return dp // 2, dp % 2, lax.axis_index("ctx")


def dot32(left, right, dims):
    return lax.dot_general(left, right, dims, preferred_element_type=F32)


def shape(dims, kind=BF):
    return jax.ShapeDtypeStruct(dims, kind)


def cost(flops, nbytes, special=0):
    return pl.CostEstimate(flops=int(flops), bytes_accessed=int(nbytes), transcendentals=special)


def call(body, ins, outs, name, in_specs=None, out_specs=None, scratch=(), flops=0, grid=()):
    moved = sum(a.size * a.dtype.itemsize for a in ins)
    moved += sum(math.prod(a.shape) * jnp.dtype(a.dtype).itemsize for a in outs)
    return pl.pallas_call(
        body,
        grid=grid,
        in_specs=in_specs or [VMEM] * len(ins),
        out_specs=out_specs or [VMEM] * len(outs),
        out_shape=outs,
        scratch_shapes=list(scratch),
        cost_estimate=cost(flops, moved),
        name=name,
    )(*ins)


def placed_call(body, pos, ins, outs, name, grid, in_specs, out_specs, scratch=(), flops=0):
    moved = sum(a.size * a.dtype.itemsize for a in ins)
    moved += sum(math.prod(a.shape) * jnp.dtype(a.dtype).itemsize for a in outs)
    return pl.pallas_call(
        body,
        grid_spec=pltpu.PrefetchScalarGridSpec(
            num_scalar_prefetch=1,
            grid=grid,
            in_specs=in_specs,
            out_specs=out_specs,
            scratch_shapes=list(scratch),
        ),
        out_shape=outs,
        cost_estimate=cost(flops, moved),
        name=name,
    )(pos, *ins)


def copies(ins, outs, moves, count, name):
    def body(*refs):
        sems = refs[-1]
        todo = moves(refs[: len(ins)], refs[len(ins) : -1])
        started = [pltpu.make_async_copy(s, d, sems.at[i]) for i, (s, d) in enumerate(todo)]
        for copy in started:
            copy.start()
        for copy in started:
            copy.wait()

    return call(
        body,
        ins,
        outs,
        name,
        in_specs=[ANY] * len(ins),
        scratch=[pltpu.SemaphoreType.DMA((count,))],
    )


def own_columns(weight, k):
    n = weight.shape[1] // 8
    parts = [
        jnp.where(k == 0, weight[:, 2 * g * n : (2 * g + 1) * n], weight[:, (2 * g + 1) * n : (2 * g + 2) * n])
        for g in range(4)
    ]
    return jnp.concatenate(parts, axis=1)


def first_kernel(qw, kw, vw, uw, small, inputs, segs, far, up_far, in0, in1, sems):
    _, c, z = place()
    rows = inputs.shape[1]
    parity = lax.rem(z, 2)
    todo = []
    for k, out in enumerate((in0, in1)):
        pick = parity if k == 0 else 1 - parity
        todo.append(pltpu.make_async_copy(inputs.at[pick], out.at[pl.ds(0, rows)], sems.at[k]))
        todo[-1].start()
        line = segs[pl.ds(pick, 1), :].astype(F32)
        out[rows:, :] = jnp.zeros((out.shape[0] - rows, out.shape[1]), BF)
        out[rows:, :rows] = jnp.broadcast_to(line, (out.shape[0] - rows, rows)).astype(BF)
    lead = qw.shape[0]
    for j, ref in enumerate((qw, kw, vw)):
        far[j * lead : (j + 1) * lead, :] = own_columns(ref[...], 1 - c)
    far[3 * lead :, :] = small[...]
    up_far[...] = own_columns(uw[...], 1 - c)
    for copy in todo:
        copy.wait()


def second_kernel(qw, kw, vw, ow, uw, small, far, up_far, attn, up):
    _, c, _ = place()
    lead, width = ow.shape
    half = width // 2
    attn[0:lead, :] = ow[:, :half]
    attn[lead : 2 * lead, :] = ow[:, half:]

    def both(out, at, own, got):
        n = own.shape[0]
        out[at : at + n, :] = jnp.where(c == 0, own, got)
        out[at + n : at + 2 * n, :] = jnp.where(c == 0, got, own)

    for j, ref in enumerate((qw, kw, vw)):
        both(attn, (2 + 2 * j) * lead, own_columns(ref[...], c), far[j * lead : (j + 1) * lead, :])
    both(attn, 8 * lead, small[...], far[3 * lead :, :])
    both(up, 0, own_columns(uw[...], c), up_far[...])


def inner_kernel_moves(n):
    def moves(ins, outs):
        todo = []
        for g in range(n):
            own, first, second, far1, far2 = ins[5 * g : 5 * g + 5]
            low, high = outs[2 * g : 2 * g + 2]
            cut = far1.shape[0]
            todo += [
                (own, low.at[0]),
                (first, low.at[1]),
                (second, high.at[0]),
                (far1, high.at[1, pl.ds(0, cut)]),
                (far2, high.at[1, pl.ds(cut, far2.shape[0])]),
            ]
        return todo

    return moves


def ring_first(value, n1, n2):
    return send(value, n1), send(value, n2)


def ring_second(a, b, f1, f2):
    cut = a.shape[0] // 2 // 16 * 16
    return send(a[:cut], f1), send(b[cut:], f2)


def ring_outer(low, high, n1, n2, f1, f2):
    b_high = send(high, n2)
    a_low = send(low, n1)
    b_low = send(low, n2)
    a_high = send(high, n1)
    return [low, high, a_low, a_high, b_low, b_high, send(a_low, f1), send(b_high, f2)]


def final_moves(ins, outs, inner, blocks):
    o, c, z = place()
    z_ring = (z, lax.rem(z + 3, 4), lax.rem(z + 1, 4), lax.rem(z + 2, 4))
    yx_ring = (o, o ^ 1, o ^ 2, o ^ 3)
    near, far = (z_ring, yx_ring) if inner == "z" else (yx_ring, z_ring)
    todo = []
    for i, (k, part) in enumerate(((0, 0), (0, 1), (1, 0), (1, 1), (2, 0), (2, 1), (3, 0), (3, 1))):
        for j in range(2):
            a, b = near[2 * part + j], far[k]
            yx, zz = (b, a) if inner == "z" else (a, b)
            todo += blocks(ins[i].at[j], outs, yx, zz)
    return todo


def moments(values):
    mean = jnp.mean(values, axis=-1, keepdims=True)
    centered = values - mean
    spread = lax.rsqrt(jnp.mean(centered * centered, axis=-1, keepdims=True) + EPS)
    return centered * spread, spread


def project_kernel(x, gain, shift, weight, bias, normed, qkv):
    n, _ = moments(x[...].astype(F32))
    value = (n * gain[...] + shift[...]).astype(BF)
    normed[...] = value
    for j in range(3):
        qkv[j] = (dot32(value, weight[j], NN) + bias[j : j + 1, :]).astype(BF)


def project(x, gain, shift, weight, bias):
    total, width = x.shape
    half = weight.shape[2]
    rows = pl.BlockSpec((BLOCK, width), lambda i: (i, 0))
    line = pl.BlockSpec((1, width), lambda i: (0, 0))
    return call(
        project_kernel,
        [x, gain, shift, weight, bias],
        [shape((total, width)), shape((3, total, half))],
        "project",
        in_specs=[
            rows,
            line,
            line,
            pl.BlockSpec((3, width, half), lambda i: (0, 0, 0)),
            pl.BlockSpec((3, half), lambda i: (0, 0)),
        ],
        out_specs=[rows, pl.BlockSpec((3, BLOCK, half), lambda i: (0, i, 0))],
        flops=6 * total * width * half,
        grid=(total // BLOCK,),
    )


def allowed_mask(column, row, i, low, high):
    rows = i * BLOCK + lax.broadcasted_iota(jnp.int32, (BLOCK, high - low), 0)
    cols = low + lax.broadcasted_iota(jnp.int32, (BLOCK, high - low), 1)
    same = column[i * BLOCK : i * BLOCK + BLOCK, :] == row[:, low:high]
    return same & (cols <= rows)


def key_range(i, total):
    return max(0, (i * BLOCK - total // 2 + 1) // BLOCK * BLOCK), (i + 1) * BLOCK


def attend_kernel(scale, column, row, q_ref, k_ref, v_ref, _, mixed_ref, log_ref):
    total = q_ref.shape[0]
    size = q_ref.shape[1] // 2
    lane = lax.broadcasted_iota(jnp.int32, (BLOCK, 2 * size), 1) < size
    for i in range(total // BLOCK):
        low, high = key_range(i, total)
        rows = pl.ds(i * BLOCK, BLOCK)
        mask = allowed_mask(column, row, i, low, high)
        keys, values = k_ref[low:high, :], v_ref[low:high, :]
        q = q_ref[rows, :]
        zero = jnp.zeros_like(q)
        outs, logs = [], []
        for own in (jnp.where(lane, q, zero), jnp.where(lane, zero, q)):
            s = jnp.where(mask, dot32(own, keys, NT) * scale, MASKED)
            top = jnp.max(s, axis=-1, keepdims=True)
            e = jnp.exp(s - top)
            tot = jnp.sum(e, axis=-1, keepdims=True)
            p = (e * (1.0 / tot)).astype(BF)
            outs.append(dot32(p, values, NN))
            logs.append(top + jnp.log(tot))
        mixed_ref[rows, :] = jnp.where(lane, outs[0], outs[1]).astype(BF)
        log_ref[rows, :] = jnp.where(lane, logs[0], logs[1])


def attend_back_kernel(
    scale, column, row, q_ref, k_ref, v_ref, log_ref, grad_ref, _, out_ref, bias_ref, dk, dv
):
    total = q_ref.shape[0]
    size = q_ref.shape[1] // 2
    lane = lax.broadcasted_iota(jnp.int32, (BLOCK, 2 * size), 1) < size
    dk[...] = jnp.zeros_like(dk)
    dv[...] = jnp.zeros_like(dv)
    dq_sum = jnp.zeros((1, 2 * size), F32)
    for i in range(total // BLOCK):
        low, high = key_range(i, total)
        rows = pl.ds(i * BLOCK, BLOCK)
        mask = allowed_mask(column, row, i, low, high)
        keys, values = k_ref[low:high, :], v_ref[low:high, :]
        q, g = q_ref[rows, :], grad_ref[rows, :]
        zero = jnp.zeros_like(q)
        dqs = []
        for h in range(2):
            qh = jnp.where(lane, q, zero) if h == 0 else jnp.where(lane, zero, q)
            gh = jnp.where(lane, g, zero) if h == 0 else jnp.where(lane, zero, g)
            log = log_ref[rows, h * size : h * size + 1]
            s = jnp.where(mask, dot32(qh, keys, NT) * scale, MASKED)
            p = jnp.exp(s - log)
            dp = dot32(gh, values, NT)
            delta = jnp.sum(p * dp, axis=-1, keepdims=True)
            ds = (p * (dp - delta)).astype(BF)
            dqs.append(dot32(ds, keys, NN))
            dk[low:high, :] += dot32(ds, qh, TN)
            dv[low:high, :] += dot32(p.astype(BF), gh, TN)
        dq = (jnp.where(lane, dqs[0], dqs[1]) * scale).astype(BF)
        out_ref[0, rows, :] = dq
        dq_sum += jnp.sum(dq.astype(F32), axis=0, keepdims=True)
    out_ref[1, :, :] = (dk[...] * scale).astype(BF)
    dvb = dv[...].astype(BF)
    out_ref[2, :, :] = dvb
    bias_ref[0:1, :] = dq_sum
    bias_ref[1:2, :] = jnp.sum(dvb.astype(F32), axis=0, keepdims=True)


def attend_specs(total, width):
    pick = lambda j: pl.BlockSpec((None, total, width), lambda h: (j, 0, h))
    return [
        pl.BlockSpec((total, 1), lambda h: (0, 0)),
        pl.BlockSpec((1, total), lambda h: (0, 0)),
        pick(0),
        pick(1),
        pick(2),
    ]


def attend(qkv, column, row, size, after):
    _, total, width = qkv.shape
    pair = 2 * size
    flat = pl.BlockSpec((total, pair), lambda h: (0, h))
    return call(
        partial(attend_kernel, 1.0 / math.sqrt(size)),
        [column, row, qkv, qkv, qkv, after],
        [shape((total, width)), shape((total, width), F32)],
        "attend",
        in_specs=attend_specs(total, pair) + [ANY],
        out_specs=[flat, flat],
        flops=total * total * width * 16,
        grid=(width // pair,),
    )


def attend_back(qkv, log, grad, column, row, size, after):
    _, total, width = qkv.shape
    pair = 2 * size
    flat = pl.BlockSpec((total, pair), lambda h: (0, h))
    return call(
        partial(attend_back_kernel, 1.0 / math.sqrt(size)),
        [column, row, qkv, qkv, qkv, log, grad, after],
        [shape((3, total, width)), shape((2, width), F32)],
        "attend_back",
        in_specs=attend_specs(total, pair) + [flat, flat, ANY],
        out_specs=[
            pl.BlockSpec((3, total, pair), lambda h: (0, 0, h)),
            pl.BlockSpec((2, pair), lambda h: (0, h)),
        ],
        scratch=[pltpu.VMEM((total, pair), F32)] * 2,
        flops=total * total * width * 24,
        grid=(width // pair,),
    )


def rows_kernel(dims, left, right, out):
    out[...] = dot32(left[...], right[...], dims).astype(out.dtype)


def rows_matmul(left, right, dims, name, kind=BF):
    total, depth = left.shape
    cols = right.shape[0] if dims is NT else right.shape[1]
    return call(
        partial(rows_kernel, dims),
        [left, right],
        [shape((total, cols), kind)],
        name,
        in_specs=[
            pl.BlockSpec((BLOCK, depth), lambda i: (i, 0)),
            pl.BlockSpec(right.shape, lambda i: (0, 0)),
        ],
        out_specs=[pl.BlockSpec((BLOCK, cols), lambda i: (i, 0))],
        flops=2 * total * depth * cols,
        grid=(total // BLOCK,),
    )[0]


def middle_kernel(x, part, got, bias, gain, shift, middle, second):
    value = x[...].astype(F32) + part[...].astype(F32) + got[...].astype(F32) + bias[...]
    middle[...] = value
    n, _ = moments(value)
    second[...] = (n * gain[...] + shift[...]).astype(BF)


def middle_norm(x, part, got, bias, gain, shift):
    total, width = x.shape
    rows = pl.BlockSpec((BLOCK, width), lambda i: (i, 0))
    line = pl.BlockSpec((1, width), lambda i: (0, 0))
    return call(
        middle_kernel,
        [x, part, got, bias, gain, shift],
        [shape((total, width), F32), shape((total, width))],
        "middle",
        in_specs=[rows] * 3 + [line] * 3,
        out_specs=[rows, rows],
        grid=(total // BLOCK,),
    )


def feed_kernel(second, cot, up, bias, down, hidden_ref, pre_ref, sum_ref):
    total = second.shape[0]
    root = math.sqrt(0.5)
    norm = 1.0 / math.sqrt(2.0 * math.pi)
    sums = jnp.zeros(sum_ref.shape, F32)
    for i in range(total // BLOCK):
        rows = pl.ds(i * BLOCK, BLOCK)
        v = dot32(second[rows, :], up[...], NN) + bias[...]
        g = dot32(cot[rows, :], down[...], NT)
        cdf = 0.5 * (1.0 + lax.erf(v * root))
        hidden_ref[rows, :] = (v * cdf).astype(BF)
        pre = (g * (cdf + v * (norm * jnp.exp(-0.5 * (v * v))))).astype(BF)
        pre_ref[rows, :] = pre
        sums += jnp.sum(pre.astype(F32), axis=0, keepdims=True)
    sum_ref[...] = sums


def feed_forward(second, cot, up, bias, down, tile=256):
    total, width = second.shape
    units = up.shape[1]
    whole = pl.BlockSpec((total, width), lambda u: (0, 0))
    cols = pl.BlockSpec((total, tile), lambda u: (0, u))
    line = pl.BlockSpec((1, tile), lambda u: (0, u))
    return call(
        feed_kernel,
        [second, cot, up, bias, down],
        [shape((total, units)), shape((total, units)), shape((1, units), F32)],
        "feed",
        in_specs=[
            whole,
            whole,
            pl.BlockSpec((width, tile), lambda u: (0, u)),
            line,
            pl.BlockSpec((tile, width), lambda u: (u, 0)),
        ],
        out_specs=[cols, cols, line],
        flops=4 * total * width * units,
        grid=(units // tile,),
    )


def down_grads_kernel(pos, hidden, cot, far1, far2, n1a, n1b, n2a, n2b, own):
    g = pl.program_id(0)
    rows = own.shape[1]
    acc = dot32(hidden[...], cot[...], TN).astype(BF)
    for k, outs in enumerate(((far1, far2), (n2a, n2b), (n1a, n1b), (own, own))):

        @pl.when(g == k)
        def _():
            for j in range(4):
                at = j if k == 3 else j % 2
                outs[j // 2][at] = acc[j * rows : (j + 1) * rows, :]


def ring_shapes(rows, cols):
    return [shape((2, rows, cols))] * 6 + [shape((4, rows, cols))]


def ring_specs(rows, cols):
    return [pl.BlockSpec((2, rows, cols), lambda g, pos: (0, 0, 0))] * 6 + [
        pl.BlockSpec((4, rows, cols), lambda g, pos: (0, 0, 0))
    ]


def down_grads(pos, hidden, cot, rows):
    total, units = hidden.shape
    width = cot.shape[1]
    return placed_call(
        down_grads_kernel,
        pos,
        [hidden, cot],
        ring_shapes(rows, width),
        "down_grads",
        (4,),
        [
            pl.BlockSpec((total, units // 4), lambda g, pos: (0, pos[0] ^ (3 - g))),
            pl.BlockSpec((total, width), lambda g, pos: (0, 0)),
        ],
        ring_specs(rows, width),
        flops=2 * total * units * width,
    )


def z_places(z):
    return lax.rem(z + 2, 4), lax.rem(z + 1, 4), lax.rem(z + 3, 4), z


def up_grads_kernel(pos, second, pre, far1, far2, n1a, n1b, n2a, n2b, own, acc):
    g = pl.program_id(0)
    lead = own.shape[1] // 2
    acc[...] = dot32(second[...], pre[...], TN).astype(BF)
    spots = z_places(pos[2])
    for half in range(2):

        @pl.when(g // 2 == half)
        def _():
            outs = ((far1, far2), (n1a, n1b), (n2a, n2b), (own, own))
            for k in range(4):
                at = g if k == 3 else lax.rem(g, 2)
                for cc in range(2):
                    start = pl.multiple_of(cc * 4 * lead + spots[k] * lead, lead)
                    outs[k][half][at, cc * lead : (cc + 1) * lead, :] = acc[pl.ds(start, lead), :]


def up_grads(pos, second, pre, lead):
    total, width = second.shape
    units = pre.shape[1]
    return placed_call(
        up_grads_kernel,
        pos,
        [second, pre],
        ring_shapes(2 * lead, units),
        "up_grads",
        (4,),
        [
            pl.BlockSpec((total, width // 4), lambda g, pos: (0, g)),
            pl.BlockSpec((total, units), lambda g, pos: (0, 0)),
        ],
        ring_specs(2 * lead, units),
        scratch=[pltpu.VMEM((width // 4, units), BF)],
        flops=2 * total * units * width,
    )


def attn_grads_kernel(pos, normed, grads, mixed, branch, *refs):
    p, q, (accv, acco) = refs[0:7], refs[7:14], refs[14:16]
    g = pl.program_id(0)
    yx = pos[0] ^ (3 - g)
    lead = accv.shape[0] // 8
    half = accv.shape[1]
    accq = dot32(normed[...], grads[0], TN).astype(BF)
    acck = dot32(normed[...], grads[1], TN).astype(BF)
    accv[...] = dot32(normed[...], grads[2], TN).astype(BF)
    acco[...] = dot32(mixed[...], branch[...], TN).astype(BF)
    far1, far2, n1a, n1b, n2a, n2b, own = p
    for k, outs in enumerate(((far1, far2), (n2a, n2b), (n1a, n1b), (own, own))):

        @pl.when(g == k)
        def _():
            for zz in range(4):
                at = zz if k == 3 else zz % 2
                for j, acc in enumerate((accq, acck)):
                    for cc in range(2):
                        row = (2 * j + cc) * lead
                        start = (cc * 4 + zz) * lead
                        outs[zz // 2][at, row : row + lead, :] = acc[start : start + lead, :]

    far1, far2, n1a, n1b, n2a, n2b, own = q
    spots = z_places(pos[2])
    for part in range(2):

        @pl.when(yx // 2 == part)
        def _():
            for k, outs in enumerate(((far1, far2), (n1a, n1b), (n2a, n2b), (own, own))):
                at = yx if k == 3 else lax.rem(yx, 2)
                out = outs[part]
                for cc in range(2):
                    start = pl.multiple_of(cc * 4 * lead + spots[k] * lead, lead)
                    out[at, cc * lead : (cc + 1) * lead, :] = accv[pl.ds(start, lead), :]
                    start = pl.multiple_of(spots[k] * lead, lead)
                    out[at, (2 + cc) * lead : (3 + cc) * lead, :] = acco[
                        pl.ds(start, lead), cc * half : (cc + 1) * half
                    ]


def attn_grads(pos, normed, grads, mixed, branch, lead):
    total, width = normed.shape
    half = width // 2
    return placed_call(
        attn_grads_kernel,
        pos,
        [normed, grads, mixed, branch],
        ring_shapes(4 * lead, half) * 2,
        "attn_grads",
        (4,),
        [
            pl.BlockSpec((total, width // 4), lambda g, pos: (0, pos[0] ^ (3 - g))),
            pl.BlockSpec((3, total, half), lambda g, pos: (0, 0, 0)),
            pl.BlockSpec((total, half // 4), lambda g, pos: (0, pos[0] ^ (3 - g))),
            pl.BlockSpec((total, width), lambda g, pos: (0, 0)),
        ],
        ring_specs(4 * lead, half) * 2,
        scratch=[pltpu.VMEM((width // 4, half), BF), pltpu.VMEM((half // 4, width), BF)],
        flops=8 * total * width * half,
    )


def add_kernel(n):
    def body(*refs):
        for a, b, out in zip(refs[:n], refs[n : 2 * n], refs[2 * n :]):
            out[...] = (a[...].astype(F32) + b[...].astype(F32)).astype(BF)

    return body


def outer_scatter(p, q, name):
    far1, far2, n1a, n1b, n2a, n2b, _ = p
    qfar1, qfar2, qn1a, qn1b, qn2a, qn2b, _ = q
    t1, t2 = send(far1, X_SWAP), send(far2, Y_SWAP)
    v1, v2 = send(qfar1, Z_UP), send(qfar2, Z_DOWN)
    p1a, p2b = send(n1a, X_SWAP), send(n2b, Y_SWAP)
    q1b, q2a = send(qn1b, Z_UP), send(qn2a, Z_DOWN)
    mine = [n1b, n2a, qn1a, qn2b]
    came = [t2, t1, v1, v2]
    m1, m2, w1, w2 = call(
        add_kernel(4), mine + came, [shape(a.shape) for a in mine], name + "_pass"
    )
    p1b, p2a = send(m1, X_SWAP), send(m2, Y_SWAP)
    q1a, q2b = send(w1, Z_UP), send(w2, Z_DOWN)
    return [p1a, p1b, p2a, p2b], [q1a, q1b, q2a, q2b], m1


def joined_kernel(extra):
    def body(*refs):
        o, c, z = place()
        ins = refs[: 10 + extra]
        outs, (ps, qs) = refs[10 + extra : 20 + extra], refs[20 + extra :]
        spots = {
            "z": z_places(z),
            "xy": (o ^ 3, o ^ 1, o ^ 2, o),
        }
        for n, (kind, acc) in enumerate((("z", ps), ("xy", qs))):
            own, r1a, r1b, r2a, r2b = ins[5 * n : 5 * n + 5]
            rows = own.shape[1]
            for j in range(4):
                r1, r2 = (r1a, r2a) if j < 2 else (r1b, r2b)
                acc[j, :rows, :] = (
                    own[j].astype(F32) + r1[j % 2].astype(F32) + r2[j % 2].astype(F32)
                )
                if n == 1 and extra:
                    acc[j, rows:, :] = sum(ref[j].astype(F32) for ref in ins[10:])
            far1, far2, first, second, mine = outs[5 * n : 5 * n + 5]
            far, one, two, me = spots[kind]
            cut = far1.shape[0]
            far1[...] = acc[far, :cut, :].astype(BF)
            far2[...] = acc[far, cut:, :].astype(BF)
            first[...] = acc[one].astype(BF)
            second[...] = acc[two].astype(BF)
            mine[...] = acc[me]

    return body


def inner_pass_kernel(p1, p2, q1, q2, t1, t2, v1, v2, p1o, p2o, q1o, q2o):
    def half(out, base, got, first):
        cut = base.shape[0] // 2 // 16 * 16
        low, high = base[:cut, :], base[cut:, :]
        plus = lambda a: (a.astype(F32) + got[...].astype(F32)).astype(BF)
        out[:cut, :] = plus(low) if first else low
        out[cut:, :] = high if first else plus(high)

    half(p1o, p1, t1, True)
    half(p2o, p2, t2, False)
    half(q1o, q1, v2, False)
    half(q2o, q2, v1, True)


def inner_scatter(p, q, p_got, q_got, extra, name):
    _, prows, pcols = p[6].shape
    _, qrows, qcols = q[6].shape
    qall = qrows + (extra[0].shape[1] if extra else 0)

    def outs(rows, cols):
        cut = rows // 2 // 16 * 16
        return [
            shape((cut, cols)),
            shape((rows - cut, cols)),
            shape((rows, cols)),
            shape((rows, cols)),
            shape((rows, cols), F32),
        ]

    pf1, pf2, p1, p2, pme, qf1, qf2, q1, q2, qme = call(
        joined_kernel(len(extra)),
        [p[6]] + p_got + [q[6]] + q_got + extra,
        outs(prows, pcols) + outs(qall, qcols),
        name + "_join",
        scratch=[pltpu.VMEM((4, prows, pcols), F32), pltpu.VMEM((4, qall, qcols), F32)],
    )
    t1, t2 = send(pf1, Z_UP), send(pf2, Z_DOWN)
    v1, v2 = send(qf1, X_SWAP), send(qf2, Y_SWAP)
    p1, p2, q1, q2 = call(
        inner_pass_kernel,
        [p1, p2, q1, q2, t1, t2, v1, v2],
        [shape(a.shape) for a in (p1, p2, q1, q2)],
        name + "_inner",
    )
    return (
        [pme, send(p1, Z_UP), send(p2, Z_DOWN)],
        [qme, send(q1, X_SWAP), send(q2, Y_SWAP)],
    )


def total_of(refs):
    return refs[0][...] + refs[1][...].astype(F32) + refs[2][...].astype(F32)


def feed_last_kernel(p0, p1, p2, q0, q1, q2, down, kept, given, acc):
    _, c, _ = place()
    down[...] = total_of((p0, p1, p2))
    acc[...] = total_of((q0, q1, q2))
    lead = kept.shape[0]
    kept[...] = acc[pl.ds(pl.multiple_of(c * lead, lead), lead), :]
    given[...] = acc[pl.ds(pl.multiple_of((1 - c) * lead, lead), lead), :]


def attn_last_kernel(p0, p1, p2, q0, q1, q2, kept, given, out, small, accp, accq):
    _, c, _ = place()
    accp[...] = total_of((p0, p1, p2))
    accq[...] = total_of((q0, q1, q2))
    lead = kept.shape[1]
    half = kept.shape[2]
    for j, (acc, at) in enumerate(((accp, 0), (accp, 2 * lead), (accq, 0))):
        kept[j] = acc[pl.ds(pl.multiple_of(at + c * lead, lead), lead), :]
        given[j] = acc[pl.ds(pl.multiple_of(at + (1 - c) * lead, lead), lead), :]
    out[:, :half] = accq[2 * lead : 3 * lead, :]
    out[:, half:] = accq[3 * lead : 4 * lead, :]
    small[...] = accq[4 * lead :, :]


def norm_back(n, spread, gain, grad):
    g = grad * gain
    return spread * (
        g - jnp.mean(g, axis=-1, keepdims=True) - n * jnp.mean(g * n, axis=-1, keepdims=True)
    )


def column(values):
    return jnp.sum(values, axis=0, keepdims=True)


def middle_back_kernel(part, got, middle, cot, gain, wout, branch, mgrad, mixed, sums):
    n, spread = moments(middle[...])
    grad = part[...].astype(F32) + got[...].astype(F32)
    c32 = cot[...].astype(F32)
    value = c32 + norm_back(n, spread, gain[...], grad)
    mgrad[...] = value
    rounded = value.astype(BF)
    branch[...] = rounded
    mixed[...] = dot32(rounded, wout[...], NT).astype(BF)

    @pl.when(pl.program_id(0) == 0)
    def _():
        sums[...] = jnp.zeros_like(sums)

    for j, v in enumerate((grad * n, grad, rounded.astype(F32), c32)):
        sums[j : j + 1, :] += column(v)


def middle_back(part, got, middle, cot, gain, wout):
    total, width = middle.shape
    half = wout.shape[0]
    rows = pl.BlockSpec((BLOCK, width), lambda i: (i, 0))
    fixed = lambda dims: pl.BlockSpec(dims, lambda i: (0, 0))
    return call(
        middle_back_kernel,
        [part, got, middle, cot, gain, wout],
        [
            shape((total, width)),
            shape((total, width), F32),
            shape((total, half)),
            shape((4, width), F32),
        ],
        "middle_back",
        in_specs=[rows] * 4 + [fixed((1, width)), fixed((half, width))],
        out_specs=[
            rows,
            rows,
            pl.BlockSpec((BLOCK, half), lambda i: (i, 0)),
            fixed((4, width)),
        ],
        flops=2 * total * width * half,
        grid=(total // BLOCK,),
    )


def source_grad_kernel(grads, weight, out):
    out[...] = sum(dot32(grads[j], weight[j], NT) for j in range(3)).astype(BF)


def source_grad(grads, weight):
    _, total, half = grads.shape
    width = weight.shape[1]
    return call(
        source_grad_kernel,
        [grads, weight],
        [shape((total, width))],
        "source_grad",
        in_specs=[
            pl.BlockSpec((3, BLOCK, half), lambda i: (0, i, 0)),
            pl.BlockSpec((3, width, half), lambda i: (0, 0, 0)),
        ],
        out_specs=[pl.BlockSpec((BLOCK, width), lambda i: (i, 0))],
        flops=6 * total * width * half,
        grid=(total // BLOCK,),
    )[0]


def own_block(g, pos):
    _, c, z = pos[0], pos[1], pos[2]
    parity = lax.rem(z, 2)
    return jnp.where(g < 2, 2 * c + (parity ^ (g & 1)), 2 * (1 - c) + (g & 1))


def input_back_kernel(pos, part, got, x, mgrad, gain, first, again, sums):
    g = pl.program_id(0)
    n, spread = moments(x[...].astype(F32))
    grad = part[...].astype(F32) + got[...].astype(F32)
    value = (mgrad[...] + norm_back(n, spread, gain[...], grad)).astype(BF)

    @pl.when(g == 0)
    def _():
        first[...] = value
        sums[...] = jnp.zeros_like(sums)

    @pl.when(g == 1)
    def _():
        again[...] = value

    for j, v in enumerate((grad * n, grad)):
        sums[j : j + 1, :] += column(v)


def input_back(pos, part, got, x, mgrad, gain):
    total, width = x.shape
    rows = pl.BlockSpec((BLOCK, width), lambda g, pos: (own_block(g, pos), 0))
    fixed = lambda n: pl.BlockSpec((n, width), lambda g, pos: (0, 0))
    return placed_call(
        input_back_kernel,
        pos,
        [part, got, x, mgrad, gain],
        [shape((BLOCK, width))] * 2 + [shape((2, width), F32)],
        "input_back",
        (total // BLOCK,),
        [rows] * 4 + [fixed(1)],
        [fixed(BLOCK), fixed(BLOCK), fixed(2)],
    )


def other_block(g, pos):
    return jnp.where(g < 2, 2 * (1 - pos[1]) + (g & 1), 2 * pos[1] + (g & 1))


def output_kernel(pos, hidden, down, middle, bias, theirs, mine):
    g = pl.program_id(0)
    value = dot32(hidden[...], down[...], NN)

    @pl.when(g < 2)
    def _():
        theirs[...] = value.astype(BF)

    @pl.when(g >= 2)
    def _():
        mine[...] = value + middle[...] + bias[...]


def output_rows(pos, hidden, down, middle, bias):
    total, units = hidden.shape
    width = down.shape[1]
    return placed_call(
        output_kernel,
        pos,
        [hidden, down, middle, bias],
        [shape((total // 2, width)), shape((total // 2, width), F32)],
        "output_rows",
        (4,),
        [
            pl.BlockSpec((BLOCK, units), lambda g, pos: (other_block(g, pos), 0)),
            pl.BlockSpec((units, width), lambda g, pos: (0, 0)),
            pl.BlockSpec((BLOCK, width), lambda g, pos: (other_block(g, pos), 0)),
            pl.BlockSpec((1, width), lambda g, pos: (0, 0)),
        ],
        [
            pl.BlockSpec((BLOCK, width), lambda g, pos: (jnp.minimum(g, 1), 0)),
            pl.BlockSpec((BLOCK, width), lambda g, pos: (jnp.maximum(g - 2, 0), 0)),
        ],
        flops=2 * total * units * width,
    )


def result_kernel(mine, got, first, again):
    _, _, z = place()
    parity = lax.rem(z, 2)
    for k, out in enumerate((first, again)):
        at = pl.multiple_of((parity ^ k) * BLOCK, BLOCK)
        out[...] = (mine[pl.ds(at, BLOCK), :] + got[pl.ds(at, BLOCK), :].astype(F32)).astype(BF)


Z_FAR = links(lambda o, c, z: (o, c, (z + 2) % 4))


def fast_local(
    inputs,
    segment_ids,
    first_gain,
    first_shift,
    query_weight,
    query_bias,
    key_weight,
    value_weight,
    value_bias,
    out_weight,
    out_bias,
    second_gain,
    second_shift,
    up_weight,
    up_bias,
    down_weight,
    down_bias,
    cotangent,
):
    batch, rows, width = inputs.shape
    o, c, z = place()
    pos = jnp.stack([o, c, z]).astype(jnp.int32)
    total = batch * rows * 2
    half = width // 2
    units = up_weight.shape[1] // 2
    lead = query_weight.shape[0]
    down_rows = down_weight.shape[0]
    size = width // H
    vector_list = [
        first_gain,
        first_shift,
        query_bias,
        value_bias,
        out_bias,
        second_gain,
        second_shift,
        down_bias,
        up_bias,
    ]
    count = 8 * lead + down_rows

    small, at = jnp.zeros((half,), BF), 0
    for vector in vector_list:
        small = small + jnp.pad(vector, (at, half - at - vector.shape[0]))
        at += vector.shape[0]
    small = jnp.pad(small.reshape(1, half), ((0, 7), (0, 0)))
    weights = [query_weight, key_weight, value_weight]
    far, up_far, in0, in1 = call(
        first_kernel,
        weights + [up_weight, small, inputs, segment_ids],
        [
            shape((3 * lead + 8, half)),
            shape((lead, units)),
            shape((rows + 16, width)),
            shape((rows + 16, width)),
        ],
        "first",
        in_specs=[VMEM] * 5 + [ANY, VMEM],
        scratch=[pltpu.SemaphoreType.DMA((2,))],
    )
    far_got, up_got = send(far, CORE_SWAP), send(up_far, CORE_SWAP)
    got = [send(in0, SEQUENCE[0]), send(in1, SEQUENCE[1])]
    attn_pay, up_pay = call(
        second_kernel,
        weights + [out_weight, up_weight, small, far_got, up_got],
        [shape((8 * lead + 16, half)), shape((2 * lead, units))],
        "second",
    )

    pa, pb = ring_first(attn_pay, Z_UP, Z_DOWN)
    qa, qb = ring_first(up_pay, X_SWAP, Y_SWAP)
    pc = ring_second(pa, pb, Z_UP, Z_DOWN)
    qc = ring_second(qa, qb, Y_SWAP, X_SWAP)
    attn_rows = 8 * lead + 16
    pl_low, pl_high, q_low, q_high = copies(
        [attn_pay, pa, pb, *pc, up_pay, qa, qb, *qc],
        [shape((2, attn_rows, half))] * 2 + [shape((2, 2 * lead, units))] * 2,
        inner_kernel_moves(2),
        10,
        "inner",
    )
    p_pieces = ring_outer(pl_low, pl_high, X_SWAP, Y_SWAP, Y_SWAP, X_SWAP)
    q_pieces = ring_outer(q_low, q_high, Z_UP, Z_DOWN, Z_UP, Z_DOWN)
    mate = [send(g, CORE_SWAP) for g in got]

    def attn_blocks(src, outs, yx, zz):
        todo = [
            (src.at[pl.ds(h * lead, lead)], outs[1].at[yx, zz, :, pl.ds(h * half, half)])
            for h in range(2)
        ]
        for j in range(3):
            for cc in range(2):
                first = (2 + 2 * j + cc) * lead
                todo.append((src.at[pl.ds(first, lead)], outs[0].at[j, yx, cc, zz]))
        todo.append((src.at[pl.ds(8 * lead, 16)], outs[2].at[yx, zz]))
        return todo

    def attn_moves(ins, outs):
        _, _, zz = place()
        parity = lax.rem(zz, 2)
        todo = final_moves(ins[:8], outs, "z", attn_blocks)
        todo += [(ins[8], outs[3])]
        todo += [(ins[9].at[parity], outs[4]), (ins[9].at[1 - parity], outs[5])]
        return todo

    wqkv, wout, small_all, down_own, cot0, cot1 = copies(
        p_pieces + [down_weight, cotangent],
        [
            shape((3, 4, 2, 4, lead, half)),
            shape((4, 4, lead, width)),
            shape((4, 4, 16, half)),
            shape(down_weight.shape),
            shape((rows, width)),
            shape((rows, width)),
        ],
        attn_moves,
        16 * 9 + 3,
        "attn_whole",
    )
    wqkv = wqkv.reshape(3, width, half)
    wout = wout.reshape(half, width)

    def up_blocks(src, outs, yx, zz):
        return [(src.at[pl.ds(cc * lead, lead)], outs[0].at[yx, cc, zz]) for cc in range(2)]

    wup = copies(
        q_pieces,
        [shape((4, 2, 4, lead, units))],
        lambda ins, outs: final_moves(ins, outs, "xy", up_blocks),
        32,
        "up_whole",
    )[0].reshape(width, units)

    def sequence_moves(ins, outs):
        _, cc, zz = place()
        parity = lax.rem(zz, 2)
        return [
            (ins[2 * m + k], outs[0].at[(1 - cc if m else cc), parity ^ k])
            for m in range(2)
            for k in range(2)
        ]

    def whole_sequence(pieces, name):
        return copies(pieces, [shape((2, 2) + pieces[0].shape)], sequence_moves, 4, name)[0]

    x_blocks = whole_sequence(got + mate, "inputs_whole")
    x = x_blocks[:, :, :rows].reshape(total, width)
    segments = x_blocks[:, :, rows, :rows].reshape(total).astype(F32)
    seg_col, seg_row = segments.reshape(total, 1), segments.reshape(1, total)

    da, db = ring_first(down_own, Z_UP, Z_DOWN)
    dc = ring_second(da, db, Z_UP, Z_DOWN)
    d_low, d_high = copies(
        [down_own, da, db, *dc],
        [shape((2, down_rows, width))] * 2,
        inner_kernel_moves(1),
        5,
        "down_inner",
    )
    d_pieces = ring_outer(d_low, d_high, X_SWAP, Y_SWAP, Y_SWAP, X_SWAP)
    cot_got = [send(cot0, SEQUENCE[0]), send(cot1, SEQUENCE[1])]
    cot_mate = [send(g, CORE_SWAP) for g in cot_got]
    wdown = copies(
        d_pieces,
        [shape((4, 4, down_rows, width))],
        lambda ins, outs: final_moves(
            ins, outs, "z", lambda src, outs, yx, zz: [(src, outs[0].at[yx, zz])]
        ),
        16,
        "down_whole",
    )[0].reshape(units, width)
    cot = whole_sequence(cot_got + cot_mate, "cotangent_whole").reshape(total, width)

    small_all = small_all.reshape(4, 4, 2, 8, half)[:, :, :, 0, :count]
    vectors = small_all[..., : 8 * lead].reshape(4, 4, 2, 8, lead).transpose(3, 0, 2, 1, 4)
    own_cols = lax.dynamic_index_in_dim(vectors, c, 2, keepdims=False).reshape(8, half)
    vectors = vectors.reshape(8, width).astype(F32)
    line = lambda j: vectors[j : j + 1]
    gain1, shift1, bias_o, gain2, shift2, bias_d = [line(j) for j in (0, 1, 4, 5, 6, 7)]
    qkv_bias = jnp.stack([own_cols[2], jnp.zeros_like(own_cols[2]), own_cols[3]]).astype(F32)
    bias_u = lax.dynamic_index_in_dim(small_all[..., 8 * lead :], c, 2, keepdims=False)
    bias_u = bias_u.reshape(1, units).astype(F32)

    normed, qkv = project(x, gain1, shift1, wqkv, qkv_bias)
    mixed, log = attend(qkv, seg_col, seg_row, size, d_low)
    part = rows_matmul(mixed, wout, NN, "attend_out")
    middle, second = middle_norm(x, part, send(part, CORE_SWAP), bias_o, gain2, shift2)
    hidden, pre_grad, up_bias_grad = feed_forward(second, cot, wup, bias_u, wdown)

    part = rows_matmul(pre_grad, wup, NT, "second_grad")
    got = send(part, CORE_SWAP)
    p = down_grads(pos, hidden, cot, down_rows)
    q = up_grads(pos, second, pre_grad, lead)
    p_got, q_got, passed = outer_scatter(p, q, "feed")
    branch, middle_grad, mixed_grad, sums2 = middle_back(part, got, middle, cot, gain2, wout)

    grads, qv_bias_grad = attend_back(qkv, log, mixed_grad, seg_col, seg_row, size, passed)
    p_last, q_last = inner_scatter(p, q, p_got, q_got, [], "feed")
    down_out, up_kept, up_given = call(
        feed_last_kernel,
        p_last + q_last,
        [shape(p_last[0].shape, F32)] + [shape((lead, units), F32)] * 2,
        "feed_last",
        scratch=[pltpu.VMEM((2 * lead, units), F32)],
    )
    up_got = send(up_given, CORE_SWAP)

    part = source_grad(grads, wqkv)
    got = send(part, CORE_SWAP)
    pq = attn_grads(pos, normed, grads, mixed, branch, lead)
    p, q = pq[:7], pq[7:]
    p_got, q_got, _ = outer_scatter(p, q, "attn")

    theirs, mine = output_rows(pos, hidden, wdown, middle, bias_d)
    blocks = call(
        result_kernel, [mine, send(theirs, CORE_SWAP)], [shape((rows, width))] * 2, "result"
    )

    def to_tokens(blocks):
        got = [send(block, pairs) for block, pairs in zip(blocks, SEQUENCE)]
        return jnp.where((z & 1) == 0, jnp.stack(got), jnp.stack(got[::-1]))

    output = to_tokens(blocks)
    in0, in1, sums1 = input_back(pos, part, got, x, middle_grad, gain1)
    input_grad = to_tokens([in0, in1]).astype(F32)

    wide = jnp.stack([sums1[0], sums1[1], sums2[2], sums2[0], sums2[1], sums2[3]])
    wide = lax.dynamic_index_in_dim(wide.reshape(6, 4, 2, 4, lead), c, 2, keepdims=False)
    wide = jnp.concatenate(
        [wide[:2], qv_bias_grad.reshape(2, 4, 4, lead), wide[2:]], axis=0
    ).transpose(2, 1, 0, 3)
    tiny = jnp.concatenate(
        [
            wide.reshape(4, 4, 8 * lead),
            up_bias_grad.reshape(4, 4, down_rows).transpose(1, 0, 2),
        ],
        axis=-1,
    ).astype(BF)
    tiny = jnp.pad(tiny[:, :, None], ((0, 0), (0, 0), (0, 15), (0, half - count)))
    pick = lambda k: lax.dynamic_index_in_dim(tiny, (z + k) % 4, 0, keepdims=False)
    extra = [pick(0), send(pick(1), Z_UP), send(pick(3), Z_DOWN), send(pick(2), Z_FAR)]

    p_last, q_last = inner_scatter(p, q, p_got, q_got, extra, "attn")
    qkv_kept, qkv_given, out_out, small_sum = call(
        attn_last_kernel,
        p_last + q_last,
        [shape((3, lead, half), F32)] * 2 + [shape((lead, width), F32), shape((16, half), F32)],
        "attn_last",
        scratch=[
            pltpu.VMEM((4 * lead, half), F32),
            pltpu.VMEM((4 * lead + 16, half), F32),
        ],
    )

    def whole_columns(kept, got):
        cols = kept.shape[-1] // 4
        kept, got = [a.reshape(a.shape[:-1] + (4, 1, cols)) for a in (kept, got)]
        both = jnp.where(
            c == 0, jnp.concatenate([kept, got], -2), jnp.concatenate([got, kept], -2)
        )
        return both.reshape(both.shape[:-3] + (8 * cols,))

    up_out = whole_columns(up_kept, up_got)
    qkv_out = whole_columns(qkv_kept, send(qkv_given, CORE_SWAP))
    small_sum = small_sum[0]
    vec = lambda j: small_sum[j * lead : (j + 1) * lead]
    return (
        output,
        input_grad,
        vec(0),
        vec(1),
        qkv_out[0],
        vec(2),
        qkv_out[1],
        qkv_out[2],
        vec(3),
        out_out,
        vec(4),
        vec(5),
        vec(6),
        up_out,
        small_sum[8 * lead : count],
        down_out,
        vec(7),
    )


def solution(mesh):
    fast = mesh.shape["dp"] == 8 and mesh.shape["ctx"] == 4
    return jax.shard_map(
        fast_local if fast else local,
        mesh=mesh,
        in_specs=(
            P("dp", "ctx", None),
            P("dp", "ctx"),
            P(("dp", "ctx")),
            P(("dp", "ctx")),
            P(("dp", "ctx"), None),
            P(("dp", "ctx")),
            P(("dp", "ctx"), None),
            P(("dp", "ctx"), None),
            P(("dp", "ctx")),
            P(("dp", "ctx"), None),
            P(("dp", "ctx")),
            P(("dp", "ctx")),
            P(("dp", "ctx")),
            P(("dp", "ctx"), None),
            P(("dp", "ctx")),
            P(("dp", "ctx"), None),
            P(("dp", "ctx")),
            P("dp", "ctx", None),
        ),
        out_specs=(
            P("dp", "ctx", None),
            P("dp", "ctx", None),
            P(("dp", "ctx")),
            P(("dp", "ctx")),
            P(("dp", "ctx"), None),
            P(("dp", "ctx")),
            P(("dp", "ctx"), None),
            P(("dp", "ctx"), None),
            P(("dp", "ctx")),
            P(("dp", "ctx"), None),
            P(("dp", "ctx")),
            P(("dp", "ctx")),
            P(("dp", "ctx")),
            P(("dp", "ctx"), None),
            P(("dp", "ctx")),
            P(("dp", "ctx"), None),
            P(("dp", "ctx")),
        ),
        check_vma=False,
    )
```

```python
from functools import partial
import math

import jax
import jax.numpy as jnp
from jax import lax
from jax.experimental import pallas as pl
from jax.experimental.pallas import tpu as pltpu
from jax.sharding import PartitionSpec as P

H = 16


EPS = 1e-05
MASKED = -1e30


def normalize(values, gain, shift):
    mean = jnp.mean(values, axis=-1, keepdims=True)
    centered = values - mean
    spread = jnp.mean(centered * centered, axis=-1, keepdims=True)
    return centered * lax.rsqrt(spread + EPS) * gain + shift


def product(left, right):
    return jnp.einsum("btd,de->bte", left, right, preferred_element_type=jnp.float32)


def product_back(left, right):
    return jnp.einsum("bte,de->btd", left, right, preferred_element_type=jnp.float32)


def outer_sum(left, right):
    return jnp.einsum("btd,bte->de", left, right, preferred_element_type=jnp.float32)


def column_sum(values):
    return jnp.sum(values.astype(jnp.float32), axis=(0, 1))


def gather_attention(
    first_gain,
    first_shift,
    query_weight,
    query_bias,
    key_weight,
    value_weight,
    value_bias,
    out_weight,
    out_bias,
):
    return (
        lax.all_gather(first_gain, ("dp", "ctx"), axis=0, tiled=True),
        lax.all_gather(first_shift, ("dp", "ctx"), axis=0, tiled=True),
        lax.all_gather(query_weight, ("dp", "ctx"), axis=0, tiled=True),
        lax.all_gather(query_bias, ("dp", "ctx"), axis=0, tiled=True),
        lax.all_gather(key_weight, ("dp", "ctx"), axis=0, tiled=True),
        lax.all_gather(value_weight, ("dp", "ctx"), axis=0, tiled=True),
        lax.all_gather(value_bias, ("dp", "ctx"), axis=0, tiled=True),
        lax.all_gather(out_weight, ("dp", "ctx"), axis=0, tiled=True),
        lax.all_gather(out_bias, ("dp", "ctx"), axis=0, tiled=True),
    )


def gather_feed(second_gain, second_shift, up_weight, up_bias, down_weight, down_bias):
    return (
        lax.all_gather(second_gain, ("dp", "ctx"), axis=0, tiled=True),
        lax.all_gather(second_shift, ("dp", "ctx"), axis=0, tiled=True),
        lax.all_gather(up_weight, ("dp", "ctx"), axis=0, tiled=True),
        lax.all_gather(up_bias, ("dp", "ctx"), axis=0, tiled=True),
        lax.all_gather(down_weight, ("dp", "ctx"), axis=0, tiled=True),
        lax.all_gather(down_bias, ("dp", "ctx"), axis=0, tiled=True),
    )


def gather_keys(keys, values, segments):
    return (
        lax.all_gather(keys, "ctx", axis=1, tiled=True),
        lax.all_gather(values, "ctx", axis=1, tiled=True),
        lax.all_gather(segments, "ctx", axis=1, tiled=True),
    )


def score_block(queries, keys_all, segments, segments_all):
    batch, rows, width = queries.shape
    size = width // H
    total_len = keys_all.shape[1]
    query_heads = queries.reshape(batch, rows, H, size)
    key_heads = keys_all.reshape(batch, total_len, H, size)
    raw = jnp.einsum("bqhd,bkhd->bhqk", query_heads, key_heads, preferred_element_type=jnp.float32)
    scores = raw * (1.0 / math.sqrt(size))
    offset = lax.axis_index("ctx") * rows
    query_pos = offset + jnp.arange(rows, dtype=jnp.int32)
    key_pos = jnp.arange(total_len, dtype=jnp.int32)
    causal = key_pos[None, :] <= query_pos[:, None]
    same_doc = segments[:, :, None] == segments_all[:, None, :]
    allowed = (causal[None] & same_doc)[:, None]
    return jnp.where(allowed, scores, MASKED)


def forward_part(inputs, segments, attn, feed):
    (
        first_gain,
        first_shift,
        query_weight,
        query_bias,
        key_weight,
        value_weight,
        value_bias,
        out_weight,
        out_bias,
    ) = attn
    second_gain, second_shift, up_weight, up_bias, down_weight, down_bias = feed
    batch, rows, width = inputs.shape
    size = width // H
    source = inputs.astype(jnp.float32)
    normed = normalize(
        source, first_gain.astype(jnp.float32), first_shift.astype(jnp.float32)
    ).astype(jnp.bfloat16)
    queries = (product(normed, query_weight) + query_bias.astype(jnp.float32)).astype(jnp.bfloat16)
    keys = product(normed, key_weight).astype(jnp.bfloat16)
    values = (product(normed, value_weight) + value_bias.astype(jnp.float32)).astype(jnp.bfloat16)
    keys_all, values_all, segments_all = gather_keys(keys, values, segments)
    scores = score_block(queries, keys_all, segments, segments_all)
    top = jnp.max(scores, axis=-1, keepdims=True)
    expo = jnp.exp(scores - top)
    row_total = jnp.sum(expo, axis=-1, keepdims=True)
    probs = (expo / row_total).astype(jnp.bfloat16)
    log_total = top + jnp.log(row_total)
    value_heads = values_all.reshape(batch, values_all.shape[1], H, size)
    mixed = jnp.einsum("bhqk,bkhd->bqhd", probs, value_heads, preferred_element_type=jnp.float32)
    mixed = mixed.reshape(batch, rows, width).astype(jnp.bfloat16)
    middle = source + product(mixed, out_weight) + out_bias.astype(jnp.float32)
    second = normalize(
        middle, second_gain.astype(jnp.float32), second_shift.astype(jnp.float32)
    ).astype(jnp.bfloat16)
    hidden_pre = product(second, up_weight) + up_bias.astype(jnp.float32)
    hidden = jax.nn.gelu(hidden_pre, approximate=False).astype(jnp.bfloat16)
    output = (middle + product(hidden, down_weight) + down_bias.astype(jnp.float32)).astype(
        jnp.bfloat16
    )
    kept = (
        source,
        normed,
        queries,
        keys,
        values,
        log_total,
        mixed,
        middle,
        second,
        hidden_pre,
        hidden,
    )
    return (output, kept, (keys_all, values_all, segments_all))


def backward_part(kept, gathered, segments, cotangent, attn, feed):
    (
        first_gain,
        first_shift,
        query_weight,
        query_bias,
        key_weight,
        value_weight,
        value_bias,
        out_weight,
        out_bias,
    ) = attn
    second_gain, second_shift, up_weight, up_bias, down_weight, down_bias = feed
    source, normed, queries, keys, values, log_total, mixed, middle, second, hidden_pre, hidden = (
        kept
    )
    keys_all, values_all, segments_all = gathered
    batch, rows, width = source.shape
    size = width // H
    total_len = keys_all.shape[1]
    scale = 1.0 / math.sqrt(size)
    down_grad = outer_sum(hidden, cotangent)
    down_bias_grad = column_sum(cotangent)
    hidden_grad = product_back(cotangent, down_weight)
    _, gelu_back = jax.vjp(partial(jax.nn.gelu, approximate=False), hidden_pre)
    pre_grad = gelu_back(hidden_grad)[0].astype(jnp.bfloat16)
    up_grad = outer_sum(second, pre_grad)
    up_bias_grad = column_sum(pre_grad)
    second_grad = product_back(pre_grad, up_weight)
    _, second_back = jax.vjp(
        normalize, middle, second_gain.astype(jnp.float32), second_shift.astype(jnp.float32)
    )
    middle_part, second_gain_grad, second_shift_grad = second_back(second_grad)
    feed_grads = (
        lax.psum_scatter(second_gain_grad, ("dp", "ctx"), scatter_dimension=0, tiled=True),
        lax.psum_scatter(second_shift_grad, ("dp", "ctx"), scatter_dimension=0, tiled=True),
        lax.psum_scatter(up_grad, ("dp", "ctx"), scatter_dimension=0, tiled=True),
        lax.psum_scatter(up_bias_grad, ("dp", "ctx"), scatter_dimension=0, tiled=True),
        lax.psum_scatter(down_grad, ("dp", "ctx"), scatter_dimension=0, tiled=True),
        lax.psum_scatter(down_bias_grad, ("dp", "ctx"), scatter_dimension=0, tiled=True),
    )
    middle_grad = cotangent.astype(jnp.float32) + middle_part
    branch_grad = middle_grad.astype(jnp.bfloat16)
    out_grad = outer_sum(mixed, branch_grad)
    out_bias_grad = column_sum(branch_grad)
    mixed_grad = product_back(branch_grad, out_weight).astype(jnp.bfloat16)
    scores = score_block(queries, keys_all, segments, segments_all)
    probs_full = jnp.exp(scores - log_total)
    probs = probs_full.astype(jnp.bfloat16)
    grad_heads = mixed_grad.reshape(batch, rows, H, size)
    query_heads = queries.reshape(batch, rows, H, size)
    key_heads = keys_all.reshape(batch, total_len, H, size)
    value_heads = values_all.reshape(batch, total_len, H, size)
    value_grad_all = jnp.einsum(
        "bhqk,bqhd->bkhd", probs, grad_heads, preferred_element_type=jnp.float32
    )
    prob_grad = jnp.einsum(
        "bqhd,bkhd->bhqk", grad_heads, value_heads, preferred_element_type=jnp.float32
    )
    delta = jnp.sum(probs_full * prob_grad, axis=-1, keepdims=True)
    score_grad = (probs_full * (prob_grad - delta)).astype(jnp.bfloat16)
    query_grad = (
        jnp.einsum("bhqk,bkhd->bqhd", score_grad, key_heads, preferred_element_type=jnp.float32)
        * scale
    )
    query_grad = query_grad.reshape(batch, rows, width).astype(jnp.bfloat16)
    key_grad_all = (
        jnp.einsum("bhqk,bqhd->bkhd", score_grad, query_heads, preferred_element_type=jnp.float32)
        * scale
    )
    key_sum, value_sum = (
        lax.psum_scatter(
            key_grad_all.reshape(batch, total_len, width).astype(jnp.bfloat16),
            "ctx",
            scatter_dimension=1,
            tiled=True,
        ).astype(jnp.float32),
        lax.psum_scatter(
            value_grad_all.reshape(batch, total_len, width).astype(jnp.bfloat16),
            "ctx",
            scatter_dimension=1,
            tiled=True,
        ).astype(jnp.float32),
    )
    key_grad = key_sum.astype(jnp.bfloat16)
    value_grad = value_sum.astype(jnp.bfloat16)
    query_weight_grad = outer_sum(normed, query_grad)
    query_bias_grad = column_sum(query_grad)
    key_weight_grad = outer_sum(normed, key_grad)
    value_weight_grad = outer_sum(normed, value_grad)
    value_bias_grad = column_sum(value_grad)
    normed_grad = (
        product_back(query_grad, query_weight)
        + product_back(key_grad, key_weight)
        + product_back(value_grad, value_weight)
    )
    _, first_back = jax.vjp(
        normalize, source, first_gain.astype(jnp.float32), first_shift.astype(jnp.float32)
    )
    input_part, first_gain_grad, first_shift_grad = first_back(normed_grad)
    input_grad = middle_grad + input_part
    attn_grads = (
        lax.psum_scatter(first_gain_grad, ("dp", "ctx"), scatter_dimension=0, tiled=True),
        lax.psum_scatter(first_shift_grad, ("dp", "ctx"), scatter_dimension=0, tiled=True),
        lax.psum_scatter(query_weight_grad, ("dp", "ctx"), scatter_dimension=0, tiled=True),
        lax.psum_scatter(query_bias_grad, ("dp", "ctx"), scatter_dimension=0, tiled=True),
        lax.psum_scatter(key_weight_grad, ("dp", "ctx"), scatter_dimension=0, tiled=True),
        lax.psum_scatter(value_weight_grad, ("dp", "ctx"), scatter_dimension=0, tiled=True),
        lax.psum_scatter(value_bias_grad, ("dp", "ctx"), scatter_dimension=0, tiled=True),
        lax.psum_scatter(out_grad, ("dp", "ctx"), scatter_dimension=0, tiled=True),
        lax.psum_scatter(out_bias_grad, ("dp", "ctx"), scatter_dimension=0, tiled=True),
    )
    return (input_grad, attn_grads, feed_grads)


def local(
    inputs,
    segment_ids,
    first_gain,
    first_shift,
    query_weight,
    query_bias,
    key_weight,
    value_weight,
    value_bias,
    out_weight,
    out_bias,
    second_gain,
    second_shift,
    up_weight,
    up_bias,
    down_weight,
    down_bias,
    cotangent,
):
    attn = gather_attention(
        first_gain,
        first_shift,
        query_weight,
        query_bias,
        key_weight,
        value_weight,
        value_bias,
        out_weight,
        out_bias,
    )
    feed = gather_feed(second_gain, second_shift, up_weight, up_bias, down_weight, down_bias)
    output, kept, gathered = forward_part(inputs, segment_ids, attn, feed)
    key_set = gather_keys(kept[3], kept[4], segment_ids)
    input_grad, attn_grads, feed_grads = backward_part(
        kept, key_set, segment_ids, cotangent, attn, feed
    )
    result = (output, input_grad)
    return result + tuple(attn_grads) + tuple(feed_grads)


AXES = ("dp", "ctx")
BLOCK = 256
BF = jnp.bfloat16
F32 = jnp.float32
NT = (((1,), (1,)), ((), ()))
NN = (((1,), (0,)), ((), ()))
TN = (((0,), (0,)), ((), ()))
ANY = pl.BlockSpec(memory_space=pl.ANY)
VMEM = pl.BlockSpec(memory_space=pltpu.VMEM)


def links(step):
    pairs = []
    for o in range(4):
        for c in range(2):
            for z in range(4):
                o2, c2, z2 = step(o, c, z)
                pairs.append(((o * 2 + c) * 4 + z, (o2 * 2 + c2) * 4 + z2))
    return pairs


X_SWAP = links(lambda o, c, z: (o ^ 1, c, z))
Y_SWAP = links(lambda o, c, z: (o ^ 2, c, z))
CORE_SWAP = links(lambda o, c, z: (o, 1 - c, z))
Z_UP = links(lambda o, c, z: (o, c, (z + 1) % 4))
Z_DOWN = links(lambda o, c, z: (o, c, (z + 3) % 4))
SEQUENCE = [links(lambda o, c, z, k=k: (o, z >> 1, 2 * c + ((z & 1) ^ k))) for k in range(2)]


def send(value, pairs):
    return lax.ppermute(value, AXES, pairs)


def place():
    dp = lax.axis_index("dp")
    return dp // 2, dp % 2, lax.axis_index("ctx")


def dot32(left, right, dims):
    return lax.dot_general(left, right, dims, preferred_element_type=F32)


def shape(dims, kind=BF):
    return jax.ShapeDtypeStruct(dims, kind)


def cost(flops, nbytes, special=0):
    return pl.CostEstimate(flops=int(flops), bytes_accessed=int(nbytes), transcendentals=special)


def moved_bytes(arrays):
    return sum(math.prod(a.shape) * jnp.dtype(a.dtype).itemsize for a in arrays)


def without(body, lead, count):
    return (lambda *refs: body(*refs[:lead], *refs[lead + count :])) if count else body


def call(
    body,
    ins,
    outs,
    name,
    in_specs=None,
    out_specs=None,
    scratch=(),
    flops=0,
    grid=(),
    after=(),
    aliases={},
):
    return pl.pallas_call(
        without(body, len(ins), len(after)),
        grid=grid,
        in_specs=list(in_specs or [VMEM] * len(ins)) + [ANY] * len(after),
        out_specs=out_specs or [VMEM] * len(outs),
        out_shape=outs,
        scratch_shapes=list(scratch),
        cost_estimate=cost(flops, moved_bytes(ins) + moved_bytes(outs)),
        input_output_aliases=aliases,
        name=name,
    )(*ins, *after)


def placed_call(
    body, pos, ins, outs, name, grid, in_specs, out_specs, scratch=(), flops=0, after=()
):
    return pl.pallas_call(
        without(body, len(ins) + 1, len(after)),
        grid_spec=pltpu.PrefetchScalarGridSpec(
            num_scalar_prefetch=1,
            grid=grid,
            in_specs=list(in_specs) + [ANY] * len(after),
            out_specs=out_specs,
            scratch_shapes=list(scratch),
        ),
        out_shape=outs,
        cost_estimate=cost(flops, moved_bytes(ins) + moved_bytes(outs)),
        name=name,
    )(pos, *ins, *after)


def copies(ins, outs, moves, count, name, after=()):
    def body(*refs):
        sems = refs[-1]
        todo = moves(refs[: len(ins)], refs[len(ins) : -1])
        started = [pltpu.make_async_copy(s, d, sems.at[i]) for i, (s, d) in enumerate(todo)]
        for copy in started:
            copy.start()
        for copy in started:
            copy.wait()

    return call(
        body,
        ins,
        outs,
        name,
        in_specs=[ANY] * len(ins),
        scratch=[pltpu.SemaphoreType.DMA((count,))],
        after=after,
    )


def own_columns(weight, k):
    n = weight.shape[1] // 8
    parts = [
        jnp.where(k == 0, weight[:, 2 * g * n : (2 * g + 1) * n], weight[:, (2 * g + 1) * n : (2 * g + 2) * n])
        for g in range(4)
    ]
    return jnp.concatenate(parts, axis=1)


def first_kernel(qw, kw, vw, uw, small, far, up_far):
    _, c, _ = place()
    lead = qw.shape[0]
    for j, ref in enumerate((qw, kw, vw)):
        far[j * lead : (j + 1) * lead, :] = own_columns(ref[...], 1 - c)
    far[3 * lead :, :] = small[...]
    up_far[...] = own_columns(uw[...], 1 - c)


def inputs_kernel(inputs, segs, in0, in1, sems):
    rows = inputs.shape[1]
    parity = lax.rem(place()[2], 2)
    todo = []
    for k, out in enumerate((in0, in1)):
        pick = parity if k == 0 else 1 - parity
        todo.append(pltpu.make_async_copy(inputs.at[pick], out.at[pl.ds(0, rows)], sems.at[k]))
        todo[-1].start()
        line = segs[pl.ds(pick, 1), :].astype(F32)
        out[rows:, :] = jnp.zeros((out.shape[0] - rows, out.shape[1]), BF)
        out[rows:, :rows] = jnp.broadcast_to(line, (out.shape[0] - rows, rows)).astype(BF)
    for copy in todo:
        copy.wait()


def second_kernel(qw, kw, vw, uw, small, far, up_far, attn, up):
    _, c, _ = place()
    lead = qw.shape[0]

    def both(out, at, own, got):
        n = own.shape[0]
        out[at : at + n, :] = jnp.where(c == 0, own, got)
        out[at + n : at + 2 * n, :] = jnp.where(c == 0, got, own)

    for j, ref in enumerate((qw, kw, vw)):
        both(attn, 2 * j * lead, own_columns(ref[...], c), far[j * lead : (j + 1) * lead, :])
    both(attn, 6 * lead, small[...], far[3 * lead :, :])
    both(up, 0, own_columns(uw[...], c), up_far[...])


def inner_moves(ins, outs):
    own, first, second, far1, far2 = ins[:5]
    cut = far1.shape[0]
    return [
        (own, outs[0].at[0]),
        (first, outs[0].at[1]),
        (second, outs[0].at[2]),
        (far1, outs[0].at[3, pl.ds(0, cut)]),
        (far2, outs[0].at[3, pl.ds(cut, far2.shape[0])]),
    ]


def ring_first(value, n1, n2):
    return send(value, n1), send(value, n2)


def ring_second(a, b, f1, f2):
    cut = a.shape[0] // 2 // 16 * 16
    return send(a[:cut], f1), send(b[cut:], f2)


def ring_outer_second(a, b, f1, f2):
    return send(a[:2], f1), send(b[2:], f2)


def final_moves(ins, outs, blocks):
    o, _, z = place()
    z_ring = (z, lax.rem(z + 3, 4), lax.rem(z + 1, 4), lax.rem(z + 2, 4))
    yx_ring = (o, o ^ 1, o ^ 2, o ^ 3)
    todo = []
    for k in range(4):
        for j in range(4):
            source = ins[k].at[j] if k < 3 else ins[3 + j // 2].at[j % 2]
            todo += blocks(source, outs, yx_ring[k], z_ring[j])
    return todo


def moments(values):
    mean = jnp.mean(values, axis=-1, keepdims=True)
    centered = values - mean
    spread = lax.rsqrt(jnp.mean(centered * centered, axis=-1, keepdims=True) + EPS)
    return centered * spread, spread


def project_kernel(x, gain, shift, weight, bias, normed, qkv):
    n, _ = moments(x[...].astype(F32))
    value = (n * gain[...] + shift[...]).astype(BF)
    normed[...] = value
    for j in range(3):
        qkv[j] = (dot32(value, weight[j], NN) + bias[j : j + 1, :]).astype(BF)


def project(x, gain, shift, weight, bias, after):
    total, width = x.shape
    half = weight.shape[2]
    rows = pl.BlockSpec((BLOCK, width), lambda i: (i, 0))
    line = pl.BlockSpec((1, width), lambda i: (0, 0))
    return call(
        project_kernel,
        [x, gain, shift, weight, bias],
        [shape((total, width)), shape((3, total, half))],
        "project",
        in_specs=[
            rows,
            line,
            line,
            pl.BlockSpec((3, width, half), lambda i: (0, 0, 0)),
            pl.BlockSpec((3, half), lambda i: (0, 0)),
        ],
        out_specs=[rows, pl.BlockSpec((3, BLOCK, half), lambda i: (0, i, 0))],
        flops=6 * total * width * half,
        grid=(total // BLOCK,),
        after=after,
    )


def allowed_mask(column, row, i, low, high):
    rows = i * BLOCK + lax.broadcasted_iota(jnp.int32, (BLOCK, high - low), 0)
    cols = low + lax.broadcasted_iota(jnp.int32, (BLOCK, high - low), 1)
    same = column[i * BLOCK : i * BLOCK + BLOCK, :] == row[:, low:high]
    return same & (cols <= rows)


def key_range(i, total):
    return max(0, (i * BLOCK - total // 2 + 1) // BLOCK * BLOCK), (i + 1) * BLOCK


def attend_kernel(scale, column, row, q_ref, k_ref, v_ref, *refs):
    mixed_ref, log_ref = refs[-2:]
    total = q_ref.shape[0]
    size = q_ref.shape[1] // 2
    lane = lax.broadcasted_iota(jnp.int32, (BLOCK, 2 * size), 1) < size
    for i in range(total // BLOCK):
        low, high = key_range(i, total)
        rows = pl.ds(i * BLOCK, BLOCK)
        mask = allowed_mask(column, row, i, low, high)
        keys, values = k_ref[low:high, :], v_ref[low:high, :]
        q = q_ref[rows, :]
        zero = jnp.zeros_like(q)
        outs, logs = [], []
        for own in (jnp.where(lane, q, zero), jnp.where(lane, zero, q)):
            s = jnp.where(mask, dot32(own, keys, NT) * scale, MASKED)
            top = jnp.max(s, axis=-1, keepdims=True)
            e = jnp.exp(s - top)
            tot = jnp.sum(e, axis=-1, keepdims=True)
            p = (e * (1.0 / tot)).astype(BF)
            outs.append(dot32(p, values, NN))
            logs.append(top + jnp.log(tot))
        mixed_ref[rows, :] = jnp.where(lane, outs[0], outs[1]).astype(BF)
        log_ref[rows, :] = jnp.where(lane, logs[0], logs[1])


def attend_back_kernel(
    scale, column, row, q_ref, k_ref, v_ref, log_ref, grad_ref, *refs
):
    out_ref, bias_ref, dk, dv = refs[-4:]
    total = q_ref.shape[0]
    size = q_ref.shape[1] // 2
    lane = lax.broadcasted_iota(jnp.int32, (BLOCK, 2 * size), 1) < size
    dk[...] = jnp.zeros_like(dk)
    dv[...] = jnp.zeros_like(dv)
    dq_sum = jnp.zeros((1, 2 * size), F32)
    for i in range(total // BLOCK):
        low, high = key_range(i, total)
        rows = pl.ds(i * BLOCK, BLOCK)
        mask = allowed_mask(column, row, i, low, high)
        keys, values = k_ref[low:high, :], v_ref[low:high, :]
        q, g = q_ref[rows, :], grad_ref[rows, :]
        zero = jnp.zeros_like(q)
        dqs = []
        for h in range(2):
            qh = jnp.where(lane, q, zero) if h == 0 else jnp.where(lane, zero, q)
            gh = jnp.where(lane, g, zero) if h == 0 else jnp.where(lane, zero, g)
            log = log_ref[rows, h * size : h * size + 1]
            s = jnp.where(mask, dot32(qh, keys, NT) * scale, MASKED)
            p = jnp.exp(s - log)
            dp = dot32(gh, values, NT)
            delta = jnp.sum(p * dp, axis=-1, keepdims=True)
            ds = (p * (dp - delta)).astype(BF)
            dqs.append(dot32(ds, keys, NN))
            dk[low:high, :] += dot32(ds, qh, TN)
            dv[low:high, :] += dot32(p.astype(BF), gh, TN)
        dq = (jnp.where(lane, dqs[0], dqs[1]) * scale).astype(BF)
        out_ref[0, rows, :] = dq
        dq_sum += jnp.sum(dq.astype(F32), axis=0, keepdims=True)
    out_ref[1, :, :] = (dk[...] * scale).astype(BF)
    dvb = dv[...].astype(BF)
    out_ref[2, :, :] = dvb
    bias_ref[0:1, :] = dq_sum
    bias_ref[1:2, :] = jnp.sum(dvb.astype(F32), axis=0, keepdims=True)


def attend_specs(total, width, first):
    pick = lambda j: pl.BlockSpec((None, total, width), lambda h: (j, 0, h + first))
    return [
        pl.BlockSpec((total, 1), lambda h: (0, 0)),
        pl.BlockSpec((1, total), lambda h: (0, 0)),
        pick(0),
        pick(1),
        pick(2),
    ]


def attend(qkv, column, row, size, part, before, after):
    _, total, width = qkv.shape
    pair = 2 * size
    count = width // pair // 2
    flat = pl.BlockSpec((total, pair), lambda h: (0, h + part * count))
    return call(
        partial(attend_kernel, 1.0 / math.sqrt(size)),
        [column, row, qkv, qkv, qkv, *before],
        [shape((total, width)), shape((total, width), F32)],
        "attend",
        in_specs=attend_specs(total, pair, part * count) + [ANY] * len(before),
        out_specs=[flat, flat],
        flops=total * total * width * 8,
        grid=(count,),
        after=after,
        aliases={5 + i: i for i in range(len(before))},
    )


def attend_back(qkv, log, grad, column, row, size, part, before, after):
    _, total, width = qkv.shape
    pair = 2 * size
    count = width // pair // 2
    flat = pl.BlockSpec((total, pair), lambda h: (0, h + part * count))
    return call(
        partial(attend_back_kernel, 1.0 / math.sqrt(size)),
        [column, row, qkv, qkv, qkv, log, grad, *before],
        [shape((3, total, width)), shape((2, width), F32)],
        "attend_back",
        in_specs=attend_specs(total, pair, part * count) + [flat, flat] + [ANY] * len(before),
        out_specs=[
            pl.BlockSpec((3, total, pair), lambda h: (0, 0, h + part * count)),
            pl.BlockSpec((2, pair), lambda h: (0, h + part * count)),
        ],
        scratch=[pltpu.VMEM((total, pair), F32)] * 2,
        flops=total * total * width * 12,
        grid=(count,),
        after=after,
        aliases={7 + i: i for i in range(len(before))},
    )


def rows_kernel(dims, left, right, out):
    out[...] = dot32(left[...], right[...], dims).astype(out.dtype)


def rows_matmul(left, right, dims, name, kind=BF, after=()):
    total, depth = left.shape
    cols = right.shape[0] if dims is NT else right.shape[1]
    return call(
        partial(rows_kernel, dims),
        [left, right],
        [shape((total, cols), kind)],
        name,
        in_specs=[
            pl.BlockSpec((BLOCK, depth), lambda i: (i, 0)),
            pl.BlockSpec(right.shape, lambda i: (0, 0)),
        ],
        out_specs=[pl.BlockSpec((BLOCK, cols), lambda i: (i, 0))],
        flops=2 * total * depth * cols,
        grid=(total // BLOCK,),
        after=after,
    )[0]


def middle_kernel(x, part, got, bias, gain, shift, middle, second):
    value = x[...].astype(F32) + part[...].astype(F32) + got[...].astype(F32) + bias[...]
    middle[...] = value
    n, _ = moments(value)
    second[...] = (n * gain[...] + shift[...]).astype(BF)


def middle_norm(x, part, got, bias, gain, shift):
    total, width = x.shape
    rows = pl.BlockSpec((BLOCK, width), lambda i: (i, 0))
    line = pl.BlockSpec((1, width), lambda i: (0, 0))
    return call(
        middle_kernel,
        [x, part, got, bias, gain, shift],
        [shape((total, width), F32), shape((total, width))],
        "middle",
        in_specs=[rows] * 3 + [line] * 3,
        out_specs=[rows, rows],
        grid=(total // BLOCK,),
    )


def feed_kernel(second, cot, up, bias, down, hidden_ref, pre_ref, sum_ref):
    total = second.shape[0]
    root = math.sqrt(0.5)
    norm = 1.0 / math.sqrt(2.0 * math.pi)
    sums = jnp.zeros(sum_ref.shape, F32)
    for i in range(total // BLOCK):
        rows = pl.ds(i * BLOCK, BLOCK)
        v = dot32(second[rows, :], up[...], NN) + bias[...]
        g = dot32(cot[rows, :], down[...], NT)
        cdf = 0.5 * (1.0 + lax.erf(v * root))
        hidden_ref[rows, :] = (v * cdf).astype(BF)
        pre = (g * (cdf + v * (norm * jnp.exp(-0.5 * (v * v))))).astype(BF)
        pre_ref[rows, :] = pre
        sums += jnp.sum(pre.astype(F32), axis=0, keepdims=True)
    sum_ref[...] = sums


def feed_forward(second, cot, up, bias, down, tile=256):
    total, width = second.shape
    units = up.shape[1]
    whole = pl.BlockSpec((total, width), lambda u: (0, 0))
    cols = pl.BlockSpec((total, tile), lambda u: (0, u))
    line = pl.BlockSpec((1, tile), lambda u: (0, u))
    return call(
        feed_kernel,
        [second, cot, up, bias, down],
        [shape((total, units)), shape((total, units)), shape((1, units), F32)],
        "feed",
        in_specs=[
            whole,
            whole,
            pl.BlockSpec((width, tile), lambda u: (0, u)),
            line,
            pl.BlockSpec((tile, width), lambda u: (u, 0)),
        ],
        out_specs=[cols, cols, line],
        flops=4 * total * width * units,
        grid=(units // tile,),
    )


def down_grads_kernel(pos, hidden, cot, far1, far2, n1, n2, own):
    g = pl.program_id(0)
    rows = own.shape[1]
    acc = dot32(hidden[...], cot[...], TN).astype(BF)
    for k, out in enumerate((None, n2, n1, own)):

        @pl.when(g == k)
        def _():
            for j in range(4):
                value = acc[j * rows : (j + 1) * rows, :]
                if k == 0:
                    (far1, far2)[j // 2][j % 2] = value
                else:
                    out[j] = value


def ring_shapes(rows, cols):
    return [shape((2, rows, cols))] * 2 + [shape((4, rows, cols))] * 3


def ring_specs(rows, cols):
    whole = lambda n: pl.BlockSpec((n, rows, cols), lambda g, pos: (0, 0, 0))
    return [whole(2)] * 2 + [whole(4)] * 3


def down_grads(pos, hidden, cot, rows, after):
    total, units = hidden.shape
    width = cot.shape[1]
    return placed_call(
        down_grads_kernel,
        pos,
        [hidden, cot],
        ring_shapes(rows, width),
        "down_grads",
        (4,),
        [
            pl.BlockSpec((total, units // 4), lambda g, pos: (0, pos[0] ^ (3 - g))),
            pl.BlockSpec((total, width), lambda g, pos: (0, 0)),
        ],
        ring_specs(rows, width),
        flops=2 * total * units * width,
        after=after,
    )


def z_places(z):
    return lax.rem(z + 2, 4), lax.rem(z + 1, 4), lax.rem(z + 3, 4), z


def split_ring(g, refs, store):
    far1, far2, n1, n2, own = refs
    for k, out in enumerate((None, n2, n1, own)):

        @pl.when(g == k)
        def _():
            for zz in range(4):
                if k:
                    store(out, zz, zz)
                else:
                    store((far1, far2)[zz // 2], zz % 2, zz)


def up_grads_kernel(pos, second, pre, *refs):
    lead = refs[-1].shape[1] // 2
    acc = dot32(second[...], pre[...], TN).astype(BF)

    def store(out, at, zz):
        for cc in range(2):
            start = (cc * 4 + zz) * lead
            out[at, cc * lead : (cc + 1) * lead, :] = acc[start : start + lead, :]

    split_ring(pl.program_id(0), refs, store)


def up_grads(pos, second, pre, lead, after):
    total, width = second.shape
    units = pre.shape[1]
    return placed_call(
        up_grads_kernel,
        pos,
        [second, pre],
        ring_shapes(2 * lead, units),
        "up_grads",
        (4,),
        [
            pl.BlockSpec((total, width // 4), lambda g, pos: (0, pos[0] ^ (3 - g))),
            pl.BlockSpec((total, units), lambda g, pos: (0, 0)),
        ],
        ring_specs(2 * lead, units),
        flops=2 * total * units * width,
        after=after,
    )


def attn_grads_kernel(pos, normed, grads, mixed, branch, *refs):
    lead = refs[-1].shape[1] // 8
    half = refs[-1].shape[2]
    accs = [dot32(normed[...], grads[j], TN).astype(BF) for j in range(3)]
    acco = dot32(mixed[...], branch[...], TN).astype(BF)

    def store(out, at, zz):
        for cc in range(2):
            for j, acc in enumerate(accs):
                row, start = (2 * j + cc) * lead, (cc * 4 + zz) * lead
                out[at, row : row + lead, :] = acc[start : start + lead, :]
            row = (6 + cc) * lead
            out[at, row : row + lead, :] = acco[
                zz * lead : (zz + 1) * lead, cc * half : (cc + 1) * half
            ]

    split_ring(pl.program_id(0), refs, store)


def attn_grads(pos, normed, grads, mixed, branch, lead, after):
    total, width = normed.shape
    half = width // 2
    return placed_call(
        attn_grads_kernel,
        pos,
        [normed, grads, mixed, branch],
        ring_shapes(8 * lead, half),
        "attn_grads",
        (4,),
        [
            pl.BlockSpec((total, width // 4), lambda g, pos: (0, pos[0] ^ (3 - g))),
            pl.BlockSpec((3, total, half), lambda g, pos: (0, 0, 0)),
            pl.BlockSpec((total, half // 4), lambda g, pos: (0, pos[0] ^ (3 - g))),
            pl.BlockSpec((total, width), lambda g, pos: (0, 0)),
        ],
        ring_specs(8 * lead, half),
        flops=8 * total * width * half,
        after=after,
    )


def pass_kernel(n1, n2, t1, t2, s1, s2):
    for s, n, t, part in ((s1, n1, t2, 1), (s2, n2, t1, 0)):
        for j in range(4):
            if j // 2 == part:
                s[j] = (n[j].astype(F32) + t[j % 2].astype(F32)).astype(BF)
            else:
                s[j] = n[j]


def far_round(ring):
    return send(ring[0], X_SWAP), send(ring[1], Y_SWAP)


def near_round(ring, got, name, after=()):
    s1, s2 = call(
        pass_kernel,
        [ring[2], ring[3], *got],
        [shape(ring[2].shape)] * 2,
        name + "_pass",
        after=after,
    )
    return s1, [send(s1, X_SWAP), send(s2, Y_SWAP)]


def joined_kernel(extra):
    def body(own, r1, r2, *refs):
        far1, far2, first, second, mine, acc = refs[extra:]
        rows = own.shape[1]
        for j in range(4):
            acc[j, :rows, :] = own[j].astype(F32) + r1[j].astype(F32) + r2[j].astype(F32)
            if extra:
                acc[j, rows:, :] = sum(ref[j].astype(F32) for ref in refs[:extra])
        far, one, two, me = z_places(place()[2])
        cut = far1.shape[0]
        far1[...] = acc[far, :cut, :].astype(BF)
        far2[...] = acc[far, cut:, :].astype(BF)
        first[...] = acc[one].astype(BF)
        second[...] = acc[two].astype(BF)
        mine[...] = acc[me]

    return body


def join(ring, got, name, extra=(), after=()):
    _, rows, cols = ring[4].shape
    rows += extra[0].shape[1] if extra else 0
    cut = rows // 2 // 16 * 16
    return call(
        joined_kernel(len(extra)),
        [ring[4], *got, *extra],
        [
            shape((cut, cols)),
            shape((rows - cut, cols)),
            shape((rows, cols)),
            shape((rows, cols)),
            shape((rows, cols), F32),
        ],
        name + "_join",
        scratch=[pltpu.VMEM((4, rows, cols), F32)],
        after=after,
    )


def inner_pass_kernel(p1, p2, t1, t2, p1o, p2o):
    cut = p1.shape[0] // 2 // 16 * 16
    plus = lambda a, got: (a.astype(F32) + got[...].astype(F32)).astype(BF)
    p1o[:cut, :] = plus(p1[:cut, :], t1)
    p1o[cut:, :] = p1[cut:, :]
    p2o[:cut, :] = p2[:cut, :]
    p2o[cut:, :] = plus(p2[cut:, :], t2)


def inner_far(joined):
    return send(joined[0], Z_UP), send(joined[1], Z_DOWN)


def inner_near(joined, came, name, after=()):
    p1, p2 = call(
        inner_pass_kernel,
        [joined[2], joined[3], *came],
        [shape(joined[2].shape)] * 2,
        name + "_inner",
        after=after,
    )
    return p1, [joined[4], send(p1, Z_UP), send(p2, Z_DOWN)]


def total_of(refs):
    return refs[0][...] + refs[1][...].astype(F32) + refs[2][...].astype(F32)


def feed_last_kernel(p0, p1, p2, q0, q1, q2, down, kept, given, acc):
    _, c, _ = place()
    down[...] = total_of((p0, p1, p2))
    acc[...] = total_of((q0, q1, q2))
    lead = kept.shape[0]
    kept[...] = acc[pl.ds(pl.multiple_of(c * lead, lead), lead), :]
    given[...] = acc[pl.ds(pl.multiple_of((1 - c) * lead, lead), lead), :]


def attn_last_kernel(p0, p1, p2, kept, given, out, small, acc):
    _, c, _ = place()
    acc[...] = total_of((p0, p1, p2))
    lead = kept.shape[1]
    half = kept.shape[2]
    for j in range(3):
        at = 2 * j * lead
        kept[j] = acc[pl.ds(pl.multiple_of(at + c * lead, lead), lead), :]
        given[j] = acc[pl.ds(pl.multiple_of(at + (1 - c) * lead, lead), lead), :]
    out[:, :half] = acc[6 * lead : 7 * lead, :]
    out[:, half:] = acc[7 * lead : 8 * lead, :]
    small[...] = acc[8 * lead :, :]


def norm_back(n, spread, gain, grad):
    g = grad * gain
    return spread * (
        g - jnp.mean(g, axis=-1, keepdims=True) - n * jnp.mean(g * n, axis=-1, keepdims=True)
    )


def column(values):
    return jnp.sum(values, axis=0, keepdims=True)


def middle_back_kernel(part, got, middle, cot, gain, wout, branch, mgrad, mixed, sums):
    n, spread = moments(middle[...])
    grad = part[...].astype(F32) + got[...].astype(F32)
    c32 = cot[...].astype(F32)
    value = c32 + norm_back(n, spread, gain[...], grad)
    mgrad[...] = value
    rounded = value.astype(BF)
    branch[...] = rounded
    mixed[...] = dot32(rounded, wout[...], NT).astype(BF)

    @pl.when(pl.program_id(0) == 0)
    def _():
        sums[...] = jnp.zeros_like(sums)

    for j, v in enumerate((grad * n, grad, rounded.astype(F32), c32)):
        sums[j : j + 1, :] += column(v)


def middle_back(part, got, middle, cot, gain, wout, after):
    total, width = middle.shape
    half = wout.shape[0]
    rows = pl.BlockSpec((BLOCK, width), lambda i: (i, 0))
    fixed = lambda dims: pl.BlockSpec(dims, lambda i: (0, 0))
    return call(
        middle_back_kernel,
        [part, got, middle, cot, gain, wout],
        [
            shape((total, width)),
            shape((total, width), F32),
            shape((total, half)),
            shape((4, width), F32),
        ],
        "middle_back",
        in_specs=[rows] * 4 + [fixed((1, width)), fixed((half, width))],
        out_specs=[
            rows,
            rows,
            pl.BlockSpec((BLOCK, half), lambda i: (i, 0)),
            fixed((4, width)),
        ],
        flops=2 * total * width * half,
        grid=(total // BLOCK,),
        after=after,
    )


def source_grad_kernel(grads, weight, out):
    out[...] = sum(dot32(grads[j], weight[j], NT) for j in range(3)).astype(BF)


def source_grad(grads, weight, after):
    _, total, half = grads.shape
    width = weight.shape[1]
    return call(
        source_grad_kernel,
        [grads, weight],
        [shape((total, width))],
        "source_grad",
        in_specs=[
            pl.BlockSpec((3, BLOCK, half), lambda i: (0, i, 0)),
            pl.BlockSpec((3, width, half), lambda i: (0, 0, 0)),
        ],
        out_specs=[pl.BlockSpec((BLOCK, width), lambda i: (i, 0))],
        flops=6 * total * width * half,
        grid=(total // BLOCK,),
        after=after,
    )[0]


def own_block(g, pos):
    _, c, z = pos[0], pos[1], pos[2]
    parity = lax.rem(z, 2)
    return jnp.where(g < 2, 2 * c + (parity ^ (g & 1)), 2 * (1 - c) + (g & 1))


def input_back_kernel(pos, part, got, x, mgrad, gain, first, again, sums):
    g = pl.program_id(0)
    n, spread = moments(x[...].astype(F32))
    grad = part[...].astype(F32) + got[...].astype(F32)
    value = (mgrad[...] + norm_back(n, spread, gain[...], grad)).astype(BF)

    @pl.when(g == 0)
    def _():
        first[...] = value
        sums[...] = jnp.zeros_like(sums)

    @pl.when(g == 1)
    def _():
        again[...] = value

    for j, v in enumerate((grad * n, grad)):
        sums[j : j + 1, :] += column(v)


def input_back(pos, part, got, x, mgrad, gain, after):
    total, width = x.shape
    rows = pl.BlockSpec((BLOCK, width), lambda g, pos: (own_block(g, pos), 0))
    fixed = lambda n: pl.BlockSpec((n, width), lambda g, pos: (0, 0))
    return placed_call(
        input_back_kernel,
        pos,
        [part, got, x, mgrad, gain],
        [shape((BLOCK, width))] * 2 + [shape((2, width), F32)],
        "input_back",
        (total // BLOCK,),
        [rows] * 4 + [fixed(1)],
        [fixed(BLOCK), fixed(BLOCK), fixed(2)],
        after=after,
    )


def other_block(g, pos):
    return jnp.where(g < 2, 2 * (1 - pos[1]) + (g & 1), 2 * pos[1] + (g & 1))


def output_kernel(pos, hidden, down, middle, bias, theirs, mine):
    g = pl.program_id(0)
    value = dot32(hidden[...], down[...], NN)

    @pl.when(g < 2)
    def _():
        theirs[...] = value.astype(BF)

    @pl.when(g >= 2)
    def _():
        mine[...] = value + middle[...] + bias[...]


def output_rows(pos, hidden, down, middle, bias, after):
    total, units = hidden.shape
    width = down.shape[1]
    return placed_call(
        output_kernel,
        pos,
        [hidden, down, middle, bias],
        [shape((total // 2, width)), shape((total // 2, width), F32)],
        "output_rows",
        (4,),
        [
            pl.BlockSpec((BLOCK, units), lambda g, pos: (other_block(g, pos), 0)),
            pl.BlockSpec((units, width), lambda g, pos: (0, 0)),
            pl.BlockSpec((BLOCK, width), lambda g, pos: (other_block(g, pos), 0)),
            pl.BlockSpec((1, width), lambda g, pos: (0, 0)),
        ],
        [
            pl.BlockSpec((BLOCK, width), lambda g, pos: (jnp.minimum(g, 1), 0)),
            pl.BlockSpec((BLOCK, width), lambda g, pos: (jnp.maximum(g - 2, 0), 0)),
        ],
        flops=2 * total * units * width,
        after=after,
    )


def result_kernel(mine, got, first, again):
    _, _, z = place()
    parity = lax.rem(z, 2)
    for k, out in enumerate((first, again)):
        at = pl.multiple_of((parity ^ k) * BLOCK, BLOCK)
        out[...] = (mine[pl.ds(at, BLOCK), :] + got[pl.ds(at, BLOCK), :].astype(F32)).astype(BF)

XY_FAR = links(lambda o, c, z: (o ^ 3, c, z))


def fast_local(
    inputs,
    segment_ids,
    first_gain,
    first_shift,
    query_weight,
    query_bias,
    key_weight,
    value_weight,
    value_bias,
    out_weight,
    out_bias,
    second_gain,
    second_shift,
    up_weight,
    up_bias,
    down_weight,
    down_bias,
    cotangent,
):
    batch, rows, width = inputs.shape
    o, c, z = place()
    pos = jnp.stack([o, c, z]).astype(jnp.int32)
    total = batch * rows * 2
    half = width // 2
    units = up_weight.shape[1] // 2
    lead = query_weight.shape[0]
    down_rows = down_weight.shape[0]
    size = width // H
    vector_list = [
        first_gain,
        first_shift,
        query_bias,
        value_bias,
        out_bias,
        second_gain,
        second_shift,
        down_bias,
        up_bias,
    ]
    count = 8 * lead + down_rows

    small, at = jnp.zeros((half,), BF), 0
    for vector in vector_list:
        small = small + jnp.pad(vector, (at, half - at - vector.shape[0]))
        at += vector.shape[0]
    small = jnp.pad(small.reshape(1, half), ((0, 7), (0, 0)))
    weights = [query_weight, key_weight, value_weight]
    far, up_far = call(
        first_kernel,
        weights + [up_weight, small],
        [shape((3 * lead + 8, half)), shape((lead, units))],
        "first",
    )
    attn_pay, up_pay = call(
        second_kernel,
        weights + [up_weight, small, send(far, CORE_SWAP), send(up_far, CORE_SWAP)],
        [shape((6 * lead + 16, half)), shape((2 * lead, units))],
        "second",
    )

    pa, pb = ring_first(attn_pay, Z_UP, Z_DOWN)
    pc = ring_second(pa, pb, Z_UP, Z_DOWN)
    attn_all, down_own = copies(
        [attn_pay, pa, pb, *pc, down_weight, out_weight],
        [shape((4,) + attn_pay.shape), shape((down_rows + lead, width))],
        lambda ins, outs: inner_moves(ins, outs)
        + [
            (ins[5], outs[1].at[pl.ds(0, down_rows)]),
            (ins[6], outs[1].at[pl.ds(down_rows, lead)]),
        ],
        7,
        "attn_inner",
    )
    aa, ab = ring_first(attn_all, X_SWAP, Y_SWAP)
    da, db = ring_first(down_own, Z_UP, Z_DOWN)
    dc = ring_second(da, db, Z_UP, Z_DOWN)
    in0, in1 = call(
        inputs_kernel,
        [inputs, segment_ids],
        [shape((rows + 16, width))] * 2,
        "inputs_own",
        in_specs=[ANY, VMEM],
        scratch=[pltpu.SemaphoreType.DMA((2,))],
        after=[attn_all],
    )
    got = [send(in0, SEQUENCE[0]), send(in1, SEQUENCE[1])]
    ac = ring_outer_second(aa, ab, Y_SWAP, X_SWAP)

    def sequence_moves(ins, outs):
        _, cc, zz = place()
        parity = lax.rem(zz, 2)
        todo = []
        for m in range(2):
            for k in range(2):
                piece = ins[2 * m + k]
                at = (1 - cc if m else cc, parity ^ k)
                todo.append((piece.at[pl.ds(0, rows)], outs[0].at[at]))
                if len(outs) > 1:
                    todo.append((piece.at[pl.ds(rows, 16)], outs[1].at[at]))
        return todo

    def whole_sequence(pieces, name, after=()):
        more = pieces[0].shape[0] > rows
        outs = [shape((2, 2, rows, width))] + [shape((2, 2, 16, width))] * more
        return copies(pieces, outs, sequence_moves, 8 if more else 4, name, after=after)

    x, segments = whole_sequence(got + [send(g, CORE_SWAP) for g in got], "inputs_whole")
    x = x.reshape(total, width)
    segments = segments[:, :, 0, :rows].reshape(total).astype(F32)
    seg_col, seg_row = segments.reshape(total, 1), segments.reshape(1, total)

    down_all, up_own = copies(
        [down_own, da, db, *dc, up_pay],
        [shape((4,) + down_own.shape), shape(up_pay.shape)],
        lambda ins, outs: inner_moves(ins, outs) + [(ins[5], outs[1])],
        6,
        "down_inner",
        after=ac,
    )
    ea, eb = ring_first(down_all, X_SWAP, Y_SWAP)
    ua, ub = ring_first(up_own, Z_UP, Z_DOWN)

    def attn_blocks(src, outs, yx, zz):
        todo = [
            (src.at[pl.ds((2 * j + cc) * lead, lead)], outs[0].at[j, yx, cc, zz])
            for j in range(3)
            for cc in range(2)
        ]
        return todo + [(src.at[pl.ds(6 * lead, 16)], outs[1].at[yx, zz])]

    wqkv, small_all = copies(
        [attn_all, aa, ab, *ac],
        [shape((3, 4, 2, 4, lead, half)), shape((4, 4, 16, half))],
        lambda ins, outs: final_moves(ins, outs, attn_blocks),
        16 * 7,
        "attn_whole",
        after=[down_all],
    )
    wqkv = wqkv.reshape(3, width, half)

    small_all = small_all.reshape(4, 4, 2, 8, half)[:, :, :, 0, :count]
    vectors = small_all[..., : 8 * lead].reshape(4, 4, 2, 8, lead).transpose(3, 0, 2, 1, 4)
    own_cols = lax.dynamic_index_in_dim(vectors, c, 2, keepdims=False).reshape(8, half)
    vectors = vectors.reshape(8, width).astype(F32)
    line = lambda j: vectors[j : j + 1]
    gain1, shift1, bias_o, gain2, shift2, bias_d = [line(j) for j in (0, 1, 4, 5, 6, 7)]
    qkv_bias = jnp.stack([own_cols[2], jnp.zeros_like(own_cols[2]), own_cols[3]]).astype(F32)
    bias_u = lax.dynamic_index_in_dim(small_all[..., 8 * lead :], c, 2, keepdims=False)
    bias_u = bias_u.reshape(1, units).astype(F32)

    normed, qkv = project(x, gain1, shift1, wqkv, qkv_bias, [])
    uc = ring_second(ua, ub, Z_UP, Z_DOWN)

    def cotangent_moves(ins, outs):
        parity = lax.rem(place()[2], 2)
        return [(ins[0].at[parity], outs[0]), (ins[0].at[1 - parity], outs[1])]

    cots = copies(
        [cotangent],
        [shape((rows, width))] * 2,
        cotangent_moves,
        2,
        "cotangent_own",
        after=[ua, ub, normed],
    )
    cot_got = [send(block, pairs) for block, pairs in zip(cots, SEQUENCE)]
    heads = attend(qkv, seg_col, seg_row, size, 0, [], cots)
    ec = ring_outer_second(ea, eb, Y_SWAP, X_SWAP)
    mixed, log = attend(qkv, seg_col, seg_row, size, 1, heads, [ea, eb])
    up_all = copies(
        [up_own, ua, ub, *uc],
        [shape((4,) + up_pay.shape)],
        inner_moves,
        5,
        "up_inner",
        after=[*ec, mixed],
    )[0]
    fa, fb = ring_first(up_all, X_SWAP, Y_SWAP)

    def down_blocks(src, outs, yx, zz):
        return [
            (src.at[pl.ds(0, down_rows)], outs[0].at[yx, zz]),
            (src.at[pl.ds(down_rows, lead)], outs[1].at[yx, zz]),
        ]

    wdown, wout = copies(
        [down_all, ea, eb, *ec],
        [shape((4, 4, down_rows, width)), shape((4, 4, lead, width))],
        lambda ins, outs: final_moves(ins, outs, down_blocks),
        32,
        "down_whole",
        after=[up_all],
    )
    wdown, wout = wdown.reshape(units, width), wout.reshape(half, width)
    part = rows_matmul(mixed, wout, NN, "attend_out")
    middle, second = middle_norm(x, part, send(part, CORE_SWAP), bias_o, gain2, shift2)
    cot = whole_sequence(
        cot_got + [send(g, CORE_SWAP) for g in cot_got], "cotangent_whole", [part]
    )[0].reshape(total, width)

    def up_blocks(src, outs, yx, zz):
        return [(src.at[pl.ds(cc * lead, lead)], outs[0].at[yx, cc, zz]) for cc in range(2)]

    wup = copies(
        [up_all, fa, fb, *ring_outer_second(fa, fb, Y_SWAP, X_SWAP)],
        [shape((4, 2, 4, lead, units))],
        lambda ins, outs: final_moves(ins, outs, up_blocks),
        32,
        "up_whole",
        after=[second],
    )[0].reshape(width, units)
    hidden, pre_grad, up_bias_grad = feed_forward(second, cot, wup, bias_u, wdown)

    def to_tokens(got):
        return jnp.where((z & 1) == 0, jnp.stack(got), jnp.stack(got[::-1]))

    theirs, mine = output_rows(pos, hidden, wdown, middle, bias_d, [])
    d = down_grads(pos, hidden, cot, down_rows, [mine])
    d_far = far_round(d)
    blocks = call(
        result_kernel,
        [mine, send(theirs, CORE_SWAP)],
        [shape((rows, width))] * 2,
        "result",
        after=[d[4]],
    )
    out_got = [send(block, pairs) for block, pairs in zip(blocks, SEQUENCE)]
    u = up_grads(pos, second, pre_grad, lead, [blocks[0]])
    u_far = far_round(u)
    passed, d_got = near_round(d, d_far, "down", [u[4]])
    part = rows_matmul(pre_grad, wup, NT, "second_grad", after=[passed])
    passed, u_got = near_round(u, u_far, "up", [part])
    branch, middle_grad, mixed_grad, sums2 = middle_back(
        part, send(part, CORE_SWAP), middle, cot, gain2, wout, [passed]
    )

    back = attend_back(qkv, log, mixed_grad, seg_col, seg_row, size, 0, [], out_got)
    output = to_tokens(out_got)
    d_joined = join(d, d_got, "down", after=[back[1]])
    d_came = inner_far(d_joined)
    grads, qv_bias_grad = attend_back(
        qkv, log, mixed_grad, seg_col, seg_row, size, 1, back, [d_joined[4]]
    )
    passed, d_last = inner_near(d_joined, d_came, "down", [qv_bias_grad])
    a = attn_grads(pos, normed, grads, mixed, branch, lead, [passed])
    a_far = far_round(a)
    u_joined = join(u, u_got, "up", after=[a[4], *d_last[1:]])
    u_came = inner_far(u_joined)
    part = source_grad(grads, wqkv, [u_joined[4]])
    got = send(part, CORE_SWAP)
    passed, u_last = inner_near(u_joined, u_came, "up", [part])
    passed, a_got = near_round(a, a_far, "attn", [passed])
    in0, in1, sums1 = input_back(pos, part, got, x, middle_grad, gain1, [passed])
    in_got = [send(block, pairs) for block, pairs in zip((in0, in1), SEQUENCE)]
    input_grad = to_tokens(in_got).astype(F32)
    down_out, up_kept, up_given = call(
        feed_last_kernel,
        d_last + u_last,
        [shape(down_weight.shape, F32)] + [shape((lead, units), F32)] * 2,
        "feed_last",
        scratch=[pltpu.VMEM((2 * lead, units), F32)],
        after=[in0],
    )

    wide = jnp.stack([sums1[0], sums1[1], sums2[2], sums2[0], sums2[1], sums2[3]])
    wide = lax.dynamic_index_in_dim(wide.reshape(6, 4, 2, 4, lead), c, 2, keepdims=False)
    wide = jnp.concatenate(
        [wide[:2], qv_bias_grad.reshape(2, 4, 4, lead), wide[2:]], axis=0
    ).transpose(2, 1, 0, 3)
    tiny = jnp.concatenate(
        [
            wide.reshape(4, 4, 8 * lead),
            up_bias_grad.reshape(4, 4, down_rows).transpose(1, 0, 2),
        ],
        axis=-1,
    ).astype(BF)
    tiny = jnp.pad(tiny[:, :, None], ((0, 0), (0, 0), (0, 15), (0, half - count)))
    pick = lambda k: lax.dynamic_index_in_dim(tiny, o ^ k, 1, keepdims=False)
    extra = [pick(0), send(pick(1), X_SWAP), send(pick(2), Y_SWAP), send(pick(3), XY_FAR)]

    joined = join(a, a_got, "attn", extra, [down_out])
    _, attn_last = inner_near(joined, inner_far(joined), "attn")
    qkv_kept, qkv_given, out_out, small_sum = call(
        attn_last_kernel,
        attn_last,
        [shape((3, lead, half), F32)] * 2 + [shape((lead, width), F32), shape((16, half), F32)],
        "attn_last",
        scratch=[pltpu.VMEM((8 * lead + 16, half), F32)],
    )

    def whole_columns(kept, got):
        cols = kept.shape[-1] // 4
        kept, got = [a.reshape(a.shape[:-1] + (4, 1, cols)) for a in (kept, got)]
        both = jnp.where(
            c == 0, jnp.concatenate([kept, got], -2), jnp.concatenate([got, kept], -2)
        )
        return both.reshape(both.shape[:-3] + (8 * cols,))

    up_out = whole_columns(up_kept, send(up_given, CORE_SWAP))
    qkv_out = whole_columns(qkv_kept, send(qkv_given, CORE_SWAP))
    small_sum = small_sum[0]
    vec = lambda j: small_sum[j * lead : (j + 1) * lead]
    return (
        output,
        input_grad,
        vec(0),
        vec(1),
        qkv_out[0],
        vec(2),
        qkv_out[1],
        qkv_out[2],
        vec(3),
        out_out,
        vec(4),
        vec(5),
        vec(6),
        up_out,
        small_sum[8 * lead : count],
        down_out,
        vec(7),
    )


def solution(mesh):
    fast = mesh.shape["dp"] == 8 and mesh.shape["ctx"] == 4
    return jax.shard_map(
        fast_local if fast else local,
        mesh=mesh,
        in_specs=(
            P("dp", "ctx", None),
            P("dp", "ctx"),
            P(("dp", "ctx")),
            P(("dp", "ctx")),
            P(("dp", "ctx"), None),
            P(("dp", "ctx")),
            P(("dp", "ctx"), None),
            P(("dp", "ctx"), None),
            P(("dp", "ctx")),
            P(("dp", "ctx"), None),
            P(("dp", "ctx")),
            P(("dp", "ctx")),
            P(("dp", "ctx")),
            P(("dp", "ctx"), None),
            P(("dp", "ctx")),
            P(("dp", "ctx"), None),
            P(("dp", "ctx")),
            P("dp", "ctx", None),
        ),
        out_specs=(
            P("dp", "ctx", None),
            P("dp", "ctx", None),
            P(("dp", "ctx")),
            P(("dp", "ctx")),
            P(("dp", "ctx"), None),
            P(("dp", "ctx")),
            P(("dp", "ctx"), None),
            P(("dp", "ctx"), None),
            P(("dp", "ctx")),
            P(("dp", "ctx"), None),
            P(("dp", "ctx")),
            P(("dp", "ctx")),
            P(("dp", "ctx")),
            P(("dp", "ctx"), None),
            P(("dp", "ctx")),
            P(("dp", "ctx"), None),
            P(("dp", "ctx")),
        ),
        check_vma=False,
    )
```

```python
from functools import partial
import math

import jax
import jax.numpy as jnp
from jax import lax
from jax.experimental import pallas as pl
from jax.experimental.pallas import tpu as pltpu
from jax.sharding import PartitionSpec as P

H = 16


EPS = 1e-05
MASKED = -1e30


def normalize(values, gain, shift):
    mean = jnp.mean(values, axis=-1, keepdims=True)
    centered = values - mean
    spread = jnp.mean(centered * centered, axis=-1, keepdims=True)
    return centered * lax.rsqrt(spread + EPS) * gain + shift


def product(left, right):
    return jnp.einsum("btd,de->bte", left, right, preferred_element_type=jnp.float32)


def product_back(left, right):
    return jnp.einsum("bte,de->btd", left, right, preferred_element_type=jnp.float32)


def outer_sum(left, right):
    return jnp.einsum("btd,bte->de", left, right, preferred_element_type=jnp.float32)


def column_sum(values):
    return jnp.sum(values.astype(jnp.float32), axis=(0, 1))


def gather_attention(
    first_gain,
    first_shift,
    query_weight,
    query_bias,
    key_weight,
    value_weight,
    value_bias,
    out_weight,
    out_bias,
):
    return (
        lax.all_gather(first_gain, ("dp", "ctx"), axis=0, tiled=True),
        lax.all_gather(first_shift, ("dp", "ctx"), axis=0, tiled=True),
        lax.all_gather(query_weight, ("dp", "ctx"), axis=0, tiled=True),
        lax.all_gather(query_bias, ("dp", "ctx"), axis=0, tiled=True),
        lax.all_gather(key_weight, ("dp", "ctx"), axis=0, tiled=True),
        lax.all_gather(value_weight, ("dp", "ctx"), axis=0, tiled=True),
        lax.all_gather(value_bias, ("dp", "ctx"), axis=0, tiled=True),
        lax.all_gather(out_weight, ("dp", "ctx"), axis=0, tiled=True),
        lax.all_gather(out_bias, ("dp", "ctx"), axis=0, tiled=True),
    )


def gather_feed(second_gain, second_shift, up_weight, up_bias, down_weight, down_bias):
    return (
        lax.all_gather(second_gain, ("dp", "ctx"), axis=0, tiled=True),
        lax.all_gather(second_shift, ("dp", "ctx"), axis=0, tiled=True),
        lax.all_gather(up_weight, ("dp", "ctx"), axis=0, tiled=True),
        lax.all_gather(up_bias, ("dp", "ctx"), axis=0, tiled=True),
        lax.all_gather(down_weight, ("dp", "ctx"), axis=0, tiled=True),
        lax.all_gather(down_bias, ("dp", "ctx"), axis=0, tiled=True),
    )


def gather_keys(keys, values, segments):
    return (
        lax.all_gather(keys, "ctx", axis=1, tiled=True),
        lax.all_gather(values, "ctx", axis=1, tiled=True),
        lax.all_gather(segments, "ctx", axis=1, tiled=True),
    )


def score_block(queries, keys_all, segments, segments_all):
    batch, rows, width = queries.shape
    size = width // H
    total_len = keys_all.shape[1]
    query_heads = queries.reshape(batch, rows, H, size)
    key_heads = keys_all.reshape(batch, total_len, H, size)
    raw = jnp.einsum("bqhd,bkhd->bhqk", query_heads, key_heads, preferred_element_type=jnp.float32)
    scores = raw * (1.0 / math.sqrt(size))
    offset = lax.axis_index("ctx") * rows
    query_pos = offset + jnp.arange(rows, dtype=jnp.int32)
    key_pos = jnp.arange(total_len, dtype=jnp.int32)
    causal = key_pos[None, :] <= query_pos[:, None]
    same_doc = segments[:, :, None] == segments_all[:, None, :]
    allowed = (causal[None] & same_doc)[:, None]
    return jnp.where(allowed, scores, MASKED)


def forward_part(inputs, segments, attn, feed):
    (
        first_gain,
        first_shift,
        query_weight,
        query_bias,
        key_weight,
        value_weight,
        value_bias,
        out_weight,
        out_bias,
    ) = attn
    second_gain, second_shift, up_weight, up_bias, down_weight, down_bias = feed
    batch, rows, width = inputs.shape
    size = width // H
    source = inputs.astype(jnp.float32)
    normed = normalize(
        source, first_gain.astype(jnp.float32), first_shift.astype(jnp.float32)
    ).astype(jnp.bfloat16)
    queries = (product(normed, query_weight) + query_bias.astype(jnp.float32)).astype(jnp.bfloat16)
    keys = product(normed, key_weight).astype(jnp.bfloat16)
    values = (product(normed, value_weight) + value_bias.astype(jnp.float32)).astype(jnp.bfloat16)
    keys_all, values_all, segments_all = gather_keys(keys, values, segments)
    scores = score_block(queries, keys_all, segments, segments_all)
    top = jnp.max(scores, axis=-1, keepdims=True)
    expo = jnp.exp(scores - top)
    row_total = jnp.sum(expo, axis=-1, keepdims=True)
    probs = (expo / row_total).astype(jnp.bfloat16)
    log_total = top + jnp.log(row_total)
    value_heads = values_all.reshape(batch, values_all.shape[1], H, size)
    mixed = jnp.einsum("bhqk,bkhd->bqhd", probs, value_heads, preferred_element_type=jnp.float32)
    mixed = mixed.reshape(batch, rows, width).astype(jnp.bfloat16)
    middle = source + product(mixed, out_weight) + out_bias.astype(jnp.float32)
    second = normalize(
        middle, second_gain.astype(jnp.float32), second_shift.astype(jnp.float32)
    ).astype(jnp.bfloat16)
    hidden_pre = product(second, up_weight) + up_bias.astype(jnp.float32)
    hidden = jax.nn.gelu(hidden_pre, approximate=False).astype(jnp.bfloat16)
    output = (middle + product(hidden, down_weight) + down_bias.astype(jnp.float32)).astype(
        jnp.bfloat16
    )
    kept = (
        source,
        normed,
        queries,
        keys,
        values,
        log_total,
        mixed,
        middle,
        second,
        hidden_pre,
        hidden,
    )
    return (output, kept, (keys_all, values_all, segments_all))


def backward_part(kept, gathered, segments, cotangent, attn, feed):
    (
        first_gain,
        first_shift,
        query_weight,
        query_bias,
        key_weight,
        value_weight,
        value_bias,
        out_weight,
        out_bias,
    ) = attn
    second_gain, second_shift, up_weight, up_bias, down_weight, down_bias = feed
    source, normed, queries, keys, values, log_total, mixed, middle, second, hidden_pre, hidden = (
        kept
    )
    keys_all, values_all, segments_all = gathered
    batch, rows, width = source.shape
    size = width // H
    total_len = keys_all.shape[1]
    scale = 1.0 / math.sqrt(size)
    down_grad = outer_sum(hidden, cotangent)
    down_bias_grad = column_sum(cotangent)
    hidden_grad = product_back(cotangent, down_weight)
    _, gelu_back = jax.vjp(partial(jax.nn.gelu, approximate=False), hidden_pre)
    pre_grad = gelu_back(hidden_grad)[0].astype(jnp.bfloat16)
    up_grad = outer_sum(second, pre_grad)
    up_bias_grad = column_sum(pre_grad)
    second_grad = product_back(pre_grad, up_weight)
    _, second_back = jax.vjp(
        normalize, middle, second_gain.astype(jnp.float32), second_shift.astype(jnp.float32)
    )
    middle_part, second_gain_grad, second_shift_grad = second_back(second_grad)
    feed_grads = (
        lax.psum_scatter(second_gain_grad, ("dp", "ctx"), scatter_dimension=0, tiled=True),
        lax.psum_scatter(second_shift_grad, ("dp", "ctx"), scatter_dimension=0, tiled=True),
        lax.psum_scatter(up_grad, ("dp", "ctx"), scatter_dimension=0, tiled=True),
        lax.psum_scatter(up_bias_grad, ("dp", "ctx"), scatter_dimension=0, tiled=True),
        lax.psum_scatter(down_grad, ("dp", "ctx"), scatter_dimension=0, tiled=True),
        lax.psum_scatter(down_bias_grad, ("dp", "ctx"), scatter_dimension=0, tiled=True),
    )
    middle_grad = cotangent.astype(jnp.float32) + middle_part
    branch_grad = middle_grad.astype(jnp.bfloat16)
    out_grad = outer_sum(mixed, branch_grad)
    out_bias_grad = column_sum(branch_grad)
    mixed_grad = product_back(branch_grad, out_weight).astype(jnp.bfloat16)
    scores = score_block(queries, keys_all, segments, segments_all)
    probs_full = jnp.exp(scores - log_total)
    probs = probs_full.astype(jnp.bfloat16)
    grad_heads = mixed_grad.reshape(batch, rows, H, size)
    query_heads = queries.reshape(batch, rows, H, size)
    key_heads = keys_all.reshape(batch, total_len, H, size)
    value_heads = values_all.reshape(batch, total_len, H, size)
    value_grad_all = jnp.einsum(
        "bhqk,bqhd->bkhd", probs, grad_heads, preferred_element_type=jnp.float32
    )
    prob_grad = jnp.einsum(
        "bqhd,bkhd->bhqk", grad_heads, value_heads, preferred_element_type=jnp.float32
    )
    delta = jnp.sum(probs_full * prob_grad, axis=-1, keepdims=True)
    score_grad = (probs_full * (prob_grad - delta)).astype(jnp.bfloat16)
    query_grad = (
        jnp.einsum("bhqk,bkhd->bqhd", score_grad, key_heads, preferred_element_type=jnp.float32)
        * scale
    )
    query_grad = query_grad.reshape(batch, rows, width).astype(jnp.bfloat16)
    key_grad_all = (
        jnp.einsum("bhqk,bqhd->bkhd", score_grad, query_heads, preferred_element_type=jnp.float32)
        * scale
    )
    key_sum, value_sum = (
        lax.psum_scatter(
            key_grad_all.reshape(batch, total_len, width).astype(jnp.bfloat16),
            "ctx",
            scatter_dimension=1,
            tiled=True,
        ).astype(jnp.float32),
        lax.psum_scatter(
            value_grad_all.reshape(batch, total_len, width).astype(jnp.bfloat16),
            "ctx",
            scatter_dimension=1,
            tiled=True,
        ).astype(jnp.float32),
    )
    key_grad = key_sum.astype(jnp.bfloat16)
    value_grad = value_sum.astype(jnp.bfloat16)
    query_weight_grad = outer_sum(normed, query_grad)
    query_bias_grad = column_sum(query_grad)
    key_weight_grad = outer_sum(normed, key_grad)
    value_weight_grad = outer_sum(normed, value_grad)
    value_bias_grad = column_sum(value_grad)
    normed_grad = (
        product_back(query_grad, query_weight)
        + product_back(key_grad, key_weight)
        + product_back(value_grad, value_weight)
    )
    _, first_back = jax.vjp(
        normalize, source, first_gain.astype(jnp.float32), first_shift.astype(jnp.float32)
    )
    input_part, first_gain_grad, first_shift_grad = first_back(normed_grad)
    input_grad = middle_grad + input_part
    attn_grads = (
        lax.psum_scatter(first_gain_grad, ("dp", "ctx"), scatter_dimension=0, tiled=True),
        lax.psum_scatter(first_shift_grad, ("dp", "ctx"), scatter_dimension=0, tiled=True),
        lax.psum_scatter(query_weight_grad, ("dp", "ctx"), scatter_dimension=0, tiled=True),
        lax.psum_scatter(query_bias_grad, ("dp", "ctx"), scatter_dimension=0, tiled=True),
        lax.psum_scatter(key_weight_grad, ("dp", "ctx"), scatter_dimension=0, tiled=True),
        lax.psum_scatter(value_weight_grad, ("dp", "ctx"), scatter_dimension=0, tiled=True),
        lax.psum_scatter(value_bias_grad, ("dp", "ctx"), scatter_dimension=0, tiled=True),
        lax.psum_scatter(out_grad, ("dp", "ctx"), scatter_dimension=0, tiled=True),
        lax.psum_scatter(out_bias_grad, ("dp", "ctx"), scatter_dimension=0, tiled=True),
    )
    return (input_grad, attn_grads, feed_grads)


def local(
    inputs,
    segment_ids,
    first_gain,
    first_shift,
    query_weight,
    query_bias,
    key_weight,
    value_weight,
    value_bias,
    out_weight,
    out_bias,
    second_gain,
    second_shift,
    up_weight,
    up_bias,
    down_weight,
    down_bias,
    cotangent,
):
    attn = gather_attention(
        first_gain,
        first_shift,
        query_weight,
        query_bias,
        key_weight,
        value_weight,
        value_bias,
        out_weight,
        out_bias,
    )
    feed = gather_feed(second_gain, second_shift, up_weight, up_bias, down_weight, down_bias)
    output, kept, gathered = forward_part(inputs, segment_ids, attn, feed)
    key_set = gather_keys(kept[3], kept[4], segment_ids)
    input_grad, attn_grads, feed_grads = backward_part(
        kept, key_set, segment_ids, cotangent, attn, feed
    )
    result = (output, input_grad)
    return result + tuple(attn_grads) + tuple(feed_grads)


AXES = ("dp", "ctx")
BLOCK = 256
BF = jnp.bfloat16
F32 = jnp.float32
NT = (((1,), (1,)), ((), ()))
NN = (((1,), (0,)), ((), ()))
TN = (((0,), (0,)), ((), ()))
ANY = pl.BlockSpec(memory_space=pl.ANY)
VMEM = pl.BlockSpec(memory_space=pltpu.VMEM)


def links(step):
    pairs = []
    for o in range(4):
        for c in range(2):
            for z in range(4):
                o2, c2, z2 = step(o, c, z)
                pairs.append(((o * 2 + c) * 4 + z, (o2 * 2 + c2) * 4 + z2))
    return pairs


X_SWAP = links(lambda o, c, z: (o ^ 1, c, z))
Y_SWAP = links(lambda o, c, z: (o ^ 2, c, z))
CORE_SWAP = links(lambda o, c, z: (o, 1 - c, z))
Z_UP = links(lambda o, c, z: (o, c, (z + 1) % 4))
Z_DOWN = links(lambda o, c, z: (o, c, (z + 3) % 4))
SEQUENCE = [links(lambda o, c, z, k=k: (o, z >> 1, 2 * c + ((z & 1) ^ k))) for k in range(2)]


def send(value, pairs):
    return lax.ppermute(value, AXES, pairs)


def place():
    dp = lax.axis_index("dp")
    return dp // 2, dp % 2, lax.axis_index("ctx")


def dot32(left, right, dims):
    return lax.dot_general(left, right, dims, preferred_element_type=F32)


def shape(dims, kind=BF):
    return jax.ShapeDtypeStruct(dims, kind)


def cost(flops, nbytes, special=0):
    return pl.CostEstimate(flops=int(flops), bytes_accessed=int(nbytes), transcendentals=special)


def moved_bytes(arrays):
    return sum(math.prod(a.shape) * jnp.dtype(a.dtype).itemsize for a in arrays)


def without(body, lead, count):
    return (lambda *refs: body(*refs[:lead], *refs[lead + count :])) if count else body


def call(
    body,
    ins,
    outs,
    name,
    in_specs=None,
    out_specs=None,
    scratch=(),
    flops=0,
    grid=(),
    after=(),
    aliases={},
):
    return pl.pallas_call(
        without(body, len(ins), len(after)),
        grid=grid,
        in_specs=list(in_specs or [VMEM] * len(ins)) + [ANY] * len(after),
        out_specs=out_specs or [VMEM] * len(outs),
        out_shape=outs,
        scratch_shapes=list(scratch),
        cost_estimate=cost(flops, moved_bytes(ins) + moved_bytes(outs)),
        input_output_aliases=aliases,
        name=name,
    )(*ins, *after)


def placed_call(
    body, pos, ins, outs, name, grid, in_specs, out_specs, scratch=(), flops=0, after=()
):
    return pl.pallas_call(
        without(body, len(ins) + 1, len(after)),
        grid_spec=pltpu.PrefetchScalarGridSpec(
            num_scalar_prefetch=1,
            grid=grid,
            in_specs=list(in_specs) + [ANY] * len(after),
            out_specs=out_specs,
            scratch_shapes=list(scratch),
        ),
        out_shape=outs,
        cost_estimate=cost(flops, moved_bytes(ins) + moved_bytes(outs)),
        name=name,
    )(pos, *ins, *after)


def copies(ins, outs, moves, count, name, after=()):
    def body(*refs):
        sems = refs[-1]
        todo = moves(refs[: len(ins)], refs[len(ins) : -1])
        started = [pltpu.make_async_copy(s, d, sems.at[i]) for i, (s, d) in enumerate(todo)]
        for copy in started:
            copy.start()
        for copy in started:
            copy.wait()

    return call(
        body,
        ins,
        outs,
        name,
        in_specs=[ANY] * len(ins),
        scratch=[pltpu.SemaphoreType.DMA((count,))],
        after=after,
    )


def own_columns(weight, k):
    n = weight.shape[1] // 8
    parts = [
        jnp.where(k == 0, weight[:, 2 * g * n : (2 * g + 1) * n], weight[:, (2 * g + 1) * n : (2 * g + 2) * n])
        for g in range(4)
    ]
    return jnp.concatenate(parts, axis=1)


def first_kernel(qw, kw, vw, uw, small, far, up_far):
    _, c, _ = place()
    lead = qw.shape[0]
    for j, ref in enumerate((qw, kw, vw)):
        far[j * lead : (j + 1) * lead, :] = own_columns(ref[...], 1 - c)
    far[3 * lead :, :] = small[...]
    up_far[...] = own_columns(uw[...], 1 - c)


def inputs_kernel(inputs, segs, in0, in1, sems):
    rows = inputs.shape[1]
    parity = lax.rem(place()[2], 2)
    todo = []
    for k, out in enumerate((in0, in1)):
        pick = parity if k == 0 else 1 - parity
        todo.append(pltpu.make_async_copy(inputs.at[pick], out.at[pl.ds(0, rows)], sems.at[k]))
        todo[-1].start()
        line = segs[pl.ds(pick, 1), :].astype(F32)
        out[rows:, :] = jnp.zeros((out.shape[0] - rows, out.shape[1]), BF)
        out[rows:, :rows] = jnp.broadcast_to(line, (out.shape[0] - rows, rows)).astype(BF)
    for copy in todo:
        copy.wait()


def second_kernel(qw, kw, vw, uw, small, far, up_far, attn, up):
    _, c, _ = place()
    lead = qw.shape[0]

    def both(out, at, own, got):
        n = own.shape[0]
        out[at : at + n, :] = jnp.where(c == 0, own, got)
        out[at + n : at + 2 * n, :] = jnp.where(c == 0, got, own)

    for j, ref in enumerate((qw, kw, vw)):
        both(attn, 2 * j * lead, own_columns(ref[...], c), far[j * lead : (j + 1) * lead, :])
    both(attn, 6 * lead, small[...], far[3 * lead :, :])
    both(up, 0, own_columns(uw[...], c), up_far[...])


def inner_moves(ins, outs):
    own, first, second, far1, far2 = ins[:5]
    cut = far1.shape[0]
    return [
        (own, outs[0].at[0]),
        (first, outs[0].at[1]),
        (second, outs[0].at[2]),
        (far1, outs[0].at[3, pl.ds(0, cut)]),
        (far2, outs[0].at[3, pl.ds(cut, far2.shape[0])]),
    ]


def ring_first(value, n1, n2):
    return send(value, n1), send(value, n2)


def ring_second(a, b, f1, f2):
    cut = a.shape[0] // 2 // 16 * 16
    return send(a[:cut], f1), send(b[cut:], f2)


def ring_outer_second(a, b, f1, f2):
    return send(a[:2], f1), send(b[2:], f2)


def final_moves(ins, outs, blocks):
    o, _, z = place()
    z_ring = (z, lax.rem(z + 3, 4), lax.rem(z + 1, 4), lax.rem(z + 2, 4))
    yx_ring = (o, o ^ 1, o ^ 2, o ^ 3)
    todo = []
    for k in range(4):
        for j in range(4):
            source = ins[k].at[j] if k < 3 else ins[3 + j // 2].at[j % 2]
            todo += blocks(source, outs, yx_ring[k], z_ring[j])
    return todo


def moments(values):
    mean = jnp.mean(values, axis=-1, keepdims=True)
    centered = values - mean
    spread = lax.rsqrt(jnp.mean(centered * centered, axis=-1, keepdims=True) + EPS)
    return centered * spread, spread


def project_kernel(x, gain, shift, weight, bias, normed, qkv):
    n, _ = moments(x[...].astype(F32))
    value = (n * gain[...] + shift[...]).astype(BF)
    normed[...] = value
    for j in range(3):
        qkv[j] = (dot32(value, weight[j], NN) + bias[j : j + 1, :]).astype(BF)


def project(x, gain, shift, weight, bias, after):
    total, width = x.shape
    half = weight.shape[2]
    rows = pl.BlockSpec((BLOCK, width), lambda i: (i, 0))
    line = pl.BlockSpec((1, width), lambda i: (0, 0))
    return call(
        project_kernel,
        [x, gain, shift, weight, bias],
        [shape((total, width)), shape((3, total, half))],
        "project",
        in_specs=[
            rows,
            line,
            line,
            pl.BlockSpec((3, width, half), lambda i: (0, 0, 0)),
            pl.BlockSpec((3, half), lambda i: (0, 0)),
        ],
        out_specs=[rows, pl.BlockSpec((3, BLOCK, half), lambda i: (0, i, 0))],
        flops=6 * total * width * half,
        grid=(total // BLOCK,),
        after=after,
    )


def allowed_mask(column, row, i, low, high):
    rows = i * BLOCK + lax.broadcasted_iota(jnp.int32, (BLOCK, high - low), 0)
    cols = low + lax.broadcasted_iota(jnp.int32, (BLOCK, high - low), 1)
    same = column[i * BLOCK : i * BLOCK + BLOCK, :] == row[:, low:high]
    return same & (cols <= rows)


def key_range(i, total):
    return max(0, (i * BLOCK - total // 2 + 1) // BLOCK * BLOCK), (i + 1) * BLOCK


def attend_kernel(scale, column, row, q_ref, k_ref, v_ref, *refs):
    mixed_ref, log_ref = refs[-2:]
    total = q_ref.shape[0]
    size = q_ref.shape[1] // 2
    lane = lax.broadcasted_iota(jnp.int32, (BLOCK, 2 * size), 1) < size
    for i in range(total // BLOCK):
        low, high = key_range(i, total)
        rows = pl.ds(i * BLOCK, BLOCK)
        mask = allowed_mask(column, row, i, low, high)
        keys, values = k_ref[low:high, :], v_ref[low:high, :]
        q = q_ref[rows, :]
        zero = jnp.zeros_like(q)
        outs, logs = [], []
        for own in (jnp.where(lane, q, zero), jnp.where(lane, zero, q)):
            s = jnp.where(mask, dot32(own, keys, NT) * scale, MASKED)
            top = jnp.max(s, axis=-1, keepdims=True)
            e = jnp.exp(s - top)
            tot = jnp.sum(e, axis=-1, keepdims=True)
            p = (e * (1.0 / tot)).astype(BF)
            outs.append(dot32(p, values, NN))
            logs.append(top + jnp.log(tot))
        mixed_ref[rows, :] = jnp.where(lane, outs[0], outs[1]).astype(BF)
        log_ref[rows, :] = jnp.where(lane, logs[0], logs[1])


def attend_back_kernel(
    scale, column, row, q_ref, k_ref, v_ref, log_ref, grad_ref, *refs
):
    out_ref, bias_ref, dk, dv = refs[-4:]
    total = q_ref.shape[0]
    size = q_ref.shape[1] // 2
    lane = lax.broadcasted_iota(jnp.int32, (BLOCK, 2 * size), 1) < size
    dk[...] = jnp.zeros_like(dk)
    dv[...] = jnp.zeros_like(dv)
    dq_sum = jnp.zeros((1, 2 * size), F32)
    for i in range(total // BLOCK):
        low, high = key_range(i, total)
        rows = pl.ds(i * BLOCK, BLOCK)
        mask = allowed_mask(column, row, i, low, high)
        keys, values = k_ref[low:high, :], v_ref[low:high, :]
        q, g = q_ref[rows, :], grad_ref[rows, :]
        zero = jnp.zeros_like(q)
        dqs = []
        for h in range(2):
            qh = jnp.where(lane, q, zero) if h == 0 else jnp.where(lane, zero, q)
            gh = jnp.where(lane, g, zero) if h == 0 else jnp.where(lane, zero, g)
            log = log_ref[rows, h * size : h * size + 1]
            s = jnp.where(mask, dot32(qh, keys, NT) * scale, MASKED)
            p = jnp.exp(s - log)
            dp = dot32(gh, values, NT)
            delta = jnp.sum(p * dp, axis=-1, keepdims=True)
            ds = (p * (dp - delta)).astype(BF)
            dqs.append(dot32(ds, keys, NN))
            dk[low:high, :] += dot32(ds, qh, TN)
            dv[low:high, :] += dot32(p.astype(BF), gh, TN)
        dq = (jnp.where(lane, dqs[0], dqs[1]) * scale).astype(BF)
        out_ref[0, rows, :] = dq
        dq_sum += jnp.sum(dq.astype(F32), axis=0, keepdims=True)
    out_ref[1, :, :] = (dk[...] * scale).astype(BF)
    dvb = dv[...].astype(BF)
    out_ref[2, :, :] = dvb
    bias_ref[0:1, :] = dq_sum
    bias_ref[1:2, :] = jnp.sum(dvb.astype(F32), axis=0, keepdims=True)


def attend_specs(total, width, first):
    pick = lambda j: pl.BlockSpec((None, total, width), lambda h: (j, 0, h + first))
    return [
        pl.BlockSpec((total, 1), lambda h: (0, 0)),
        pl.BlockSpec((1, total), lambda h: (0, 0)),
        pick(0),
        pick(1),
        pick(2),
    ]


def attend(qkv, column, row, size, part, before, after):
    _, total, width = qkv.shape
    pair = 2 * size
    count = width // pair // 2
    flat = pl.BlockSpec((total, pair), lambda h: (0, h + part * count))
    return call(
        partial(attend_kernel, 1.0 / math.sqrt(size)),
        [column, row, qkv, qkv, qkv, *before],
        [shape((total, width)), shape((total, width), F32)],
        "attend",
        in_specs=attend_specs(total, pair, part * count) + [ANY] * len(before),
        out_specs=[flat, flat],
        flops=total * total * width * 8,
        grid=(count,),
        after=after,
        aliases={5 + i: i for i in range(len(before))},
    )


def attend_back(qkv, log, grad, column, row, size, part, before, after):
    _, total, width = qkv.shape
    pair = 2 * size
    count = width // pair // 2
    flat = pl.BlockSpec((total, pair), lambda h: (0, h + part * count))
    return call(
        partial(attend_back_kernel, 1.0 / math.sqrt(size)),
        [column, row, qkv, qkv, qkv, log, grad, *before],
        [shape((3, total, width)), shape((2, width), F32)],
        "attend_back",
        in_specs=attend_specs(total, pair, part * count) + [flat, flat] + [ANY] * len(before),
        out_specs=[
            pl.BlockSpec((3, total, pair), lambda h: (0, 0, h + part * count)),
            pl.BlockSpec((2, pair), lambda h: (0, h + part * count)),
        ],
        scratch=[pltpu.VMEM((total, pair), F32)] * 2,
        flops=total * total * width * 12,
        grid=(count,),
        after=after,
        aliases={7 + i: i for i in range(len(before))},
    )


def rows_kernel(dims, left, right, out):
    out[...] = dot32(left[...], right[...], dims).astype(out.dtype)


def rows_matmul(left, right, dims, name, kind=BF, after=()):
    total, depth = left.shape
    cols = right.shape[0] if dims is NT else right.shape[1]
    return call(
        partial(rows_kernel, dims),
        [left, right],
        [shape((total, cols), kind)],
        name,
        in_specs=[
            pl.BlockSpec((BLOCK, depth), lambda i: (i, 0)),
            pl.BlockSpec(right.shape, lambda i: (0, 0)),
        ],
        out_specs=[pl.BlockSpec((BLOCK, cols), lambda i: (i, 0))],
        flops=2 * total * depth * cols,
        grid=(total // BLOCK,),
        after=after,
    )[0]


def middle_kernel(x, part, got, bias, gain, shift, middle, second):
    value = x[...].astype(F32) + part[...].astype(F32) + got[...].astype(F32) + bias[...]
    middle[...] = value
    n, _ = moments(value)
    second[...] = (n * gain[...] + shift[...]).astype(BF)


def middle_norm(x, part, got, bias, gain, shift):
    total, width = x.shape
    rows = pl.BlockSpec((BLOCK, width), lambda i: (i, 0))
    line = pl.BlockSpec((1, width), lambda i: (0, 0))
    return call(
        middle_kernel,
        [x, part, got, bias, gain, shift],
        [shape((total, width), F32), shape((total, width))],
        "middle",
        in_specs=[rows] * 3 + [line] * 3,
        out_specs=[rows, rows],
        grid=(total // BLOCK,),
    )


def feed_kernel(second, cot, up, bias, down, hidden_ref, pre_ref, sum_ref):
    total = second.shape[0]
    root = math.sqrt(0.5)
    norm = 1.0 / math.sqrt(2.0 * math.pi)
    sums = jnp.zeros(sum_ref.shape, F32)
    for i in range(total // BLOCK):
        rows = pl.ds(i * BLOCK, BLOCK)
        v = dot32(second[rows, :], up[...], NN) + bias[...]
        g = dot32(cot[rows, :], down[...], NT)
        cdf = 0.5 * (1.0 + lax.erf(v * root))
        hidden_ref[rows, :] = (v * cdf).astype(BF)
        pre = (g * (cdf + v * (norm * jnp.exp(-0.5 * (v * v))))).astype(BF)
        pre_ref[rows, :] = pre
        sums += jnp.sum(pre.astype(F32), axis=0, keepdims=True)
    sum_ref[...] = sums


def feed_forward(second, cot, up, bias, down, tile=256):
    total, width = second.shape
    units = up.shape[1]
    whole = pl.BlockSpec((total, width), lambda u: (0, 0))
    cols = pl.BlockSpec((total, tile), lambda u: (0, u))
    line = pl.BlockSpec((1, tile), lambda u: (0, u))
    return call(
        feed_kernel,
        [second, cot, up, bias, down],
        [shape((total, units)), shape((total, units)), shape((1, units), F32)],
        "feed",
        in_specs=[
            whole,
            whole,
            pl.BlockSpec((width, tile), lambda u: (0, u)),
            line,
            pl.BlockSpec((tile, width), lambda u: (u, 0)),
        ],
        out_specs=[cols, cols, line],
        flops=4 * total * width * units,
        grid=(units // tile,),
    )


def down_grads_kernel(pos, hidden, cot, far1, far2, n1, n2, own):
    g = pl.program_id(0)
    rows = own.shape[1]
    acc = dot32(hidden[...], cot[...], TN).astype(BF)
    for k, out in enumerate((None, n2, n1, own)):

        @pl.when(g == k)
        def _():
            for j in range(4):
                value = acc[j * rows : (j + 1) * rows, :]
                if k == 0:
                    (far1, far2)[j // 2][j % 2] = value
                else:
                    out[j] = value


def ring_shapes(rows, cols):
    return [shape((2, rows, cols))] * 2 + [shape((4, rows, cols))] * 3


def ring_specs(rows, cols):
    whole = lambda n: pl.BlockSpec((n, rows, cols), lambda g, pos: (0, 0, 0))
    return [whole(2)] * 2 + [whole(4)] * 3


def down_grads(pos, hidden, cot, rows, after):
    total, units = hidden.shape
    width = cot.shape[1]
    return placed_call(
        down_grads_kernel,
        pos,
        [hidden, cot],
        ring_shapes(rows, width),
        "down_grads",
        (4,),
        [
            pl.BlockSpec((total, units // 4), lambda g, pos: (0, pos[0] ^ (3 - g))),
            pl.BlockSpec((total, width), lambda g, pos: (0, 0)),
        ],
        ring_specs(rows, width),
        flops=2 * total * units * width,
        after=after,
    )


def z_places(z):
    return lax.rem(z + 2, 4), lax.rem(z + 1, 4), lax.rem(z + 3, 4), z


def split_ring(g, refs, store):
    far1, far2, n1, n2, own = refs
    for k, out in enumerate((None, n2, n1, own)):

        @pl.when(g == k)
        def _():
            for zz in range(4):
                if k:
                    store(out, zz, zz)
                else:
                    store((far1, far2)[zz // 2], zz % 2, zz)


def up_grads_kernel(pos, second, pre, *refs):
    lead = refs[-1].shape[1] // 2
    acc = dot32(second[...], pre[...], TN).astype(BF)

    def store(out, at, zz):
        for cc in range(2):
            start = (cc * 4 + zz) * lead
            out[at, cc * lead : (cc + 1) * lead, :] = acc[start : start + lead, :]

    split_ring(pl.program_id(0), refs, store)


def up_grads(pos, second, pre, lead, after):
    total, width = second.shape
    units = pre.shape[1]
    return placed_call(
        up_grads_kernel,
        pos,
        [second, pre],
        ring_shapes(2 * lead, units),
        "up_grads",
        (4,),
        [
            pl.BlockSpec((total, width // 4), lambda g, pos: (0, pos[0] ^ (3 - g))),
            pl.BlockSpec((total, units), lambda g, pos: (0, 0)),
        ],
        ring_specs(2 * lead, units),
        flops=2 * total * units * width,
        after=after,
    )


def attn_grads_kernel(pos, normed, grads, mixed, branch, *refs):
    lead = refs[-1].shape[1] // 8
    half = refs[-1].shape[2]
    accs = [dot32(normed[...], grads[j], TN).astype(BF) for j in range(3)]
    acco = dot32(mixed[...], branch[...], TN).astype(BF)

    def store(out, at, zz):
        for cc in range(2):
            for j, acc in enumerate(accs):
                row, start = (2 * j + cc) * lead, (cc * 4 + zz) * lead
                out[at, row : row + lead, :] = acc[start : start + lead, :]
            row = (6 + cc) * lead
            out[at, row : row + lead, :] = acco[
                zz * lead : (zz + 1) * lead, cc * half : (cc + 1) * half
            ]

    split_ring(pl.program_id(0), refs, store)


def attn_grads(pos, normed, grads, mixed, branch, lead, after):
    total, width = normed.shape
    half = width // 2
    return placed_call(
        attn_grads_kernel,
        pos,
        [normed, grads, mixed, branch],
        ring_shapes(8 * lead, half),
        "attn_grads",
        (4,),
        [
            pl.BlockSpec((total, width // 4), lambda g, pos: (0, pos[0] ^ (3 - g))),
            pl.BlockSpec((3, total, half), lambda g, pos: (0, 0, 0)),
            pl.BlockSpec((total, half // 4), lambda g, pos: (0, pos[0] ^ (3 - g))),
            pl.BlockSpec((total, width), lambda g, pos: (0, 0)),
        ],
        ring_specs(8 * lead, half),
        flops=8 * total * width * half,
        after=after,
    )


def pass_kernel(n1, n2, t1, t2, s1, s2):
    for s, n, t, part in ((s1, n1, t2, 1), (s2, n2, t1, 0)):
        for j in range(4):
            if j // 2 == part:
                s[j] = (n[j].astype(F32) + t[j % 2].astype(F32)).astype(BF)
            else:
                s[j] = n[j]


def far_round(ring):
    return send(ring[0], X_SWAP), send(ring[1], Y_SWAP)


def near_round(ring, got, name, after=()):
    s1, s2 = call(
        pass_kernel,
        [ring[2], ring[3], *got],
        [shape(ring[2].shape)] * 2,
        name + "_pass",
        after=after,
    )
    return s1, [send(s1, X_SWAP), send(s2, Y_SWAP)]


def joined_kernel(extra):
    def body(own, r1, r2, *refs):
        far1, far2, first, second, mine, acc = refs[extra:]
        rows = own.shape[1]
        for j in range(4):
            acc[j, :rows, :] = own[j].astype(F32) + r1[j].astype(F32) + r2[j].astype(F32)
            if extra:
                acc[j, rows:, :] = sum(ref[j].astype(F32) for ref in refs[:extra])
        far, one, two, me = z_places(place()[2])
        cut = far1.shape[0]
        far1[...] = acc[far, :cut, :].astype(BF)
        far2[...] = acc[far, cut:, :].astype(BF)
        first[...] = acc[one].astype(BF)
        second[...] = acc[two].astype(BF)
        mine[...] = acc[me]

    return body


def join(ring, got, name, extra=(), after=()):
    _, rows, cols = ring[4].shape
    rows += extra[0].shape[1] if extra else 0
    cut = rows // 2 // 16 * 16
    return call(
        joined_kernel(len(extra)),
        [ring[4], *got, *extra],
        [
            shape((cut, cols)),
            shape((rows - cut, cols)),
            shape((rows, cols)),
            shape((rows, cols)),
            shape((rows, cols), F32),
        ],
        name + "_join",
        scratch=[pltpu.VMEM((4, rows, cols), F32)],
        after=after,
    )


def inner_pass_kernel(p1, p2, t1, t2, p1o, p2o):
    cut = p1.shape[0] // 2 // 16 * 16
    plus = lambda a, got: (a.astype(F32) + got[...].astype(F32)).astype(BF)
    p1o[:cut, :] = plus(p1[:cut, :], t1)
    p1o[cut:, :] = p1[cut:, :]
    p2o[:cut, :] = p2[:cut, :]
    p2o[cut:, :] = plus(p2[cut:, :], t2)


def inner_far(joined):
    return send(joined[0], Z_UP), send(joined[1], Z_DOWN)


def inner_near(joined, came, name, after=()):
    p1, p2 = call(
        inner_pass_kernel,
        [joined[2], joined[3], *came],
        [shape(joined[2].shape)] * 2,
        name + "_inner",
        after=after,
    )
    return p1, [joined[4], send(p1, Z_UP), send(p2, Z_DOWN)]


def total_of(refs):
    return refs[0][...] + refs[1][...].astype(F32) + refs[2][...].astype(F32)


def feed_last_kernel(p0, p1, p2, q0, q1, q2, down, kept, given, acc):
    _, c, _ = place()
    down[...] = total_of((p0, p1, p2))
    acc[...] = total_of((q0, q1, q2))
    lead = kept.shape[0]
    kept[...] = acc[pl.ds(pl.multiple_of(c * lead, lead), lead), :]
    given[...] = acc[pl.ds(pl.multiple_of((1 - c) * lead, lead), lead), :]


def attn_last_kernel(p0, p1, p2, kept, given, out, small, acc):
    _, c, _ = place()
    acc[...] = total_of((p0, p1, p2))
    lead = kept.shape[1]
    half = kept.shape[2]
    for j in range(3):
        at = 2 * j * lead
        kept[j] = acc[pl.ds(pl.multiple_of(at + c * lead, lead), lead), :]
        given[j] = acc[pl.ds(pl.multiple_of(at + (1 - c) * lead, lead), lead), :]
    out[:, :half] = acc[6 * lead : 7 * lead, :]
    out[:, half:] = acc[7 * lead : 8 * lead, :]
    small[...] = acc[8 * lead :, :]


def norm_back(n, spread, gain, grad):
    g = grad * gain
    return spread * (
        g - jnp.mean(g, axis=-1, keepdims=True) - n * jnp.mean(g * n, axis=-1, keepdims=True)
    )


def column(values):
    return jnp.sum(values, axis=0, keepdims=True)


def middle_back_kernel(part, got, middle, cot, gain, wout, branch, mgrad, mixed, sums):
    n, spread = moments(middle[...])
    grad = part[...].astype(F32) + got[...].astype(F32)
    c32 = cot[...].astype(F32)
    value = c32 + norm_back(n, spread, gain[...], grad)
    mgrad[...] = value
    rounded = value.astype(BF)
    branch[...] = rounded
    mixed[...] = dot32(rounded, wout[...], NT).astype(BF)

    @pl.when(pl.program_id(0) == 0)
    def _():
        sums[...] = jnp.zeros_like(sums)

    for j, v in enumerate((grad * n, grad, rounded.astype(F32), c32)):
        sums[j : j + 1, :] += column(v)


def middle_back(part, got, middle, cot, gain, wout, after):
    total, width = middle.shape
    half = wout.shape[0]
    rows = pl.BlockSpec((BLOCK, width), lambda i: (i, 0))
    fixed = lambda dims: pl.BlockSpec(dims, lambda i: (0, 0))
    return call(
        middle_back_kernel,
        [part, got, middle, cot, gain, wout],
        [
            shape((total, width)),
            shape((total, width), F32),
            shape((total, half)),
            shape((4, width), F32),
        ],
        "middle_back",
        in_specs=[rows] * 4 + [fixed((1, width)), fixed((half, width))],
        out_specs=[
            rows,
            rows,
            pl.BlockSpec((BLOCK, half), lambda i: (i, 0)),
            fixed((4, width)),
        ],
        flops=2 * total * width * half,
        grid=(total // BLOCK,),
        after=after,
    )


def source_grad_kernel(grads, weight, out):
    out[...] = sum(dot32(grads[j], weight[j], NT) for j in range(3)).astype(BF)


def source_grad(grads, weight, after):
    _, total, half = grads.shape
    width = weight.shape[1]
    return call(
        source_grad_kernel,
        [grads, weight],
        [shape((total, width))],
        "source_grad",
        in_specs=[
            pl.BlockSpec((3, BLOCK, half), lambda i: (0, i, 0)),
            pl.BlockSpec((3, width, half), lambda i: (0, 0, 0)),
        ],
        out_specs=[pl.BlockSpec((BLOCK, width), lambda i: (i, 0))],
        flops=6 * total * width * half,
        grid=(total // BLOCK,),
        after=after,
    )[0]


def own_block(g, pos):
    _, c, z = pos[0], pos[1], pos[2]
    parity = lax.rem(z, 2)
    return jnp.where(g < 2, 2 * c + (parity ^ (g & 1)), 2 * (1 - c) + (g & 1))


def input_back_kernel(pos, part, got, x, mgrad, gain, first, again, sums):
    g = pl.program_id(0)
    n, spread = moments(x[...].astype(F32))
    grad = part[...].astype(F32) + got[...].astype(F32)
    value = (mgrad[...] + norm_back(n, spread, gain[...], grad)).astype(BF)

    @pl.when(g == 0)
    def _():
        first[...] = value
        sums[...] = jnp.zeros_like(sums)

    @pl.when(g == 1)
    def _():
        again[...] = value

    for j, v in enumerate((grad * n, grad)):
        sums[j : j + 1, :] += column(v)


def input_back(pos, part, got, x, mgrad, gain, after):
    total, width = x.shape
    rows = pl.BlockSpec((BLOCK, width), lambda g, pos: (own_block(g, pos), 0))
    fixed = lambda n: pl.BlockSpec((n, width), lambda g, pos: (0, 0))
    return placed_call(
        input_back_kernel,
        pos,
        [part, got, x, mgrad, gain],
        [shape((BLOCK, width))] * 2 + [shape((2, width), F32)],
        "input_back",
        (total // BLOCK,),
        [rows] * 4 + [fixed(1)],
        [fixed(BLOCK), fixed(BLOCK), fixed(2)],
        after=after,
    )


def other_block(g, pos):
    return jnp.where(g < 2, 2 * (1 - pos[1]) + (g & 1), 2 * pos[1] + (g & 1))


def output_kernel(pos, hidden, down, middle, bias, theirs, mine):
    g = pl.program_id(0)
    value = dot32(hidden[...], down[...], NN)

    @pl.when(g < 2)
    def _():
        theirs[...] = value.astype(BF)

    @pl.when(g >= 2)
    def _():
        mine[...] = value + middle[...] + bias[...]


def output_rows(pos, hidden, down, middle, bias, after):
    total, units = hidden.shape
    width = down.shape[1]
    return placed_call(
        output_kernel,
        pos,
        [hidden, down, middle, bias],
        [shape((total // 2, width)), shape((total // 2, width), F32)],
        "output_rows",
        (4,),
        [
            pl.BlockSpec((BLOCK, units), lambda g, pos: (other_block(g, pos), 0)),
            pl.BlockSpec((units, width), lambda g, pos: (0, 0)),
            pl.BlockSpec((BLOCK, width), lambda g, pos: (other_block(g, pos), 0)),
            pl.BlockSpec((1, width), lambda g, pos: (0, 0)),
        ],
        [
            pl.BlockSpec((BLOCK, width), lambda g, pos: (jnp.minimum(g, 1), 0)),
            pl.BlockSpec((BLOCK, width), lambda g, pos: (jnp.maximum(g - 2, 0), 0)),
        ],
        flops=2 * total * units * width,
        after=after,
    )


def result_kernel(mine, got, first, again):
    _, _, z = place()
    parity = lax.rem(z, 2)
    for k, out in enumerate((first, again)):
        at = pl.multiple_of((parity ^ k) * BLOCK, BLOCK)
        out[...] = (mine[pl.ds(at, BLOCK), :] + got[pl.ds(at, BLOCK), :].astype(F32)).astype(BF)

XY_FAR = links(lambda o, c, z: (o ^ 3, c, z))


def fast_local(
    inputs,
    segment_ids,
    first_gain,
    first_shift,
    query_weight,
    query_bias,
    key_weight,
    value_weight,
    value_bias,
    out_weight,
    out_bias,
    second_gain,
    second_shift,
    up_weight,
    up_bias,
    down_weight,
    down_bias,
    cotangent,
):
    batch, rows, width = inputs.shape
    o, c, z = place()
    pos = jnp.stack([o, c, z]).astype(jnp.int32)
    total = batch * rows * 2
    half = width // 2
    units = up_weight.shape[1] // 2
    lead = query_weight.shape[0]
    down_rows = down_weight.shape[0]
    size = width // H
    vector_list = [
        first_gain,
        first_shift,
        query_bias,
        value_bias,
        out_bias,
        second_gain,
        second_shift,
        down_bias,
        up_bias,
    ]
    count = 8 * lead + down_rows

    small, at = jnp.zeros((half,), BF), 0
    for vector in vector_list:
        small = small + jnp.pad(vector, (at, half - at - vector.shape[0]))
        at += vector.shape[0]
    small = jnp.pad(small.reshape(1, half), ((0, 7), (0, 0)))
    weights = [query_weight, key_weight, value_weight]
    far, up_far = call(
        first_kernel,
        weights + [up_weight, small],
        [shape((3 * lead + 8, half)), shape((lead, units))],
        "first",
    )
    attn_pay, up_pay = call(
        second_kernel,
        weights + [up_weight, small, send(far, CORE_SWAP), send(up_far, CORE_SWAP)],
        [shape((6 * lead + 16, half)), shape((2 * lead, units))],
        "second",
    )

    pa, pb = ring_first(attn_pay, Z_UP, Z_DOWN)
    pc = ring_second(pa, pb, Z_UP, Z_DOWN)
    attn_all, down_own = copies(
        [attn_pay, pa, pb, *pc, down_weight, out_weight],
        [shape((4,) + attn_pay.shape), shape((down_rows + lead, width))],
        lambda ins, outs: inner_moves(ins, outs)
        + [
            (ins[5], outs[1].at[pl.ds(0, down_rows)]),
            (ins[6], outs[1].at[pl.ds(down_rows, lead)]),
        ],
        7,
        "attn_inner",
    )
    aa, ab = ring_first(attn_all, X_SWAP, Y_SWAP)
    da, db = ring_first(down_own, Z_UP, Z_DOWN)
    dc = ring_second(da, db, Z_UP, Z_DOWN)
    ac = ring_outer_second(aa, ab, Y_SWAP, X_SWAP)

    in0, in1 = call(
        inputs_kernel,
        [inputs, segment_ids],
        [shape((rows + 16, width))] * 2,
        "inputs_own",
        in_specs=[ANY, VMEM],
        scratch=[pltpu.SemaphoreType.DMA((2,))],
        after=[aa, ab, *dc],
    )
    got = [send(in0, SEQUENCE[0]), send(in1, SEQUENCE[1])]

    def sequence_moves(ins, outs):
        _, cc, zz = place()
        parity = lax.rem(zz, 2)
        todo = []
        for m in range(2):
            for k in range(2):
                piece = ins[2 * m + k]
                at = (1 - cc if m else cc, parity ^ k)
                todo.append((piece.at[pl.ds(0, rows)], outs[0].at[at]))
                if len(outs) > 1:
                    todo.append((piece.at[pl.ds(rows, 16)], outs[1].at[at]))
        return todo + ([(ins[4], outs[2])] if len(outs) > 1 else [])

    def whole_sequence(pieces, name, after=(), more=()):
        outs = [shape((2, 2, rows, width))]
        if more:
            outs += [shape((2, 2, 16, width)), shape(more[0].shape)]
        return copies(
            pieces + list(more), outs, sequence_moves, 9 if more else 4, name, after=after
        )

    down_all = copies(
        [down_own, da, db, *dc],
        [shape((4,) + down_own.shape)],
        inner_moves,
        5,
        "down_inner",
        after=[*ac, in0],
    )[0]
    ea, eb = ring_first(down_all, X_SWAP, Y_SWAP)
    *got, _ = lax.optimization_barrier((*got, down_all))
    x, segments, up_own = whole_sequence(
        got + [send(g, CORE_SWAP) for g in got], "inputs_whole", more=[up_pay]
    )
    x = x.reshape(total, width)
    segments = segments[:, :, 0, :rows].reshape(total).astype(F32)
    seg_col, seg_row = segments.reshape(total, 1), segments.reshape(1, total)

    ua, ub = ring_first(up_own, Z_UP, Z_DOWN)

    def attn_blocks(src, outs, yx, zz):
        todo = [
            (src.at[pl.ds((2 * j + cc) * lead, lead)], outs[0].at[j, yx, cc, zz])
            for j in range(3)
            for cc in range(2)
        ]
        return todo + [(src.at[pl.ds(6 * lead, 16)], outs[1].at[yx, zz])]

    wqkv, small_all = copies(
        [attn_all, aa, ab, *ac],
        [shape((3, 4, 2, 4, lead, half)), shape((4, 4, 16, half))],
        lambda ins, outs: final_moves(ins, outs, attn_blocks),
        16 * 7,
        "attn_whole",
        after=[down_all],
    )
    wqkv = wqkv.reshape(3, width, half)

    small_all = small_all.reshape(4, 4, 2, 8, half)[:, :, :, 0, :count]
    vectors = small_all[..., : 8 * lead].reshape(4, 4, 2, 8, lead).transpose(3, 0, 2, 1, 4)
    own_cols = lax.dynamic_index_in_dim(vectors, c, 2, keepdims=False).reshape(8, half)
    vectors = vectors.reshape(8, width).astype(F32)
    line = lambda j: vectors[j : j + 1]
    gain1, shift1, bias_o, gain2, shift2, bias_d = [line(j) for j in (0, 1, 4, 5, 6, 7)]
    qkv_bias = jnp.stack([own_cols[2], jnp.zeros_like(own_cols[2]), own_cols[3]]).astype(F32)
    bias_u = lax.dynamic_index_in_dim(small_all[..., 8 * lead :], c, 2, keepdims=False)
    bias_u = bias_u.reshape(1, units).astype(F32)

    normed, qkv = project(x, gain1, shift1, wqkv, qkv_bias, [])
    uc = ring_second(ua, ub, Z_UP, Z_DOWN)

    def cotangent_moves(ins, outs):
        parity = lax.rem(place()[2], 2)
        return [(ins[0].at[parity], outs[0]), (ins[0].at[1 - parity], outs[1])]

    cots = copies(
        [cotangent],
        [shape((rows, width))] * 2,
        cotangent_moves,
        2,
        "cotangent_own",
        after=[*uc, normed],
    )
    cot_got = [send(block, pairs) for block, pairs in zip(cots, SEQUENCE)]
    ec = ring_outer_second(ea, eb, Y_SWAP, X_SWAP)
    up_all = copies(
        [up_own, ua, ub, *uc],
        [shape((4,) + up_pay.shape)],
        inner_moves,
        5,
        "up_inner",
        after=[*ec, normed],
    )[0]
    heads = attend(qkv, seg_col, seg_row, size, 0, [], [up_all, *cots])
    mixed, log = attend(qkv, seg_col, seg_row, size, 1, heads, [])
    fa, fb = ring_first(up_all, X_SWAP, Y_SWAP)

    def down_blocks(src, outs, yx, zz):
        return [
            (src.at[pl.ds(0, down_rows)], outs[0].at[yx, zz]),
            (src.at[pl.ds(down_rows, lead)], outs[1].at[yx, zz]),
        ]

    wdown, wout = copies(
        [down_all, ea, eb, *ec],
        [shape((4, 4, down_rows, width)), shape((4, 4, lead, width))],
        lambda ins, outs: final_moves(ins, outs, down_blocks),
        32,
        "down_whole",
        after=[mixed],
    )
    wdown, wout = wdown.reshape(units, width), wout.reshape(half, width)
    part = rows_matmul(mixed, wout, NN, "attend_out", after=[fa, fb, *cot_got])
    middle, second = middle_norm(x, part, send(part, CORE_SWAP), bias_o, gain2, shift2)
    cot = whole_sequence(
        cot_got + [send(g, CORE_SWAP) for g in cot_got], "cotangent_whole", [part]
    )[0].reshape(total, width)

    def up_blocks(src, outs, yx, zz):
        return [(src.at[pl.ds(cc * lead, lead)], outs[0].at[yx, cc, zz]) for cc in range(2)]

    wup = copies(
        [up_all, fa, fb, *ring_outer_second(fa, fb, Y_SWAP, X_SWAP)],
        [shape((4, 2, 4, lead, units))],
        lambda ins, outs: final_moves(ins, outs, up_blocks),
        32,
        "up_whole",
        after=[second],
    )[0].reshape(width, units)
    hidden, pre_grad, up_bias_grad = feed_forward(second, cot, wup, bias_u, wdown)

    def to_tokens(got):
        return jnp.where((z & 1) == 0, jnp.stack(got), jnp.stack(got[::-1]))

    theirs, mine = output_rows(pos, hidden, wdown, middle, bias_d, [])
    part = rows_matmul(pre_grad, wup, NT, "second_grad", after=[mine])
    d = down_grads(pos, hidden, cot, down_rows, [part])
    d_far = far_round(d)
    u = up_grads(pos, second, pre_grad, lead, [d[4]])
    u_far = far_round(u)
    passed, d_got = near_round(d, d_far, "down", [u[4]])
    blocks = call(
        result_kernel,
        [mine, send(theirs, CORE_SWAP)],
        [shape((rows, width))] * 2,
        "result",
        after=[passed],
    )
    out_got = [send(block, pairs) for block, pairs in zip(blocks, SEQUENCE)]
    branch, middle_grad, mixed_grad, sums2 = middle_back(
        part, send(part, CORE_SWAP), middle, cot, gain2, wout, [blocks[0]]
    )

    passed, u_got = near_round(u, u_far, "up", [branch])
    back = attend_back(qkv, log, mixed_grad, seg_col, seg_row, size, 0, [], [passed])
    output = to_tokens(out_got)
    d_joined = join(d, d_got, "down", after=[back[1]])
    d_came = inner_far(d_joined)
    grads, qv_bias_grad = attend_back(
        qkv, log, mixed_grad, seg_col, seg_row, size, 1, back, [d_joined[4]]
    )
    passed, d_last = inner_near(d_joined, d_came, "down", [qv_bias_grad, *out_got])
    u_joined = list(join(u, u_got, "up", after=[passed]))
    part = source_grad(grads, wqkv, [u_joined[4]])
    got = send(part, CORE_SWAP)
    a = attn_grads(pos, normed, grads, mixed, branch, lead, [part])
    a_far = far_round(a)
    in0, in1, sums1 = input_back(pos, part, got, x, middle_grad, gain1, [a[4], *d_last[1:]])
    in_got = [send(block, pairs) for block, pairs in zip((in0, in1), SEQUENCE)]
    input_grad = to_tokens(in_got).astype(F32)

    wide = jnp.stack([sums1[0], sums1[1], sums2[2], sums2[0], sums2[1], sums2[3]])
    wide = lax.dynamic_index_in_dim(wide.reshape(6, 4, 2, 4, lead), c, 2, keepdims=False)
    wide = jnp.concatenate(
        [wide[:2], qv_bias_grad.reshape(2, 4, 4, lead), wide[2:]], axis=0
    ).transpose(2, 1, 0, 3)
    tiny = jnp.concatenate(
        [
            wide.reshape(4, 4, 8 * lead),
            up_bias_grad.reshape(4, 4, down_rows).transpose(1, 0, 2),
        ],
        axis=-1,
    ).astype(BF)
    tiny = jnp.pad(tiny[:, :, None], ((0, 0), (0, 0), (0, 15), (0, half - count)))
    pick = lambda k: lax.dynamic_index_in_dim(tiny, o ^ k, 1, keepdims=False)
    extra = [pick(0), send(pick(1), X_SWAP), send(pick(2), Y_SWAP), send(pick(3), XY_FAR)]

    passed, a_got = near_round(a, a_far, "attn", [in0, *extra[1:]])
    joined = join(a, a_got, "attn", extra, in_got)
    came = inner_far(joined)
    *u_joined[:2], _ = lax.optimization_barrier((*u_joined[:2], joined[4]))
    u_came = inner_far(u_joined)
    passed, attn_last = inner_near(joined, came, "attn")
    _, u_last = inner_near(u_joined, u_came, "up", [passed])
    qkv_kept, qkv_given, out_out, small_sum = call(
        attn_last_kernel,
        attn_last,
        [shape((3, lead, half), F32)] * 2 + [shape((lead, width), F32), shape((16, half), F32)],
        "attn_last",
        scratch=[pltpu.VMEM((8 * lead + 16, half), F32)],
    )

    down_out, up_kept, up_given = call(
        feed_last_kernel,
        d_last + u_last,
        [shape(down_weight.shape, F32)] + [shape((lead, units), F32)] * 2,
        "feed_last",
        scratch=[pltpu.VMEM((2 * lead, units), F32)],
        after=[small_sum],
    )

    def whole_columns(kept, got):
        cols = kept.shape[-1] // 4
        kept, got = [a.reshape(a.shape[:-1] + (4, 1, cols)) for a in (kept, got)]
        both = jnp.where(
            c == 0, jnp.concatenate([kept, got], -2), jnp.concatenate([got, kept], -2)
        )
        return both.reshape(both.shape[:-3] + (8 * cols,))

    up_out = whole_columns(up_kept, send(up_given, CORE_SWAP))
    qkv_out = whole_columns(qkv_kept, send(qkv_given, CORE_SWAP))
    small_sum = small_sum[0]
    vec = lambda j: small_sum[j * lead : (j + 1) * lead]
    return (
        output,
        input_grad,
        vec(0),
        vec(1),
        qkv_out[0],
        vec(2),
        qkv_out[1],
        qkv_out[2],
        vec(3),
        out_out,
        vec(4),
        vec(5),
        vec(6),
        up_out,
        small_sum[8 * lead : count],
        down_out,
        vec(7),
    )


def solution(mesh):
    fast = mesh.shape["dp"] == 8 and mesh.shape["ctx"] == 4
    return jax.shard_map(
        fast_local if fast else local,
        mesh=mesh,
        in_specs=(
            P("dp", "ctx", None),
            P("dp", "ctx"),
            P(("dp", "ctx")),
            P(("dp", "ctx")),
            P(("dp", "ctx"), None),
            P(("dp", "ctx")),
            P(("dp", "ctx"), None),
            P(("dp", "ctx"), None),
            P(("dp", "ctx")),
            P(("dp", "ctx"), None),
            P(("dp", "ctx")),
            P(("dp", "ctx")),
            P(("dp", "ctx")),
            P(("dp", "ctx"), None),
            P(("dp", "ctx")),
            P(("dp", "ctx"), None),
            P(("dp", "ctx")),
            P("dp", "ctx", None),
        ),
        out_specs=(
            P("dp", "ctx", None),
            P("dp", "ctx", None),
            P(("dp", "ctx")),
            P(("dp", "ctx")),
            P(("dp", "ctx"), None),
            P(("dp", "ctx")),
            P(("dp", "ctx"), None),
            P(("dp", "ctx"), None),
            P(("dp", "ctx")),
            P(("dp", "ctx"), None),
            P(("dp", "ctx")),
            P(("dp", "ctx")),
            P(("dp", "ctx")),
            P(("dp", "ctx"), None),
            P(("dp", "ctx")),
            P(("dp", "ctx"), None),
            P(("dp", "ctx")),
        ),
        check_vma=False,
    )
```

```python
from functools import partial
import math

import jax
import jax.numpy as jnp
from jax import lax
from jax.experimental import pallas as pl
from jax.experimental.pallas import tpu as pltpu
from jax.sharding import PartitionSpec as P

H = 16


EPS = 1e-05
MASKED = -1e30


def normalize(values, gain, shift):
    mean = jnp.mean(values, axis=-1, keepdims=True)
    centered = values - mean
    spread = jnp.mean(centered * centered, axis=-1, keepdims=True)
    return centered * lax.rsqrt(spread + EPS) * gain + shift


def product(left, right):
    return jnp.einsum("btd,de->bte", left, right, preferred_element_type=jnp.float32)


def product_back(left, right):
    return jnp.einsum("bte,de->btd", left, right, preferred_element_type=jnp.float32)


def outer_sum(left, right):
    return jnp.einsum("btd,bte->de", left, right, preferred_element_type=jnp.float32)


def column_sum(values):
    return jnp.sum(values.astype(jnp.float32), axis=(0, 1))


def gather_attention(
    first_gain,
    first_shift,
    query_weight,
    query_bias,
    key_weight,
    value_weight,
    value_bias,
    out_weight,
    out_bias,
):
    return (
        lax.all_gather(first_gain, ("dp", "ctx"), axis=0, tiled=True),
        lax.all_gather(first_shift, ("dp", "ctx"), axis=0, tiled=True),
        lax.all_gather(query_weight, ("dp", "ctx"), axis=0, tiled=True),
        lax.all_gather(query_bias, ("dp", "ctx"), axis=0, tiled=True),
        lax.all_gather(key_weight, ("dp", "ctx"), axis=0, tiled=True),
        lax.all_gather(value_weight, ("dp", "ctx"), axis=0, tiled=True),
        lax.all_gather(value_bias, ("dp", "ctx"), axis=0, tiled=True),
        lax.all_gather(out_weight, ("dp", "ctx"), axis=0, tiled=True),
        lax.all_gather(out_bias, ("dp", "ctx"), axis=0, tiled=True),
    )


def gather_feed(second_gain, second_shift, up_weight, up_bias, down_weight, down_bias):
    return (
        lax.all_gather(second_gain, ("dp", "ctx"), axis=0, tiled=True),
        lax.all_gather(second_shift, ("dp", "ctx"), axis=0, tiled=True),
        lax.all_gather(up_weight, ("dp", "ctx"), axis=0, tiled=True),
        lax.all_gather(up_bias, ("dp", "ctx"), axis=0, tiled=True),
        lax.all_gather(down_weight, ("dp", "ctx"), axis=0, tiled=True),
        lax.all_gather(down_bias, ("dp", "ctx"), axis=0, tiled=True),
    )


def gather_keys(keys, values, segments):
    return (
        lax.all_gather(keys, "ctx", axis=1, tiled=True),
        lax.all_gather(values, "ctx", axis=1, tiled=True),
        lax.all_gather(segments, "ctx", axis=1, tiled=True),
    )


def score_block(queries, keys_all, segments, segments_all):
    batch, rows, width = queries.shape
    size = width // H
    total_len = keys_all.shape[1]
    query_heads = queries.reshape(batch, rows, H, size)
    key_heads = keys_all.reshape(batch, total_len, H, size)
    raw = jnp.einsum("bqhd,bkhd->bhqk", query_heads, key_heads, preferred_element_type=jnp.float32)
    scores = raw * (1.0 / math.sqrt(size))
    offset = lax.axis_index("ctx") * rows
    query_pos = offset + jnp.arange(rows, dtype=jnp.int32)
    key_pos = jnp.arange(total_len, dtype=jnp.int32)
    causal = key_pos[None, :] <= query_pos[:, None]
    same_doc = segments[:, :, None] == segments_all[:, None, :]
    allowed = (causal[None] & same_doc)[:, None]
    return jnp.where(allowed, scores, MASKED)


def forward_part(inputs, segments, attn, feed):
    (
        first_gain,
        first_shift,
        query_weight,
        query_bias,
        key_weight,
        value_weight,
        value_bias,
        out_weight,
        out_bias,
    ) = attn
    second_gain, second_shift, up_weight, up_bias, down_weight, down_bias = feed
    batch, rows, width = inputs.shape
    size = width // H
    source = inputs.astype(jnp.float32)
    normed = normalize(
        source, first_gain.astype(jnp.float32), first_shift.astype(jnp.float32)
    ).astype(jnp.bfloat16)
    queries = (product(normed, query_weight) + query_bias.astype(jnp.float32)).astype(jnp.bfloat16)
    keys = product(normed, key_weight).astype(jnp.bfloat16)
    values = (product(normed, value_weight) + value_bias.astype(jnp.float32)).astype(jnp.bfloat16)
    keys_all, values_all, segments_all = gather_keys(keys, values, segments)
    scores = score_block(queries, keys_all, segments, segments_all)
    top = jnp.max(scores, axis=-1, keepdims=True)
    expo = jnp.exp(scores - top)
    row_total = jnp.sum(expo, axis=-1, keepdims=True)
    probs = (expo / row_total).astype(jnp.bfloat16)
    log_total = top + jnp.log(row_total)
    value_heads = values_all.reshape(batch, values_all.shape[1], H, size)
    mixed = jnp.einsum("bhqk,bkhd->bqhd", probs, value_heads, preferred_element_type=jnp.float32)
    mixed = mixed.reshape(batch, rows, width).astype(jnp.bfloat16)
    middle = source + product(mixed, out_weight) + out_bias.astype(jnp.float32)
    second = normalize(
        middle, second_gain.astype(jnp.float32), second_shift.astype(jnp.float32)
    ).astype(jnp.bfloat16)
    hidden_pre = product(second, up_weight) + up_bias.astype(jnp.float32)
    hidden = jax.nn.gelu(hidden_pre, approximate=False).astype(jnp.bfloat16)
    output = (middle + product(hidden, down_weight) + down_bias.astype(jnp.float32)).astype(
        jnp.bfloat16
    )
    kept = (
        source,
        normed,
        queries,
        keys,
        values,
        log_total,
        mixed,
        middle,
        second,
        hidden_pre,
        hidden,
    )
    return (output, kept, (keys_all, values_all, segments_all))


def backward_part(kept, gathered, segments, cotangent, attn, feed):
    (
        first_gain,
        first_shift,
        query_weight,
        query_bias,
        key_weight,
        value_weight,
        value_bias,
        out_weight,
        out_bias,
    ) = attn
    second_gain, second_shift, up_weight, up_bias, down_weight, down_bias = feed
    source, normed, queries, keys, values, log_total, mixed, middle, second, hidden_pre, hidden = (
        kept
    )
    keys_all, values_all, segments_all = gathered
    batch, rows, width = source.shape
    size = width // H
    total_len = keys_all.shape[1]
    scale = 1.0 / math.sqrt(size)
    down_grad = outer_sum(hidden, cotangent)
    down_bias_grad = column_sum(cotangent)
    hidden_grad = product_back(cotangent, down_weight)
    _, gelu_back = jax.vjp(partial(jax.nn.gelu, approximate=False), hidden_pre)
    pre_grad = gelu_back(hidden_grad)[0].astype(jnp.bfloat16)
    up_grad = outer_sum(second, pre_grad)
    up_bias_grad = column_sum(pre_grad)
    second_grad = product_back(pre_grad, up_weight)
    _, second_back = jax.vjp(
        normalize, middle, second_gain.astype(jnp.float32), second_shift.astype(jnp.float32)
    )
    middle_part, second_gain_grad, second_shift_grad = second_back(second_grad)
    feed_grads = (
        lax.psum_scatter(second_gain_grad, ("dp", "ctx"), scatter_dimension=0, tiled=True),
        lax.psum_scatter(second_shift_grad, ("dp", "ctx"), scatter_dimension=0, tiled=True),
        lax.psum_scatter(up_grad, ("dp", "ctx"), scatter_dimension=0, tiled=True),
        lax.psum_scatter(up_bias_grad, ("dp", "ctx"), scatter_dimension=0, tiled=True),
        lax.psum_scatter(down_grad, ("dp", "ctx"), scatter_dimension=0, tiled=True),
        lax.psum_scatter(down_bias_grad, ("dp", "ctx"), scatter_dimension=0, tiled=True),
    )
    middle_grad = cotangent.astype(jnp.float32) + middle_part
    branch_grad = middle_grad.astype(jnp.bfloat16)
    out_grad = outer_sum(mixed, branch_grad)
    out_bias_grad = column_sum(branch_grad)
    mixed_grad = product_back(branch_grad, out_weight).astype(jnp.bfloat16)
    scores = score_block(queries, keys_all, segments, segments_all)
    probs_full = jnp.exp(scores - log_total)
    probs = probs_full.astype(jnp.bfloat16)
    grad_heads = mixed_grad.reshape(batch, rows, H, size)
    query_heads = queries.reshape(batch, rows, H, size)
    key_heads = keys_all.reshape(batch, total_len, H, size)
    value_heads = values_all.reshape(batch, total_len, H, size)
    value_grad_all = jnp.einsum(
        "bhqk,bqhd->bkhd", probs, grad_heads, preferred_element_type=jnp.float32
    )
    prob_grad = jnp.einsum(
        "bqhd,bkhd->bhqk", grad_heads, value_heads, preferred_element_type=jnp.float32
    )
    delta = jnp.sum(probs_full * prob_grad, axis=-1, keepdims=True)
    score_grad = (probs_full * (prob_grad - delta)).astype(jnp.bfloat16)
    query_grad = (
        jnp.einsum("bhqk,bkhd->bqhd", score_grad, key_heads, preferred_element_type=jnp.float32)
        * scale
    )
    query_grad = query_grad.reshape(batch, rows, width).astype(jnp.bfloat16)
    key_grad_all = (
        jnp.einsum("bhqk,bqhd->bkhd", score_grad, query_heads, preferred_element_type=jnp.float32)
        * scale
    )
    key_sum, value_sum = (
        lax.psum_scatter(
            key_grad_all.reshape(batch, total_len, width).astype(jnp.bfloat16),
            "ctx",
            scatter_dimension=1,
            tiled=True,
        ).astype(jnp.float32),
        lax.psum_scatter(
            value_grad_all.reshape(batch, total_len, width).astype(jnp.bfloat16),
            "ctx",
            scatter_dimension=1,
            tiled=True,
        ).astype(jnp.float32),
    )
    key_grad = key_sum.astype(jnp.bfloat16)
    value_grad = value_sum.astype(jnp.bfloat16)
    query_weight_grad = outer_sum(normed, query_grad)
    query_bias_grad = column_sum(query_grad)
    key_weight_grad = outer_sum(normed, key_grad)
    value_weight_grad = outer_sum(normed, value_grad)
    value_bias_grad = column_sum(value_grad)
    normed_grad = (
        product_back(query_grad, query_weight)
        + product_back(key_grad, key_weight)
        + product_back(value_grad, value_weight)
    )
    _, first_back = jax.vjp(
        normalize, source, first_gain.astype(jnp.float32), first_shift.astype(jnp.float32)
    )
    input_part, first_gain_grad, first_shift_grad = first_back(normed_grad)
    input_grad = middle_grad + input_part
    attn_grads = (
        lax.psum_scatter(first_gain_grad, ("dp", "ctx"), scatter_dimension=0, tiled=True),
        lax.psum_scatter(first_shift_grad, ("dp", "ctx"), scatter_dimension=0, tiled=True),
        lax.psum_scatter(query_weight_grad, ("dp", "ctx"), scatter_dimension=0, tiled=True),
        lax.psum_scatter(query_bias_grad, ("dp", "ctx"), scatter_dimension=0, tiled=True),
        lax.psum_scatter(key_weight_grad, ("dp", "ctx"), scatter_dimension=0, tiled=True),
        lax.psum_scatter(value_weight_grad, ("dp", "ctx"), scatter_dimension=0, tiled=True),
        lax.psum_scatter(value_bias_grad, ("dp", "ctx"), scatter_dimension=0, tiled=True),
        lax.psum_scatter(out_grad, ("dp", "ctx"), scatter_dimension=0, tiled=True),
        lax.psum_scatter(out_bias_grad, ("dp", "ctx"), scatter_dimension=0, tiled=True),
    )
    return (input_grad, attn_grads, feed_grads)


def local(
    inputs,
    segment_ids,
    first_gain,
    first_shift,
    query_weight,
    query_bias,
    key_weight,
    value_weight,
    value_bias,
    out_weight,
    out_bias,
    second_gain,
    second_shift,
    up_weight,
    up_bias,
    down_weight,
    down_bias,
    cotangent,
):
    attn = gather_attention(
        first_gain,
        first_shift,
        query_weight,
        query_bias,
        key_weight,
        value_weight,
        value_bias,
        out_weight,
        out_bias,
    )
    feed = gather_feed(second_gain, second_shift, up_weight, up_bias, down_weight, down_bias)
    output, kept, gathered = forward_part(inputs, segment_ids, attn, feed)
    key_set = gather_keys(kept[3], kept[4], segment_ids)
    input_grad, attn_grads, feed_grads = backward_part(
        kept, key_set, segment_ids, cotangent, attn, feed
    )
    result = (output, input_grad)
    return result + tuple(attn_grads) + tuple(feed_grads)


AXES = ("dp", "ctx")
BLOCK = 256
BF = jnp.bfloat16
F32 = jnp.float32
NT = (((1,), (1,)), ((), ()))
NN = (((1,), (0,)), ((), ()))
TN = (((0,), (0,)), ((), ()))
ANY = pl.BlockSpec(memory_space=pl.ANY)
VMEM = pl.BlockSpec(memory_space=pltpu.VMEM)


def links(step):
    pairs = []
    for o in range(4):
        for c in range(2):
            for z in range(4):
                o2, c2, z2 = step(o, c, z)
                pairs.append(((o * 2 + c) * 4 + z, (o2 * 2 + c2) * 4 + z2))
    return pairs


X_SWAP = links(lambda o, c, z: (o ^ 1, c, z))
Y_SWAP = links(lambda o, c, z: (o ^ 2, c, z))
CORE_SWAP = links(lambda o, c, z: (o, 1 - c, z))
Z_UP = links(lambda o, c, z: (o, c, (z + 1) % 4))
Z_DOWN = links(lambda o, c, z: (o, c, (z + 3) % 4))
SEQUENCE = [links(lambda o, c, z, k=k: (o, z >> 1, 2 * c + ((z & 1) ^ k))) for k in range(2)]


def send(value, pairs):
    return lax.ppermute(value, AXES, pairs)


def place():
    dp = lax.axis_index("dp")
    return dp // 2, dp % 2, lax.axis_index("ctx")


def dot32(left, right, dims):
    return lax.dot_general(left, right, dims, preferred_element_type=F32)


def shape(dims, kind=BF):
    return jax.ShapeDtypeStruct(dims, kind)


def cost(flops, nbytes, special=0):
    return pl.CostEstimate(flops=int(flops), bytes_accessed=int(nbytes), transcendentals=special)


def moved_bytes(arrays):
    return sum(math.prod(a.shape) * jnp.dtype(a.dtype).itemsize for a in arrays)


def without(body, lead, count):
    return (lambda *refs: body(*refs[:lead], *refs[lead + count :])) if count else body


def call(
    body,
    ins,
    outs,
    name,
    in_specs=None,
    out_specs=None,
    scratch=(),
    flops=0,
    grid=(),
    after=(),
    aliases={},
):
    return pl.pallas_call(
        without(body, len(ins), len(after)),
        grid=grid,
        in_specs=list(in_specs or [VMEM] * len(ins)) + [ANY] * len(after),
        out_specs=out_specs or [VMEM] * len(outs),
        out_shape=outs,
        scratch_shapes=list(scratch),
        cost_estimate=cost(flops, moved_bytes(ins) + moved_bytes(outs)),
        input_output_aliases=aliases,
        name=name,
    )(*ins, *after)


def placed_call(
    body, pos, ins, outs, name, grid, in_specs, out_specs, scratch=(), flops=0, after=()
):
    return pl.pallas_call(
        without(body, len(ins) + 1, len(after)),
        grid_spec=pltpu.PrefetchScalarGridSpec(
            num_scalar_prefetch=1,
            grid=grid,
            in_specs=list(in_specs) + [ANY] * len(after),
            out_specs=out_specs,
            scratch_shapes=list(scratch),
        ),
        out_shape=outs,
        cost_estimate=cost(flops, moved_bytes(ins) + moved_bytes(outs)),
        name=name,
    )(pos, *ins, *after)


def copies(ins, outs, moves, count, name, after=()):
    def body(*refs):
        sems = refs[-1]
        todo = moves(refs[: len(ins)], refs[len(ins) : -1])
        started = [pltpu.make_async_copy(s, d, sems.at[i]) for i, (s, d) in enumerate(todo)]
        for copy in started:
            copy.start()
        for copy in started:
            copy.wait()

    return call(
        body,
        ins,
        outs,
        name,
        in_specs=[ANY] * len(ins),
        scratch=[pltpu.SemaphoreType.DMA((count,))],
        after=after,
    )


def own_columns(weight, k):
    n = weight.shape[1] // 8
    parts = [
        jnp.where(k == 0, weight[:, 2 * g * n : (2 * g + 1) * n], weight[:, (2 * g + 1) * n : (2 * g + 2) * n])
        for g in range(4)
    ]
    return jnp.concatenate(parts, axis=1)


def first_kernel(qw, kw, vw, uw, small, far, up_far):
    _, c, _ = place()
    lead = qw.shape[0]
    for j, ref in enumerate((qw, kw, vw)):
        far[j * lead : (j + 1) * lead, :] = own_columns(ref[...], 1 - c)
    far[3 * lead :, :] = small[...]
    up_far[...] = own_columns(uw[...], 1 - c)


def inputs_kernel(inputs, segs, in0, in1, sems):
    rows = inputs.shape[1]
    parity = lax.rem(place()[2], 2)
    todo = []
    for k, out in enumerate((in0, in1)):
        pick = parity if k == 0 else 1 - parity
        todo.append(pltpu.make_async_copy(inputs.at[pick], out.at[pl.ds(0, rows)], sems.at[k]))
        todo[-1].start()
        line = segs[pl.ds(pick, 1), :].astype(F32)
        out[rows:, :] = jnp.zeros((out.shape[0] - rows, out.shape[1]), BF)
        out[rows:, :rows] = jnp.broadcast_to(line, (out.shape[0] - rows, rows)).astype(BF)
    for copy in todo:
        copy.wait()


def second_kernel(qw, kw, vw, uw, small, far, up_far, attn, up):
    _, c, _ = place()
    lead = qw.shape[0]

    def both(out, at, own, got):
        n = own.shape[0]
        out[at : at + n, :] = jnp.where(c == 0, own, got)
        out[at + n : at + 2 * n, :] = jnp.where(c == 0, got, own)

    for j, ref in enumerate((qw, kw, vw)):
        both(attn, 2 * j * lead, own_columns(ref[...], c), far[j * lead : (j + 1) * lead, :])
    both(attn, 6 * lead, small[...], far[3 * lead :, :])
    both(up, 0, own_columns(uw[...], c), up_far[...])


def inner_moves(ins, outs):
    own, first, second, far1, far2 = ins[:5]
    cut = far1.shape[0]
    return [
        (own, outs[0].at[0]),
        (first, outs[0].at[1]),
        (second, outs[0].at[2]),
        (far1, outs[0].at[3, pl.ds(0, cut)]),
        (far2, outs[0].at[3, pl.ds(cut, far2.shape[0])]),
    ]


def ring_first(value, n1, n2):
    return send(value, n1), send(value, n2)


def ring_second(a, b, f1, f2):
    cut = a.shape[0] // 2 // 16 * 16
    return send(a[:cut], f1), send(b[cut:], f2)


def ring_outer_second(a, b, f1, f2):
    return send(a[:2], f1), send(b[2:], f2)


def final_moves(ins, outs, blocks):
    o, _, z = place()
    z_ring = (z, lax.rem(z + 3, 4), lax.rem(z + 1, 4), lax.rem(z + 2, 4))
    yx_ring = (o, o ^ 1, o ^ 2, o ^ 3)
    todo = []
    for k in range(4):
        for j in range(4):
            source = ins[k].at[j] if k < 3 else ins[3 + j // 2].at[j % 2]
            todo += blocks(source, outs, yx_ring[k], z_ring[j])
    return todo


def moments(values):
    mean = jnp.mean(values, axis=-1, keepdims=True)
    centered = values - mean
    spread = lax.rsqrt(jnp.mean(centered * centered, axis=-1, keepdims=True) + EPS)
    return centered * spread, spread


def project_kernel(x, gain, shift, weight, bias, normed, qkv):
    n, _ = moments(x[...].astype(F32))
    value = (n * gain[...] + shift[...]).astype(BF)
    normed[...] = value
    for j in range(3):
        qkv[j] = (dot32(value, weight[j], NN) + bias[j : j + 1, :]).astype(BF)


def project(x, gain, shift, weight, bias, after):
    total, width = x.shape
    half = weight.shape[2]
    rows = pl.BlockSpec((BLOCK, width), lambda i: (i, 0))
    line = pl.BlockSpec((1, width), lambda i: (0, 0))
    return call(
        project_kernel,
        [x, gain, shift, weight, bias],
        [shape((total, width)), shape((3, total, half))],
        "project",
        in_specs=[
            rows,
            line,
            line,
            pl.BlockSpec((3, width, half), lambda i: (0, 0, 0)),
            pl.BlockSpec((3, half), lambda i: (0, 0)),
        ],
        out_specs=[rows, pl.BlockSpec((3, BLOCK, half), lambda i: (0, i, 0))],
        flops=6 * total * width * half,
        grid=(total // BLOCK,),
        after=after,
    )


def allowed_mask(column, row, i, low, high):
    rows = i * BLOCK + lax.broadcasted_iota(jnp.int32, (BLOCK, high - low), 0)
    cols = low + lax.broadcasted_iota(jnp.int32, (BLOCK, high - low), 1)
    same = column[i * BLOCK : i * BLOCK + BLOCK, :] == row[:, low:high]
    return same & (cols <= rows)


def key_range(i, total):
    return max(0, (i * BLOCK - total // 2 + 1) // BLOCK * BLOCK), (i + 1) * BLOCK


def attend_kernel(scale, column, row, q_ref, k_ref, v_ref, *refs):
    mixed_ref, log_ref = refs[-2:]
    total = q_ref.shape[0]
    size = q_ref.shape[1] // 2
    lane = lax.broadcasted_iota(jnp.int32, (BLOCK, 2 * size), 1) < size
    for i in range(total // BLOCK):
        low, high = key_range(i, total)
        rows = pl.ds(i * BLOCK, BLOCK)
        mask = allowed_mask(column, row, i, low, high)
        keys, values = k_ref[low:high, :], v_ref[low:high, :]
        q = q_ref[rows, :]
        zero = jnp.zeros_like(q)
        outs, logs = [], []
        for own in (jnp.where(lane, q, zero), jnp.where(lane, zero, q)):
            s = jnp.where(mask, dot32(own, keys, NT) * scale, MASKED)
            top = jnp.max(s, axis=-1, keepdims=True)
            e = jnp.exp(s - top)
            tot = jnp.sum(e, axis=-1, keepdims=True)
            p = (e * (1.0 / tot)).astype(BF)
            outs.append(dot32(p, values, NN))
            logs.append(top + jnp.log(tot))
        mixed_ref[rows, :] = jnp.where(lane, outs[0], outs[1]).astype(BF)
        log_ref[rows, :] = jnp.where(lane, logs[0], logs[1])


def attend_back_kernel(
    scale, column, row, q_ref, k_ref, v_ref, log_ref, grad_ref, *refs
):
    out_ref, bias_ref, dk, dv = refs[-4:]
    total = q_ref.shape[0]
    size = q_ref.shape[1] // 2
    lane = lax.broadcasted_iota(jnp.int32, (BLOCK, 2 * size), 1) < size
    dk[...] = jnp.zeros_like(dk)
    dv[...] = jnp.zeros_like(dv)
    dq_sum = jnp.zeros((1, 2 * size), F32)
    for i in range(total // BLOCK):
        low, high = key_range(i, total)
        rows = pl.ds(i * BLOCK, BLOCK)
        mask = allowed_mask(column, row, i, low, high)
        keys, values = k_ref[low:high, :], v_ref[low:high, :]
        q, g = q_ref[rows, :], grad_ref[rows, :]
        zero = jnp.zeros_like(q)
        dqs = []
        for h in range(2):
            qh = jnp.where(lane, q, zero) if h == 0 else jnp.where(lane, zero, q)
            gh = jnp.where(lane, g, zero) if h == 0 else jnp.where(lane, zero, g)
            log = log_ref[rows, h * size : h * size + 1]
            s = jnp.where(mask, dot32(qh, keys, NT) * scale, MASKED)
            p = jnp.exp(s - log)
            dp = dot32(gh, values, NT)
            delta = jnp.sum(p * dp, axis=-1, keepdims=True)
            ds = (p * (dp - delta)).astype(BF)
            dqs.append(dot32(ds, keys, NN))
            dk[low:high, :] += dot32(ds, qh, TN)
            dv[low:high, :] += dot32(p.astype(BF), gh, TN)
        dq = (jnp.where(lane, dqs[0], dqs[1]) * scale).astype(BF)
        out_ref[0, rows, :] = dq
        dq_sum += jnp.sum(dq.astype(F32), axis=0, keepdims=True)
    out_ref[1, :, :] = (dk[...] * scale).astype(BF)
    dvb = dv[...].astype(BF)
    out_ref[2, :, :] = dvb
    bias_ref[0:1, :] = dq_sum
    bias_ref[1:2, :] = jnp.sum(dvb.astype(F32), axis=0, keepdims=True)


def attend_specs(total, width, first):
    pick = lambda j: pl.BlockSpec((None, total, width), lambda h: (j, 0, h + first))
    return [
        pl.BlockSpec((total, 1), lambda h: (0, 0)),
        pl.BlockSpec((1, total), lambda h: (0, 0)),
        pick(0),
        pick(1),
        pick(2),
    ]


def attend(qkv, column, row, size, part, before, after):
    _, total, width = qkv.shape
    pair = 2 * size
    count = width // pair // 2
    flat = pl.BlockSpec((total, pair), lambda h: (0, h + part * count))
    return call(
        partial(attend_kernel, 1.0 / math.sqrt(size)),
        [column, row, qkv, qkv, qkv, *before],
        [shape((total, width)), shape((total, width), F32)],
        "attend",
        in_specs=attend_specs(total, pair, part * count) + [ANY] * len(before),
        out_specs=[flat, flat],
        flops=total * total * width * 8,
        grid=(count,),
        after=after,
        aliases={5 + i: i for i in range(len(before))},
    )


def attend_back(qkv, log, grad, column, row, size, part, before, after):
    _, total, width = qkv.shape
    pair = 2 * size
    count = width // pair // 2
    flat = pl.BlockSpec((total, pair), lambda h: (0, h + part * count))
    return call(
        partial(attend_back_kernel, 1.0 / math.sqrt(size)),
        [column, row, qkv, qkv, qkv, log, grad, *before],
        [shape((3, total, width)), shape((2, width), F32)],
        "attend_back",
        in_specs=attend_specs(total, pair, part * count) + [flat, flat] + [ANY] * len(before),
        out_specs=[
            pl.BlockSpec((3, total, pair), lambda h: (0, 0, h + part * count)),
            pl.BlockSpec((2, pair), lambda h: (0, h + part * count)),
        ],
        scratch=[pltpu.VMEM((total, pair), F32)] * 2,
        flops=total * total * width * 12,
        grid=(count,),
        after=after,
        aliases={7 + i: i for i in range(len(before))},
    )


def rows_kernel(dims, left, right, out):
    out[...] = dot32(left[...], right[...], dims).astype(out.dtype)


def rows_matmul(left, right, dims, name, kind=BF, after=()):
    total, depth = left.shape
    cols = right.shape[0] if dims is NT else right.shape[1]
    return call(
        partial(rows_kernel, dims),
        [left, right],
        [shape((total, cols), kind)],
        name,
        in_specs=[
            pl.BlockSpec((BLOCK, depth), lambda i: (i, 0)),
            pl.BlockSpec(right.shape, lambda i: (0, 0)),
        ],
        out_specs=[pl.BlockSpec((BLOCK, cols), lambda i: (i, 0))],
        flops=2 * total * depth * cols,
        grid=(total // BLOCK,),
        after=after,
    )[0]


def middle_kernel(x, part, got, bias, gain, shift, middle, second):
    value = x[...].astype(F32) + part[...].astype(F32) + got[...].astype(F32) + bias[...]
    middle[...] = value
    n, _ = moments(value)
    second[...] = (n * gain[...] + shift[...]).astype(BF)


def middle_norm(x, part, got, bias, gain, shift):
    total, width = x.shape
    rows = pl.BlockSpec((BLOCK, width), lambda i: (i, 0))
    line = pl.BlockSpec((1, width), lambda i: (0, 0))
    return call(
        middle_kernel,
        [x, part, got, bias, gain, shift],
        [shape((total, width), F32), shape((total, width))],
        "middle",
        in_specs=[rows] * 3 + [line] * 3,
        out_specs=[rows, rows],
        grid=(total // BLOCK,),
    )


def feed_kernel(second, cot, up, bias, down, hidden_ref, pre_ref, sum_ref):
    total = second.shape[0]
    root = math.sqrt(0.5)
    norm = 1.0 / math.sqrt(2.0 * math.pi)
    sums = jnp.zeros(sum_ref.shape, F32)
    for i in range(total // BLOCK):
        rows = pl.ds(i * BLOCK, BLOCK)
        v = dot32(second[rows, :], up[...], NN) + bias[...]
        g = dot32(cot[rows, :], down[...], NT)
        cdf = 0.5 * (1.0 + lax.erf(v * root))
        hidden_ref[rows, :] = (v * cdf).astype(BF)
        pre = (g * (cdf + v * (norm * jnp.exp(-0.5 * (v * v))))).astype(BF)
        pre_ref[rows, :] = pre
        sums += jnp.sum(pre.astype(F32), axis=0, keepdims=True)
    sum_ref[...] = sums


def feed_forward(second, cot, up, bias, down, tile=256):
    total, width = second.shape
    units = up.shape[1]
    whole = pl.BlockSpec((total, width), lambda u: (0, 0))
    cols = pl.BlockSpec((total, tile), lambda u: (0, u))
    line = pl.BlockSpec((1, tile), lambda u: (0, u))
    return call(
        feed_kernel,
        [second, cot, up, bias, down],
        [shape((total, units)), shape((total, units)), shape((1, units), F32)],
        "feed",
        in_specs=[
            whole,
            whole,
            pl.BlockSpec((width, tile), lambda u: (0, u)),
            line,
            pl.BlockSpec((tile, width), lambda u: (u, 0)),
        ],
        out_specs=[cols, cols, line],
        flops=4 * total * width * units,
        grid=(units // tile,),
    )


def down_grads_kernel(pos, hidden, cot, far1, far2, n1, n2, own):
    g = pl.program_id(0)
    rows = own.shape[1]
    acc = dot32(hidden[...], cot[...], TN).astype(BF)
    for k, out in enumerate((None, n2, n1, own)):

        @pl.when(g == k)
        def _():
            for j in range(4):
                value = acc[j * rows : (j + 1) * rows, :]
                if k == 0:
                    (far1, far2)[j // 2][j % 2] = value
                else:
                    out[j] = value


def ring_shapes(rows, cols):
    return [shape((2, rows, cols))] * 2 + [shape((4, rows, cols))] * 3


def ring_specs(rows, cols):
    whole = lambda n: pl.BlockSpec((n, rows, cols), lambda g, pos: (0, 0, 0))
    return [whole(2)] * 2 + [whole(4)] * 3


def down_grads(pos, hidden, cot, rows, after):
    total, units = hidden.shape
    width = cot.shape[1]
    return placed_call(
        down_grads_kernel,
        pos,
        [hidden, cot],
        ring_shapes(rows, width),
        "down_grads",
        (4,),
        [
            pl.BlockSpec((total, units // 4), lambda g, pos: (0, pos[0] ^ (3 - g))),
            pl.BlockSpec((total, width), lambda g, pos: (0, 0)),
        ],
        ring_specs(rows, width),
        flops=2 * total * units * width,
        after=after,
    )


def z_places(z):
    return lax.rem(z + 2, 4), lax.rem(z + 1, 4), lax.rem(z + 3, 4), z


def split_ring(g, refs, store):
    far1, far2, n1, n2, own = refs
    for k, out in enumerate((None, n2, n1, own)):

        @pl.when(g == k)
        def _():
            for zz in range(4):
                if k:
                    store(out, zz, zz)
                else:
                    store((far1, far2)[zz // 2], zz % 2, zz)


def up_grads_kernel(pos, second, pre, *refs):
    lead = refs[-1].shape[1] // 2
    acc = dot32(second[...], pre[...], TN).astype(BF)

    def store(out, at, zz):
        for cc in range(2):
            start = (cc * 4 + zz) * lead
            out[at, cc * lead : (cc + 1) * lead, :] = acc[start : start + lead, :]

    split_ring(pl.program_id(0), refs, store)


def up_grads(pos, second, pre, lead, after):
    total, width = second.shape
    units = pre.shape[1]
    return placed_call(
        up_grads_kernel,
        pos,
        [second, pre],
        ring_shapes(2 * lead, units),
        "up_grads",
        (4,),
        [
            pl.BlockSpec((total, width // 4), lambda g, pos: (0, pos[0] ^ (3 - g))),
            pl.BlockSpec((total, units), lambda g, pos: (0, 0)),
        ],
        ring_specs(2 * lead, units),
        flops=2 * total * units * width,
        after=after,
    )


def attn_grads_kernel(pos, normed, grads, mixed, branch, *refs):
    lead = refs[-1].shape[1] // 8
    half = refs[-1].shape[2]
    accs = [dot32(normed[...], grads[j], TN).astype(BF) for j in range(3)]
    acco = dot32(mixed[...], branch[...], TN).astype(BF)

    def store(out, at, zz):
        for cc in range(2):
            for j, acc in enumerate(accs):
                row, start = (2 * j + cc) * lead, (cc * 4 + zz) * lead
                out[at, row : row + lead, :] = acc[start : start + lead, :]
            row = (6 + cc) * lead
            out[at, row : row + lead, :] = acco[
                zz * lead : (zz + 1) * lead, cc * half : (cc + 1) * half
            ]

    split_ring(pl.program_id(0), refs, store)


def attn_grads(pos, normed, grads, mixed, branch, lead, after):
    total, width = normed.shape
    half = width // 2
    return placed_call(
        attn_grads_kernel,
        pos,
        [normed, grads, mixed, branch],
        ring_shapes(8 * lead, half),
        "attn_grads",
        (4,),
        [
            pl.BlockSpec((total, width // 4), lambda g, pos: (0, pos[0] ^ (3 - g))),
            pl.BlockSpec((3, total, half), lambda g, pos: (0, 0, 0)),
            pl.BlockSpec((total, half // 4), lambda g, pos: (0, pos[0] ^ (3 - g))),
            pl.BlockSpec((total, width), lambda g, pos: (0, 0)),
        ],
        ring_specs(8 * lead, half),
        flops=8 * total * width * half,
        after=after,
    )


def pass_kernel(n1, n2, t1, t2, s1, s2):
    for s, n, t, part in ((s1, n1, t2, 1), (s2, n2, t1, 0)):
        for j in range(4):
            if j // 2 == part:
                s[j] = (n[j].astype(F32) + t[j % 2].astype(F32)).astype(BF)
            else:
                s[j] = n[j]


def far_round(ring):
    return send(ring[0], X_SWAP), send(ring[1], Y_SWAP)


def near_round(ring, got, name, after=()):
    s1, s2 = call(
        pass_kernel,
        [ring[2], ring[3], *got],
        [shape(ring[2].shape)] * 2,
        name + "_pass",
        after=after,
    )
    return s1, [send(s1, X_SWAP), send(s2, Y_SWAP)]


def joined_kernel(extra):
    def body(own, r1, r2, *refs):
        far1, far2, first, second, mine, acc = refs[extra:]
        rows = own.shape[1]
        for j in range(4):
            acc[j, :rows, :] = own[j].astype(F32) + r1[j].astype(F32) + r2[j].astype(F32)
            if extra:
                acc[j, rows:, :] = sum(ref[j].astype(F32) for ref in refs[:extra])
        far, one, two, me = z_places(place()[2])
        cut = far1.shape[0]
        far1[...] = acc[far, :cut, :].astype(BF)
        far2[...] = acc[far, cut:, :].astype(BF)
        first[...] = acc[one].astype(BF)
        second[...] = acc[two].astype(BF)
        mine[...] = acc[me]

    return body


def join(ring, got, name, extra=(), after=()):
    _, rows, cols = ring[4].shape
    rows += extra[0].shape[1] if extra else 0
    cut = rows // 2 // 16 * 16
    return call(
        joined_kernel(len(extra)),
        [ring[4], *got, *extra],
        [
            shape((cut, cols)),
            shape((rows - cut, cols)),
            shape((rows, cols)),
            shape((rows, cols)),
            shape((rows, cols), F32),
        ],
        name + "_join",
        scratch=[pltpu.VMEM((4, rows, cols), F32)],
        after=after,
    )


def inner_pass_kernel(p1, p2, t1, t2, p1o, p2o):
    cut = p1.shape[0] // 2 // 16 * 16
    plus = lambda a, got: (a.astype(F32) + got[...].astype(F32)).astype(BF)
    p1o[:cut, :] = plus(p1[:cut, :], t1)
    p1o[cut:, :] = p1[cut:, :]
    p2o[:cut, :] = p2[:cut, :]
    p2o[cut:, :] = plus(p2[cut:, :], t2)


def inner_far(joined):
    return send(joined[0], Z_UP), send(joined[1], Z_DOWN)


def inner_near(joined, came, name, after=()):
    p1, p2 = call(
        inner_pass_kernel,
        [joined[2], joined[3], *came],
        [shape(joined[2].shape)] * 2,
        name + "_inner",
        after=after,
    )
    return p1, [joined[4], send(p1, Z_UP), send(p2, Z_DOWN)]


def total_of(refs):
    return refs[0][...] + refs[1][...].astype(F32) + refs[2][...].astype(F32)


def feed_last_kernel(p0, p1, p2, q0, q1, q2, down, kept, given, acc):
    _, c, _ = place()
    down[...] = total_of((p0, p1, p2))
    acc[...] = total_of((q0, q1, q2))
    lead = kept.shape[0]
    kept[...] = acc[pl.ds(pl.multiple_of(c * lead, lead), lead), :]
    given[...] = acc[pl.ds(pl.multiple_of((1 - c) * lead, lead), lead), :]


def attn_last_kernel(p0, p1, p2, kept, given, out, small, acc):
    _, c, _ = place()
    acc[...] = total_of((p0, p1, p2))
    lead = kept.shape[1]
    half = kept.shape[2]
    for j in range(3):
        at = 2 * j * lead
        kept[j] = acc[pl.ds(pl.multiple_of(at + c * lead, lead), lead), :]
        given[j] = acc[pl.ds(pl.multiple_of(at + (1 - c) * lead, lead), lead), :]
    out[:, :half] = acc[6 * lead : 7 * lead, :]
    out[:, half:] = acc[7 * lead : 8 * lead, :]
    small[...] = acc[8 * lead :, :]


def norm_back(n, spread, gain, grad):
    g = grad * gain
    return spread * (
        g - jnp.mean(g, axis=-1, keepdims=True) - n * jnp.mean(g * n, axis=-1, keepdims=True)
    )


def column(values):
    return jnp.sum(values, axis=0, keepdims=True)


def middle_back_kernel(part, got, middle, cot, gain, wout, branch, mgrad, mixed, sums):
    n, spread = moments(middle[...])
    grad = part[...].astype(F32) + got[...].astype(F32)
    c32 = cot[...].astype(F32)
    value = c32 + norm_back(n, spread, gain[...], grad)
    mgrad[...] = value
    rounded = value.astype(BF)
    branch[...] = rounded
    mixed[...] = dot32(rounded, wout[...], NT).astype(BF)

    @pl.when(pl.program_id(0) == 0)
    def _():
        sums[...] = jnp.zeros_like(sums)

    for j, v in enumerate((grad * n, grad, rounded.astype(F32), c32)):
        sums[j : j + 1, :] += column(v)


def middle_back(part, got, middle, cot, gain, wout, after):
    total, width = middle.shape
    half = wout.shape[0]
    rows = pl.BlockSpec((BLOCK, width), lambda i: (i, 0))
    fixed = lambda dims: pl.BlockSpec(dims, lambda i: (0, 0))
    return call(
        middle_back_kernel,
        [part, got, middle, cot, gain, wout],
        [
            shape((total, width)),
            shape((total, width), F32),
            shape((total, half)),
            shape((4, width), F32),
        ],
        "middle_back",
        in_specs=[rows] * 4 + [fixed((1, width)), fixed((half, width))],
        out_specs=[
            rows,
            rows,
            pl.BlockSpec((BLOCK, half), lambda i: (i, 0)),
            fixed((4, width)),
        ],
        flops=2 * total * width * half,
        grid=(total // BLOCK,),
        after=after,
    )


def source_grad_kernel(grads, weight, out):
    out[...] = sum(dot32(grads[j], weight[j], NT) for j in range(3)).astype(BF)


def source_grad(grads, weight, after):
    _, total, half = grads.shape
    width = weight.shape[1]
    return call(
        source_grad_kernel,
        [grads, weight],
        [shape((total, width))],
        "source_grad",
        in_specs=[
            pl.BlockSpec((3, BLOCK, half), lambda i: (0, i, 0)),
            pl.BlockSpec((3, width, half), lambda i: (0, 0, 0)),
        ],
        out_specs=[pl.BlockSpec((BLOCK, width), lambda i: (i, 0))],
        flops=6 * total * width * half,
        grid=(total // BLOCK,),
        after=after,
    )[0]


def own_block(g, pos):
    _, c, z = pos[0], pos[1], pos[2]
    parity = lax.rem(z, 2)
    return jnp.where(g < 2, 2 * c + (parity ^ (g & 1)), 2 * (1 - c) + (g & 1))


def input_back_kernel(pos, part, got, x, mgrad, gain, first, again, sums):
    g = pl.program_id(0)
    n, spread = moments(x[...].astype(F32))
    grad = part[...].astype(F32) + got[...].astype(F32)
    value = (mgrad[...] + norm_back(n, spread, gain[...], grad)).astype(BF)

    @pl.when(g == 0)
    def _():
        first[...] = value
        sums[...] = jnp.zeros_like(sums)

    @pl.when(g == 1)
    def _():
        again[...] = value

    for j, v in enumerate((grad * n, grad)):
        sums[j : j + 1, :] += column(v)


def input_back(pos, part, got, x, mgrad, gain, after):
    total, width = x.shape
    rows = pl.BlockSpec((BLOCK, width), lambda g, pos: (own_block(g, pos), 0))
    fixed = lambda n: pl.BlockSpec((n, width), lambda g, pos: (0, 0))
    return placed_call(
        input_back_kernel,
        pos,
        [part, got, x, mgrad, gain],
        [shape((BLOCK, width))] * 2 + [shape((2, width), F32)],
        "input_back",
        (total // BLOCK,),
        [rows] * 4 + [fixed(1)],
        [fixed(BLOCK), fixed(BLOCK), fixed(2)],
        after=after,
    )


def other_block(g, pos):
    return jnp.where(g < 2, 2 * (1 - pos[1]) + (g & 1), 2 * pos[1] + (g & 1))


def output_kernel(pos, hidden, down, middle, bias, theirs, mine):
    g = pl.program_id(0)
    value = dot32(hidden[...], down[...], NN)

    @pl.when(g < 2)
    def _():
        theirs[...] = value.astype(BF)

    @pl.when(g >= 2)
    def _():
        mine[...] = value + middle[...] + bias[...]


def output_rows(pos, hidden, down, middle, bias, after):
    total, units = hidden.shape
    width = down.shape[1]
    return placed_call(
        output_kernel,
        pos,
        [hidden, down, middle, bias],
        [shape((total // 2, width)), shape((total // 2, width), F32)],
        "output_rows",
        (4,),
        [
            pl.BlockSpec((BLOCK, units), lambda g, pos: (other_block(g, pos), 0)),
            pl.BlockSpec((units, width), lambda g, pos: (0, 0)),
            pl.BlockSpec((BLOCK, width), lambda g, pos: (other_block(g, pos), 0)),
            pl.BlockSpec((1, width), lambda g, pos: (0, 0)),
        ],
        [
            pl.BlockSpec((BLOCK, width), lambda g, pos: (jnp.minimum(g, 1), 0)),
            pl.BlockSpec((BLOCK, width), lambda g, pos: (jnp.maximum(g - 2, 0), 0)),
        ],
        flops=2 * total * units * width,
        after=after,
    )


def result_kernel(mine, got, first, again):
    _, _, z = place()
    parity = lax.rem(z, 2)
    for k, out in enumerate((first, again)):
        at = pl.multiple_of((parity ^ k) * BLOCK, BLOCK)
        out[...] = (mine[pl.ds(at, BLOCK), :] + got[pl.ds(at, BLOCK), :].astype(F32)).astype(BF)

XY_FAR = links(lambda o, c, z: (o ^ 3, c, z))


def fast_local(
    inputs,
    segment_ids,
    first_gain,
    first_shift,
    query_weight,
    query_bias,
    key_weight,
    value_weight,
    value_bias,
    out_weight,
    out_bias,
    second_gain,
    second_shift,
    up_weight,
    up_bias,
    down_weight,
    down_bias,
    cotangent,
):
    batch, rows, width = inputs.shape
    o, c, z = place()
    pos = jnp.stack([o, c, z]).astype(jnp.int32)
    total = batch * rows * 2
    half = width // 2
    units = up_weight.shape[1] // 2
    lead = query_weight.shape[0]
    down_rows = down_weight.shape[0]
    size = width // H
    vector_list = [
        first_gain,
        first_shift,
        query_bias,
        value_bias,
        out_bias,
        second_gain,
        second_shift,
        down_bias,
        up_bias,
    ]
    count = 8 * lead + down_rows

    small, at = jnp.zeros((half,), BF), 0
    for vector in vector_list:
        small = small + jnp.pad(vector, (at, half - at - vector.shape[0]))
        at += vector.shape[0]
    small = jnp.pad(small.reshape(1, half), ((0, 7), (0, 0)))
    weights = [query_weight, key_weight, value_weight]
    far, up_far = call(
        first_kernel,
        weights + [up_weight, small],
        [shape((3 * lead + 8, half)), shape((lead, units))],
        "first",
    )
    attn_pay, up_pay = call(
        second_kernel,
        weights + [up_weight, small, send(far, CORE_SWAP), send(up_far, CORE_SWAP)],
        [shape((6 * lead + 16, half)), shape((2 * lead, units))],
        "second",
    )

    pa, pb = ring_first(attn_pay, Z_UP, Z_DOWN)
    pc = ring_second(pa, pb, Z_UP, Z_DOWN)
    attn_all, down_own = copies(
        [attn_pay, pa, pb, *pc, down_weight, out_weight],
        [shape((4,) + attn_pay.shape), shape((down_rows + lead, width))],
        lambda ins, outs: inner_moves(ins, outs)
        + [
            (ins[5], outs[1].at[pl.ds(0, down_rows)]),
            (ins[6], outs[1].at[pl.ds(down_rows, lead)]),
        ],
        7,
        "attn_inner",
    )
    aa, ab = ring_first(attn_all, X_SWAP, Y_SWAP)
    da, db = ring_first(down_own, Z_UP, Z_DOWN)
    dc = ring_second(da, db, Z_UP, Z_DOWN)
    ac = ring_outer_second(aa, ab, Y_SWAP, X_SWAP)

    in0, in1 = call(
        inputs_kernel,
        [inputs, segment_ids],
        [shape((rows + 16, width))] * 2,
        "inputs_own",
        in_specs=[ANY, VMEM],
        scratch=[pltpu.SemaphoreType.DMA((2,))],
        after=[aa, ab, *dc],
    )
    got = [send(in0, SEQUENCE[0]), send(in1, SEQUENCE[1])]

    def sequence_moves(ins, outs):
        _, cc, zz = place()
        parity = lax.rem(zz, 2)
        todo = []
        for m in range(2):
            for k in range(2):
                piece = ins[2 * m + k]
                at = (1 - cc if m else cc, parity ^ k)
                todo.append((piece.at[pl.ds(0, rows)], outs[0].at[at]))
                if len(outs) > 1:
                    todo.append((piece.at[pl.ds(rows, 16)], outs[1].at[at]))
        return todo + ([(ins[4], outs[2])] if len(outs) > 1 else [])

    def whole_sequence(pieces, name, after=(), more=()):
        outs = [shape((2, 2, rows, width))]
        if more:
            outs += [shape((2, 2, 16, width)), shape(more[0].shape)]
        return copies(
            pieces + list(more), outs, sequence_moves, 9 if more else 4, name, after=after
        )

    down_all = copies(
        [down_own, da, db, *dc],
        [shape((4,) + down_own.shape)],
        inner_moves,
        5,
        "down_inner",
        after=[*ac, in0],
    )[0]
    ea, eb = ring_first(down_all, X_SWAP, Y_SWAP)
    *got, _ = lax.optimization_barrier((*got, down_all))
    x, segments, up_own = whole_sequence(
        got + [send(g, CORE_SWAP) for g in got], "inputs_whole", more=[up_pay]
    )
    x = x.reshape(total, width)
    segments = segments[:, :, 0, :rows].reshape(total).astype(F32)
    seg_col, seg_row = segments.reshape(total, 1), segments.reshape(1, total)

    ua, ub = ring_first(up_own, Z_UP, Z_DOWN)

    def attn_blocks(src, outs, yx, zz):
        todo = [
            (src.at[pl.ds((2 * j + cc) * lead, lead)], outs[0].at[j, yx, cc, zz])
            for j in range(3)
            for cc in range(2)
        ]
        return todo + [(src.at[pl.ds(6 * lead, 16)], outs[1].at[yx, zz])]

    wqkv, small_all = copies(
        [attn_all, aa, ab, *ac],
        [shape((3, 4, 2, 4, lead, half)), shape((4, 4, 16, half))],
        lambda ins, outs: final_moves(ins, outs, attn_blocks),
        16 * 7,
        "attn_whole",
        after=[down_all],
    )
    wqkv = wqkv.reshape(3, width, half)

    small_all = small_all.reshape(4, 4, 2, 8, half)[:, :, :, 0, :count]
    vectors = small_all[..., : 8 * lead].reshape(4, 4, 2, 8, lead).transpose(3, 0, 2, 1, 4)
    own_cols = lax.dynamic_index_in_dim(vectors, c, 2, keepdims=False).reshape(8, half)
    vectors = vectors.reshape(8, width).astype(F32)
    line = lambda j: vectors[j : j + 1]
    gain1, shift1, bias_o, gain2, shift2, bias_d = [line(j) for j in (0, 1, 4, 5, 6, 7)]
    qkv_bias = jnp.stack([own_cols[2], jnp.zeros_like(own_cols[2]), own_cols[3]]).astype(F32)
    bias_u = lax.dynamic_index_in_dim(small_all[..., 8 * lead :], c, 2, keepdims=False)
    bias_u = bias_u.reshape(1, units).astype(F32)

    normed, qkv = project(x, gain1, shift1, wqkv, qkv_bias, [])
    uc = ring_second(ua, ub, Z_UP, Z_DOWN)

    def cotangent_moves(ins, outs):
        parity = lax.rem(place()[2], 2)
        return [(ins[0].at[parity], outs[0]), (ins[0].at[1 - parity], outs[1])]

    cots = copies(
        [cotangent],
        [shape((rows, width))] * 2,
        cotangent_moves,
        2,
        "cotangent_own",
        after=[*uc, normed],
    )
    cot_got = [send(block, pairs) for block, pairs in zip(cots, SEQUENCE)]
    ec = ring_outer_second(ea, eb, Y_SWAP, X_SWAP)
    up_all = copies(
        [up_own, ua, ub, *uc],
        [shape((4,) + up_pay.shape)],
        inner_moves,
        5,
        "up_inner",
        after=[*ec, normed],
    )[0]
    heads = attend(qkv, seg_col, seg_row, size, 0, [], [up_all, *cots])
    mixed, log = attend(qkv, seg_col, seg_row, size, 1, heads, [])
    fa, fb = ring_first(up_all, X_SWAP, Y_SWAP)

    def down_blocks(src, outs, yx, zz):
        return [
            (src.at[pl.ds(0, down_rows)], outs[0].at[yx, zz]),
            (src.at[pl.ds(down_rows, lead)], outs[1].at[yx, zz]),
        ]

    wdown, wout = copies(
        [down_all, ea, eb, *ec],
        [shape((4, 4, down_rows, width)), shape((4, 4, lead, width))],
        lambda ins, outs: final_moves(ins, outs, down_blocks),
        32,
        "down_whole",
        after=[mixed],
    )
    wdown, wout = wdown.reshape(units, width), wout.reshape(half, width)
    *cot_got, _ = lax.optimization_barrier((*cot_got, mixed))
    cot = whole_sequence(
        cot_got + [send(g, CORE_SWAP) for g in cot_got], "cotangent_whole", [wout]
    )[0].reshape(total, width)
    part = rows_matmul(mixed, wout, NN, "attend_out", after=[fa, fb, cot])
    middle, second = middle_norm(x, part, send(part, CORE_SWAP), bias_o, gain2, shift2)
    def up_blocks(src, outs, yx, zz):
        return [(src.at[pl.ds(cc * lead, lead)], outs[0].at[yx, cc, zz]) for cc in range(2)]

    wup = copies(
        [up_all, fa, fb, *ring_outer_second(fa, fb, Y_SWAP, X_SWAP)],
        [shape((4, 2, 4, lead, units))],
        lambda ins, outs: final_moves(ins, outs, up_blocks),
        32,
        "up_whole",
        after=[second],
    )[0].reshape(width, units)
    hidden, pre_grad, up_bias_grad = feed_forward(second, cot, wup, bias_u, wdown)

    def to_tokens(got):
        return jnp.where((z & 1) == 0, jnp.stack(got), jnp.stack(got[::-1]))

    theirs, mine = output_rows(pos, hidden, wdown, middle, bias_d, [])
    part = rows_matmul(pre_grad, wup, NT, "second_grad", after=[mine])
    d = down_grads(pos, hidden, cot, down_rows, [part])
    d_far = far_round(d)
    u = up_grads(pos, second, pre_grad, lead, [d[4]])
    u_far = far_round(u)
    passed, d_got = near_round(d, d_far, "down", [u[4]])
    blocks = call(
        result_kernel,
        [mine, send(theirs, CORE_SWAP)],
        [shape((rows, width))] * 2,
        "result",
        after=[passed],
    )
    out_got = [send(block, pairs) for block, pairs in zip(blocks, SEQUENCE)]
    branch, middle_grad, mixed_grad, sums2 = middle_back(
        part, send(part, CORE_SWAP), middle, cot, gain2, wout, [blocks[0]]
    )

    passed, u_got = near_round(u, u_far, "up", [branch])
    back = attend_back(qkv, log, mixed_grad, seg_col, seg_row, size, 0, [], [passed])
    output = to_tokens(out_got)
    d_joined = join(d, d_got, "down", after=[back[1]])
    d_came = inner_far(d_joined)
    grads, qv_bias_grad = attend_back(
        qkv, log, mixed_grad, seg_col, seg_row, size, 1, back, [d_joined[4]]
    )
    passed, d_last = inner_near(d_joined, d_came, "down", [qv_bias_grad, *out_got])
    u_joined = list(join(u, u_got, "up", after=[passed]))
    part = source_grad(grads, wqkv, [u_joined[4]])
    got = send(part, CORE_SWAP)
    a = attn_grads(pos, normed, grads, mixed, branch, lead, [part])
    a_far = far_round(a)
    in0, in1, sums1 = input_back(pos, part, got, x, middle_grad, gain1, [a[4], *d_last[1:]])
    in_got = [send(block, pairs) for block, pairs in zip((in0, in1), SEQUENCE)]
    input_grad = to_tokens(in_got).astype(F32)

    wide = jnp.stack([sums1[0], sums1[1], sums2[2], sums2[0], sums2[1], sums2[3]])
    wide = lax.dynamic_index_in_dim(wide.reshape(6, 4, 2, 4, lead), c, 2, keepdims=False)
    wide = jnp.concatenate(
        [wide[:2], qv_bias_grad.reshape(2, 4, 4, lead), wide[2:]], axis=0
    ).transpose(2, 1, 0, 3)
    tiny = jnp.concatenate(
        [
            wide.reshape(4, 4, 8 * lead),
            up_bias_grad.reshape(4, 4, down_rows).transpose(1, 0, 2),
        ],
        axis=-1,
    ).astype(BF)
    tiny = jnp.pad(tiny[:, :, None], ((0, 0), (0, 0), (0, 15), (0, half - count)))
    pick = lambda k: lax.dynamic_index_in_dim(tiny, o ^ k, 1, keepdims=False)
    extra = [pick(0), send(pick(1), X_SWAP), send(pick(2), Y_SWAP), send(pick(3), XY_FAR)]

    passed, a_got = near_round(a, a_far, "attn", [in0, *extra[1:]])
    joined = join(a, a_got, "attn", extra, in_got)
    came = inner_far(joined)
    *u_joined[:2], _ = lax.optimization_barrier((*u_joined[:2], joined[4]))
    u_came = inner_far(u_joined)
    passed, attn_last = inner_near(joined, came, "attn")
    _, u_last = inner_near(u_joined, u_came, "up", [passed])
    qkv_kept, qkv_given, out_out, small_sum = call(
        attn_last_kernel,
        attn_last,
        [shape((3, lead, half), F32)] * 2 + [shape((lead, width), F32), shape((16, half), F32)],
        "attn_last",
        scratch=[pltpu.VMEM((8 * lead + 16, half), F32)],
    )

    down_out, up_kept, up_given = call(
        feed_last_kernel,
        d_last + u_last,
        [shape(down_weight.shape, F32)] + [shape((lead, units), F32)] * 2,
        "feed_last",
        scratch=[pltpu.VMEM((2 * lead, units), F32)],
        after=[small_sum],
    )

    def whole_columns(kept, got):
        cols = kept.shape[-1] // 4
        kept, got = [a.reshape(a.shape[:-1] + (4, 1, cols)) for a in (kept, got)]
        both = jnp.where(
            c == 0, jnp.concatenate([kept, got], -2), jnp.concatenate([got, kept], -2)
        )
        return both.reshape(both.shape[:-3] + (8 * cols,))

    up_out = whole_columns(up_kept, send(up_given, CORE_SWAP))
    qkv_out = whole_columns(qkv_kept, send(qkv_given, CORE_SWAP))
    small_sum = small_sum[0]
    vec = lambda j: small_sum[j * lead : (j + 1) * lead]
    return (
        output,
        input_grad,
        vec(0),
        vec(1),
        qkv_out[0],
        vec(2),
        qkv_out[1],
        qkv_out[2],
        vec(3),
        out_out,
        vec(4),
        vec(5),
        vec(6),
        up_out,
        small_sum[8 * lead : count],
        down_out,
        vec(7),
    )


def solution(mesh):
    fast = mesh.shape["dp"] == 8 and mesh.shape["ctx"] == 4
    return jax.shard_map(
        fast_local if fast else local,
        mesh=mesh,
        in_specs=(
            P("dp", "ctx", None),
            P("dp", "ctx"),
            P(("dp", "ctx")),
            P(("dp", "ctx")),
            P(("dp", "ctx"), None),
            P(("dp", "ctx")),
            P(("dp", "ctx"), None),
            P(("dp", "ctx"), None),
            P(("dp", "ctx")),
            P(("dp", "ctx"), None),
            P(("dp", "ctx")),
            P(("dp", "ctx")),
            P(("dp", "ctx")),
            P(("dp", "ctx"), None),
            P(("dp", "ctx")),
            P(("dp", "ctx"), None),
            P(("dp", "ctx")),
            P("dp", "ctx", None),
        ),
        out_specs=(
            P("dp", "ctx", None),
            P("dp", "ctx", None),
            P(("dp", "ctx")),
            P(("dp", "ctx")),
            P(("dp", "ctx"), None),
            P(("dp", "ctx")),
            P(("dp", "ctx"), None),
            P(("dp", "ctx"), None),
            P(("dp", "ctx")),
            P(("dp", "ctx"), None),
            P(("dp", "ctx")),
            P(("dp", "ctx")),
            P(("dp", "ctx")),
            P(("dp", "ctx"), None),
            P(("dp", "ctx")),
            P(("dp", "ctx"), None),
            P(("dp", "ctx")),
        ),
        check_vma=False,
    )
```
